32 devices in a mesh: dp: 4 (over y, x), ep: 8 (over z, core).
Axes of the slice: x: 2, y: 2, z: 4, core: 2. Of those that a mesh axis runs over, the one named last changes fastest.
Arguments:
- tokens: bfloat16 [4096, 7168], P(('dp', 'ep')), may hold values from -6 to 6
- out_grad: bfloat16 [4096, 7168], P(('dp', 'ep')), may hold values from -3 to 3
- route_weight: float32 [4096, 1], P(('dp', 'ep')), may hold values from 0.2 to 1
- expert_ids: int32 [4096, 1], P(('dp', 'ep')), may hold values from 0 to 1
- w_gate: bfloat16 [1024, 14336], P('dp', 'ep'), may hold values from -0.0625 to 0.0625
- w_up: bfloat16 [1024, 14336], P('dp', 'ep'), may hold values from -0.0625 to 0.0625
- w_down: bfloat16 [1024, 14336], P('dp', 'ep'), may hold values from -0.1875 to 0.1875
Outputs:
- in_grad: bfloat16 [4096, 7168], P(('dp', 'ep'))
- grad_gate: bfloat16 [1024, 14336], P('dp', 'ep')
- grad_up: bfloat16 [1024, 14336], P('dp', 'ep')
- grad_down: bfloat16 [1024, 14336], P('dp', 'ep')
The draws below stay inside these ranges and needn't reach their ends.
All inputs are finite; a program needn't handle non-finite values.
Results may differ from the reference program's by a relative error of at most 0.012.
Values may be sent and summed in bfloat16 or wider, within the bound.
A program may use at most 128 MiB of HBM per device.

```python
import jax
import jax.numpy as jnp
from jax import lax

D = 7168
FF = 1024
GROUP = 4
TOP = 1
TOK_DEV = 128
EXPERTS = 2
CAP = 48
TOKENS = 4096
N_DP = 4
N_EP = 8


def shard_levels(key, dims, pieces, low, top_value):
    factor_of, own = 1.0, jax.random.fold_in(key, 6)
    for dim, parts in pieces:
        heights = jnp.exp(jax.random.uniform(jax.random.fold_in(own, dim), (parts,), jnp.float32, low / len(pieces), top_value / len(pieces)))
        factor_of = factor_of * jnp.repeat(heights, dims[dim] // parts).reshape([-1 if axis == dim else 1 for axis in range(len(dims))])
    return factor_of


def picks_of(own_key, rows, count, top, lift):
    sequence = jax.random.permutation(jax.random.fold_in(own_key, 1), count)
    pull = sequence
    for power in range(3):
        pull = pull * pull // count
    pull = pull * lift // count
    chance = jax.random.randint(jax.random.fold_in(own_key, 2), (rows, count), 0, 4096) + pull
    fixed_rows = jax.random.permutation(jax.random.fold_in(own_key, 3), rows)[jnp.arange(count) % rows]
    chance = jnp.where(jnp.arange(rows)[:, None] == fixed_rows[None, :], 1 << 14, chance)
    score = chance * count + jnp.arange(count)
    return lax.top_k(score.astype(jnp.int32), top)[1].astype(jnp.int32)


def centred(rng, dims, width, most, cuts=(), held_as=jnp.bfloat16):
    drawn = width * jax.random.normal(rng, dims, jnp.float32)
    if cuts:
        drawn = drawn * shard_levels(rng, dims, cuts, -0.22, 0.18)
    return jnp.clip(drawn, -most, most).astype(held_as)


def setup_inputs(seed: int = 0) -> dict:
    splits = jax.random.split(jax.random.key(seed), 8)
    tokens = centred(splits[0], (TOKENS, D), 1.0, 6.0, ((0, 32),))
    out_grad = centred(splits[1], (TOKENS, D), 0.5, 3.0, ((0, 32),))
    route_weight = jnp.clip(0.2 + 0.8 * jax.random.uniform(splits[2], (TOKENS, TOP), jnp.float32) ** shard_levels(splits[2], (TOKENS, TOP), ((0, 32),), -0.2, 0.2), 0.2, 1.0)
    expert_ids = picks_of(splits[3], TOKENS, EXPERTS, TOP, 8192)
    w_gate = centred(splits[4], (FF, EXPERTS * D), D ** -0.5, 0.0625, ((0, 4), (1, 8)))
    w_up = centred(splits[5], (FF, EXPERTS * D), D ** -0.5, 0.0625, ((0, 4), (1, 8)))
    w_down = centred(splits[6], (FF, EXPERTS * D), FF ** -0.5, 0.1875, ((0, 4), (1, 8)))
    return {"tokens": tokens, "out_grad": out_grad, "route_weight": route_weight, "expert_ids": expert_ids, "w_gate": w_gate, "w_up": w_up, "w_down": w_down}


CONTRACT_LAST = (((1,), (1,)), ((), ()))
CONTRACT_FIRST = (((0,), (0,)), ((), ()))


def slot_tables(expert_ids, route_weight, experts, capacity):
    token_count, top_count = expert_ids.shape
    pair_count = token_count * top_count
    flat_ids = expert_ids.reshape(pair_count)
    onehot = (flat_ids[:, None] == jnp.arange(experts, dtype=jnp.int32)[None, :]).astype(jnp.int32)
    before = jnp.cumsum(onehot, axis=0) - onehot
    ranks = jnp.sum(before * onehot, axis=1)
    kept = ranks < capacity
    slots = jnp.where(kept, flat_ids * capacity + ranks, 0).astype(jnp.int32)
    slot_ids = jnp.arange(experts * capacity, dtype=jnp.int32)
    match = (slots[None, :] == slot_ids[:, None]) & kept[None, :]
    pair_ids = jnp.arange(pair_count, dtype=jnp.int32)
    pair_of_slot = jnp.sum(jnp.where(match, pair_ids[None, :], 0), axis=1).astype(jnp.int32)
    filled = jnp.any(match, axis=1)
    flat_weight = route_weight.reshape(pair_count)
    weight_of_slot = jnp.sum(jnp.where(match, flat_weight[None, :], jnp.float32(0.0)), axis=1)
    return kept, slots, pair_of_slot // top_count, filled, weight_of_slot


def source_slots(tokens, out_grad, route_weight, expert_ids):
    kept, slots, token_of_slot, filled, weight_of_slot = slot_tables(expert_ids, route_weight, EXPERTS, CAP)
    x_slots = jnp.take(tokens, token_of_slot, axis=0) * filled[:, None].astype(jnp.bfloat16)
    d_slots = (jnp.take(out_grad, token_of_slot, axis=0).astype(jnp.float32) * weight_of_slot[:, None]).astype(jnp.bfloat16)
    return x_slots, d_slots, kept, slots


def quarter_sum(left, weight):
    quarter = D // GROUP
    total = jnp.zeros((left.shape[0], weight.shape[0]), jnp.float32)
    for piece in range(GROUP):
        part = lax.dot_general(left[:, piece * quarter:(piece + 1) * quarter], weight[:, piece * quarter:(piece + 1) * quarter], CONTRACT_LAST, preferred_element_type=jnp.float32)
        total = total + lax.optimization_barrier(part.astype(jnp.bfloat16)).astype(jnp.float32)
    return total


def activations(gate, up, back):
    logistic = jax.nn.sigmoid(gate)
    silu = gate * logistic
    hidden = (silu * up).astype(jnp.bfloat16)
    d_gate = (back * up * logistic * (1.0 + gate * (1.0 - logistic))).astype(jnp.bfloat16)
    d_up = (back * silu).astype(jnp.bfloat16)
    return hidden, d_gate, d_up


def expert_work(operands):
    x_rows, d_rows, gate_w, up_w, down_w = operands
    gate = quarter_sum(x_rows, gate_w)
    up = quarter_sum(x_rows, up_w)
    back = quarter_sum(d_rows, down_w)
    hidden, d_gate, d_up = activations(gate, up, back)
    expert_dx = (jnp.dot(d_gate, gate_w, preferred_element_type=jnp.float32) + jnp.dot(d_up, up_w, preferred_element_type=jnp.float32)).astype(jnp.bfloat16)
    gate_term = lax.dot_general(d_gate, x_rows, CONTRACT_FIRST, preferred_element_type=jnp.float32).astype(jnp.bfloat16)
    up_term = lax.dot_general(d_up, x_rows, CONTRACT_FIRST, preferred_element_type=jnp.float32).astype(jnp.bfloat16)
    down_term = lax.dot_general(hidden, d_rows, CONTRACT_FIRST, preferred_element_type=jnp.float32).astype(jnp.bfloat16)
    return expert_dx, gate_term, up_term, down_term


def reference(tokens, out_grad, route_weight, expert_ids, w_gate, w_up, w_down):
    sources = N_DP * N_EP
    x_src = tokens.reshape(sources, TOK_DEV, D)
    d_src = out_grad.reshape(sources, TOK_DEV, D)
    w_src = route_weight.reshape(sources, TOK_DEV, TOP)
    i_src = expert_ids.reshape(sources, TOK_DEV, TOP)
    x_slots, d_slots, kept, slots = jax.vmap(source_slots)(x_src, d_src, w_src, i_src)
    x_slots = x_slots.reshape(N_DP, N_EP, EXPERTS, CAP, D)
    d_slots = d_slots.reshape(N_DP, N_EP, EXPERTS, CAP, D)
    gate_e = w_gate.reshape(FF, EXPERTS, D).transpose(1, 0, 2)
    up_e = w_up.reshape(FF, EXPERTS, D).transpose(1, 0, 2)
    down_e = w_down.reshape(FF, EXPERTS, D).transpose(1, 0, 2)
    grad_sums = [jnp.zeros((EXPERTS, FF, D), jnp.float32) for which in range(3)]
    returned = []
    for row in range(N_DP):
        x_rows = x_slots[row].transpose(1, 0, 2, 3).reshape(EXPERTS, N_EP * CAP, D)
        d_rows = d_slots[row].transpose(1, 0, 2, 3).reshape(EXPERTS, N_EP * CAP, D)
        expert_dx, gate_term, up_term, down_term = lax.map(expert_work, (x_rows, d_rows, gate_e, up_e, down_e))
        grad_sums = [grad_sums[0] + gate_term.astype(jnp.float32), grad_sums[1] + up_term.astype(jnp.float32), grad_sums[2] + down_term.astype(jnp.float32)]
        returned.append(expert_dx.reshape(EXPERTS, N_EP, CAP, D).transpose(1, 0, 2, 3).reshape(N_EP, EXPERTS * CAP, D))
    slot_rows = jnp.stack(returned, axis=0).reshape(sources, EXPERTS * CAP, D)

    def gather_back(rows, kept_one, slots_one):
        pair_rows = jnp.take(rows, slots_one, axis=0) * kept_one[:, None].astype(jnp.bfloat16)
        return jnp.sum(pair_rows.reshape(TOK_DEV, TOP, D).astype(jnp.float32), axis=1).astype(jnp.bfloat16)

    in_grad = jax.vmap(gather_back)(slot_rows, kept, slots).reshape(TOK_DEV * sources, D)
    outs = [total.astype(jnp.bfloat16).transpose(1, 0, 2).reshape(FF, EXPERTS * D) for total in grad_sums]
    return in_grad, outs[0], outs[1], outs[2]
```

```python
import jax
import jax.numpy as jnp
from jax import lax
from jax.experimental import pallas as pl
from jax.experimental.pallas import tpu as pltpu
from jax.sharding import PartitionSpec as P

D = 7168
GROUP = 4
TOP = 1


CONTRACT_LAST = (((1,), (1,)), ((), ()))
CONTRACT_FIRST = (((0,), (0,)), ((), ()))


def as_sent(value):

    def short(part):
        return part.astype(jnp.bfloat16) if part.dtype == jnp.float32 else part

    return jax.tree.map(short, value)


def from_partner(value, axis, distance):
    mask = 2**distance
    pairs = [(source, source ^ mask) for source in range(lax.axis_size(axis))]
    return lax.ppermute(value, axis, pairs)


def slot_tables(expert_ids, route_weight, experts, capacity):
    token_count, top_count = expert_ids.shape
    pair_count = token_count * top_count
    flat_ids = expert_ids.reshape(pair_count)
    onehot = (flat_ids[:, None] == jnp.arange(experts, dtype=jnp.int32)[None, :]).astype(jnp.int32)
    before = jnp.cumsum(onehot, axis=0) - onehot
    ranks = jnp.sum(before * onehot, axis=1)
    kept = ranks < capacity
    slots = jnp.where(kept, flat_ids * capacity + ranks, 0)
    slot_ids = jnp.arange(experts * capacity, dtype=jnp.int32)
    match = (slots[None, :] == slot_ids[:, None]) & kept[None, :]
    pair_ids = jnp.arange(pair_count, dtype=jnp.int32)
    pair_of_slot = jnp.sum(jnp.where(match, pair_ids[None, :], 0), axis=1)
    filled = jnp.any(match, axis=1)
    flat_weight = route_weight.reshape(pair_count)
    weight_of_slot = jnp.sum(jnp.where(match, flat_weight[None, :], jnp.float32(0.0)), axis=1)
    return (kept, slots, pair_of_slot // top_count, filled, weight_of_slot)


def activations(gate, up, back):
    logistic = jax.nn.sigmoid(gate)
    silu = gate * logistic
    hidden = (silu * up).astype(jnp.bfloat16)
    d_gate = (back * up * logistic * (1.0 + gate * (1.0 - logistic))).astype(jnp.bfloat16)
    d_up = (back * silu).astype(jnp.bfloat16)
    return (hidden, d_gate, d_up)


def swap(value, axis, distance):
    return from_partner(value, axis, distance)


def wide(value):
    return value.astype(jnp.float32)


def dot_last(left, right):
    return lax.dot_general(left, right, CONTRACT_LAST, preferred_element_type=jnp.float32)


def dot_first(left, right):
    return lax.dot_general(left, right, CONTRACT_FIRST, preferred_element_type=jnp.float32)


def body(tokens, out_grad, route_weight, expert_ids, w_gate, w_up, w_down):
    devices_ep = lax.axis_size("ep")
    experts = devices_ep // GROUP
    token_count = tokens.shape[0]
    capacity = 6 * GROUP * token_count * TOP // (8 * devices_ep)
    quarter = D // GROUP
    short = jnp.bfloat16
    kept, slots, token_of_slot, filled, weight_of_slot = slot_tables(
        expert_ids, route_weight, experts, capacity
    )
    other_w = tuple(swap(w, "dp", 1) for w in (w_gate, w_up, w_down))
    token_ids = jnp.arange(token_count, dtype=jnp.int32)
    pick = ((token_of_slot[:, None] == token_ids[None, :]) & filled[:, None]).astype(short)
    x_slots = jnp.dot(pick, tokens, preferred_element_type=jnp.float32).astype(short)
    d_slots = (
        jnp.dot(pick, out_grad, preferred_element_type=jnp.float32) * weight_of_slot[:, None]
    ).astype(short)

    def to_owners(rows):
        shaped = rows.reshape(experts, capacity, GROUP, quarter).transpose(0, 2, 1, 3)
        return shaped.reshape(devices_ep, capacity, quarter)

    def sent(rows):
        return lax.all_to_all(to_owners(rows), "ep", split_axis=0, concat_axis=0, tiled=True)

    row_count = devices_ep * capacity
    x_own = sent(x_slots).reshape(row_count, quarter)
    d_own = sent(d_slots).reshape(row_count, quarter)
    x_other, d_other = swap(x_own, "dp", 0), swap(d_own, "dp", 0)
    core = lax.axis_index("ep") % 2
    weights = ((w_gate, w_up, w_down), other_w)
    acts = []
    for x_rows, d_rows in ((x_own, d_own), (x_other, d_other)):
        terms = [
            jnp.concatenate(
                [dot_last(x_rows, wg), dot_last(x_rows, wu), dot_last(d_rows, wd)], axis=1
            ).astype(short)
            for wg, wu, wd in weights
        ]
        give = jnp.where(core == 0, terms[1], terms[0])
        keep = jnp.where(core == 0, terms[0], terms[1])
        pair = (wide(keep) + wide(swap(give, "ep", 0))).astype(short)
        total = wide(pair) + wide(swap(pair, "ep", 1))
        width = total.shape[1] // 3
        mine = jnp.concatenate(
            activations(total[:, :width], total[:, width : 2 * width], total[:, 2 * width :]), axis=1
        )
        theirs = swap(mine, "ep", 0)
        first = jnp.where(core == 0, mine, theirs)
        second = jnp.where(core == 0, theirs, mine)
        acts.append(
            tuple(
                tuple(half[:, piece * width : (piece + 1) * width] for piece in range(3))
                for half in (first, second)
            )
        )

    def grads(half):
        (h0, g0, u0), (h1, g1, u1) = acts[0][half], acts[1][half]
        return (
            dot_first(g0, x_own) + dot_first(g1, x_other),
            dot_first(u0, x_own) + dot_first(u1, x_other),
            dot_first(h0, d_own) + dot_first(h1, d_other),
        )

    def dx(rows):
        return sum(
            jnp.dot(acts[rows][half][1], weights[half][0], preferred_element_type=jnp.float32)
            + jnp.dot(acts[rows][half][2], weights[half][1], preferred_element_type=jnp.float32)
            for half in range(2)
        )

    dx_in = swap(dx(1).astype(short), "dp", 0)
    away = tuple(swap(term.astype(short), "dp", 1) for term in grads(1))
    expert_dx = (dx(0) + wide(dx_in)).astype(short)
    grad_gate, grad_up, grad_down = (
        (own + wide(term)).astype(short) for own, term in zip(grads(0), away)
    )
    returned = lax.all_to_all(
        expert_dx.reshape(devices_ep, capacity, quarter),
        "ep",
        split_axis=0,
        concat_axis=0,
        tiled=True,
    )
    slot_rows = (
        returned.reshape(experts, GROUP, capacity, quarter)
        .transpose(0, 2, 1, 3)
        .reshape(experts * capacity, D)
    )
    in_grad = dot_first(pick, slot_rows).astype(short)
    return (in_grad, grad_gate, grad_up, grad_down)

MESH = pl.DeviceIdType.MESH


def flip(index, bit):
    size = 1 << bit
    return index + size - 2 * size * lax.rem(lax.div(index, size), 2)


def expert_kernel(
    tokens, out_grad, route, ids, wg, wu, wd, in_grad, grad_gate, grad_up, grad_down,
    tok, ogr, pick, pick_t, scale, xs, ds, slot_rows, x_all, d_all, w_all, part, got, pair, across,
    act, act_t, term_out, term_in, term_own, dx_out, dx_in, dx_own, dx_sum,
    in_sem, w_local, w_send, w_recv, self_sem, x_send, x_recv, d_send, d_recv,
    fx_send, fx_recv, fd_send, fd_recv, give_send, give_recv, pair_send, pair_recv,
    act_send, act_recv, term_send, term_recv, dx_send, dx_recv, back_send, back_recv,
):
    devices_ep, capacity, quarter = dx_sum.shape
    rows = devices_ep * capacity
    half_rows = rows // 2
    hidden = wg.shape[0]
    slots, token_count = pick.shape
    experts = slots // capacity
    short = jnp.bfloat16
    r, s = lax.axis_index("dp"), lax.axis_index("ep")
    core, z = lax.rem(s, 2), lax.div(s, 2)
    side = lax.div(z, 2)
    at_end = lax.rem(z, 2) == side
    row_mate, weight_mate = (flip(r, 0), s), (flip(r, 1), s)
    core_mate, chip_mate = (r, flip(s, 0)), (r, flip(s, 1))
    far_mid, far_end = 2 * (2 - side), 2 * (3 - 3 * side)
    near = [flip(s, 1), flip(flip(s, 1), 0)]
    mids = [far_mid + core, far_mid + 1 - core]
    ends = [far_end + core, far_end + 1 - core]
    others = [flip(s, 0)] + near + ends + mids
    CORE, NEAR, FAR = [0], [1, 2], [3, 4, 5, 6]

    def local(source, target, sem):
        copy = pltpu.make_async_copy(source, target, sem)
        copy.start()
        return copy

    weights = (wg, wu, wd)
    own_w = [local(w, w_all.at[0, i], w_local.at[i]) for i, w in enumerate(weights)]
    tok_copy = local(tokens, tok, in_sem.at[0])
    ogr_copy = local(out_grad, ogr, in_sem.at[1])

    barrier = pltpu.get_barrier_semaphore()
    peers = [row_mate, weight_mate] + [(r, other) for other in others]
    for peer in peers:
        pl.semaphore_signal(barrier, inc=1, device_id=peer, device_id_type=MESH)

    named = ids[...]
    wide_rows = max(8, experts)
    expert_row = lax.broadcasted_iota(jnp.int32, (wide_rows, token_count), 0)
    onehot = jnp.where(expert_row == named, 1.0, 0.0)
    earlier = lax.broadcasted_iota(jnp.int32, (token_count, token_count), 0) < (
        lax.broadcasted_iota(jnp.int32, (token_count, token_count), 1)
    )
    before = jnp.dot(
        onehot.astype(short), jnp.where(earlier, 1.0, 0.0).astype(short),
        preferred_element_type=jnp.float32,
    )
    rank = jnp.sum(before * onehot, axis=0, keepdims=True)
    slot = jnp.where(rank < capacity, named.astype(jnp.float32) * capacity + rank, -1.0)
    slot_row = lax.broadcasted_iota(jnp.int32, (slots, token_count), 0).astype(jnp.float32)
    match = jnp.where(slot_row == slot, 1.0, 0.0)
    pick[...] = match.astype(short)
    scale[...] = jnp.sum(match * route[...], axis=1, keepdims=True)
    pick_t[...] = match.T.astype(short)

    pl.semaphore_wait(barrier, len(peers))

    def remote(source, target, send, recv, peer, start=True):
        copy = pltpu.make_async_remote_copy(
            src_ref=source, dst_ref=target, send_sem=send, recv_sem=recv,
            device_id=peer, device_id_type=MESH,
        )
        if start:
            copy.start()
        return copy

    def owned(ref, device):
        row = pl.multiple_of(lax.div(device, GROUP) * capacity, capacity)
        column = pl.multiple_of(lax.rem(device, GROUP) * quarter, 128)
        return ref.at[pl.ds(row, capacity), pl.ds(column, quarter)]

    w_copies = []
    for i in range(3):
        own_w[i].wait()
        w_copies.append(
            remote(w_all.at[0, i], w_all.at[1, i], w_send.at[i], w_recv.at[i], weight_mate)
        )

    def by_quarters(fn):
        def one(n, carry):
            fn(pl.ds(pl.multiple_of(n * quarter, quarter), quarter))
            return carry

        lax.fori_loop(0, GROUP, one, 0)

    def fill_x(at):
        xs[:, at] = jnp.dot(
            pick[...], tok[:, at], preferred_element_type=jnp.float32
        ).astype(short)

    def fill_d(at):
        ds[:, at] = (
            jnp.dot(pick[...], ogr[:, at], preferred_element_type=jnp.float32) * scale[...]
        ).astype(short)

    kinds = ((xs, x_all, x_send, x_recv), (ds, d_all, d_send, d_recv))

    def flow(kind, n):
        source, target, send, recv = kinds[kind]
        peer = others[n]
        return remote(
            owned(source, peer), target.at[0, s], send.at[n], recv.at[s], (r, peer), start=False
        )

    def send(kind, which):
        for n in which:
            flow(kind, n).start()

    self_copies = []
    tok_copy.wait()
    by_quarters(fill_x)
    send(0, CORE + NEAR)
    self_copies.append(local(owned(xs, s), x_all.at[0, s], self_sem.at[0]))

    @pl.when(jnp.logical_not(at_end))
    def _():
        send(0, FAR)

    ogr_copy.wait()
    by_quarters(fill_d)
    send(1, CORE + NEAR)
    self_copies.append(local(owned(ds, s), d_all.at[0, s], self_sem.at[1]))

    @pl.when(at_end)
    def _():
        send(0, FAR)

    passed = ([], [])

    def pass_on(kind, n):
        _, target, _, recv = kinds[kind]
        if n is None:
            origin = s
            self_copies[kind].wait()
        else:
            origin = others[n]
            remote(
                target.at[0, origin], target.at[0, origin], x_send.at[0], recv.at[origin],
                (r, origin), start=False,
            ).wait_recv()
        to_send, to_recv = ((fx_send, fx_recv), (fd_send, fd_recv))[kind]
        passed[kind].append(
            remote(
                target.at[0, origin], target.at[1, origin], to_send.at[origin],
                to_recv.at[origin], row_mate,
            )
        )

    def project(k, which, i):
        block = (x_all if i < 2 else d_all)[k].reshape(rows, quarter)
        part[k, which, i] = dot_last(block, w_all[which, i]).astype(short)

    STEP = 48

    def by_rows(fn):
        def one(n, carry):
            fn(pl.ds(pl.multiple_of(n * STEP, STEP), STEP))
            return carry

        lax.fori_loop(0, rows // STEP, one, 0)

    give_copies, pair_copies, act_copies = {}, {}, {}

    def hand_over(k, i):
        give_copies[k, i] = remote(
            part.at[k, 1 - core, i], got.at[k, i],
            give_send.at[3 * k + i], give_recv.at[3 * k + i], core_mate,
        )

    def send_pair(k, i):
        give_copies[k, i].wait_recv()

        def add_pair(at):
            pair[k, i, at, :] = (wide(part[k, core, i, at, :]) + wide(got[k, i, at, :])).astype(
                short
            )

        by_rows(add_pair)
        pair_copies[k, i] = remote(
            pair.at[k, i], across.at[k, i],
            pair_send.at[3 * k + i], pair_recv.at[3 * k + i], chip_mate,
        )

    def total(k, i, at):
        return wide(pair[k, i, at, :]) + wide(across[k, i, at, :])

    def make_hidden(k):
        for i in range(2):
            pair_copies[k, i].wait_recv()

        def one(at):
            gate, up = total(k, 0, at), total(k, 1, at)
            act[k, core, 0, at, :] = (gate * jax.nn.sigmoid(gate) * up).astype(short)

        by_rows(one)
        act_copies[k, 0] = remote(
            act.at[k, core, 0], act.at[k, core, 0],
            act_send.at[2 * k], act_recv.at[2 * k], core_mate,
        )

    def make_slopes(k):
        pair_copies[k, 2].wait_recv()

        def one(at):
            made = activations(total(k, 0, at), total(k, 1, at), total(k, 2, at))
            act[k, core, 1, at, :] = made[1]
            act[k, core, 2, at, :] = made[2]

        by_rows(one)
        act_copies[k, 1] = remote(
            act.at[k, core, pl.ds(1, 2)], act.at[k, core, pl.ds(1, 2)],
            act_send.at[2 * k + 1], act_recv.at[2 * k + 1], core_mate,
        )

    def transpose(which, piece):
        for k in range(2):
            act_t[which, piece, :, k * rows : (k + 1) * rows] = act[k, which, piece].T

    LANES = 896

    def by_columns(fn):
        def one(n, carry):
            fn(pl.ds(pl.multiple_of(n * LANES, LANES), LANES))
            return carry

        lax.fori_loop(0, quarter // LANES, one, 0)

    def term(which, i, at):
        block = (x_all if i < 2 else d_all)[:, :, :, at].reshape(2 * rows, LANES)
        return jnp.dot(
            act_t[which, (i + 1) % 3], block, preferred_element_type=jnp.float32
        )

    CUTS = 4
    term_copies = {}

    def send_term(i):
        def make(at):
            term_out[i, :, at] = term(1, i, at).astype(short)

        by_columns(make)
        size = hidden // CUTS
        for n in range(CUTS):
            cut = pl.ds(n * size, size)
            term_copies[i, n] = remote(
                term_out.at[i, cut], term_in.at[i, cut],
                term_send.at[CUTS * i + n], term_recv.at[CUTS * i + n], weight_mate,
            )

    def own_term(i):
        def make(at):
            term_own[i, :, at] = term(0, i, at)

        by_columns(make)

    def finish(i):
        size = hidden // CUTS
        out = (grad_gate, grad_up, grad_down)[i]
        for n in range(CUTS):
            cut = pl.ds(n * size, size)
            term_copies[i, n].wait_recv()
            out[cut, :] = (term_own[i, cut, :] + wide(term_in[i, cut, :])).astype(short)

    def expert_dx(k, part_of, at):
        here = pl.ds(pl.multiple_of(part_of * half_rows, half_rows), half_rows)
        return sum(
            jnp.dot(
                act[k, which, i + 1, here, :], w_all[which, i, :, at],
                preferred_element_type=jnp.float32,
            )
            for which in range(2)
            for i in range(2)
        ).reshape(devices_ep // 2, capacity, LANES)

    dx_blocks = ends + mids + near + [flip(s, 0), s]
    dx_copies = []

    def send_dx(part_of, blocks):
        here = pl.ds(part_of * (devices_ep // 2), devices_ep // 2)

        def make(at):
            dx_out[here, :, at] = expert_dx(1, part_of, at).astype(short)

        by_columns(make)
        for n in blocks:
            block = dx_blocks[n]
            dx_copies.append(
                remote(
                    dx_out.at[block], dx_in.at[block], dx_send.at[n], dx_recv.at[n], row_mate
                )
            )

    def own_dx(part_of):
        here = pl.ds(part_of * (devices_ep // 2), devices_ep // 2)

        def make(at):
            dx_own[here, :, at] = expert_dx(0, part_of, at)

        by_columns(make)

    backs = []

    def give_back(n):
        block = dx_blocks[n]
        dx_copies[n].wait_recv()
        dx_sum[block] = (dx_own[block] + wide(dx_in[block])).astype(short)
        if n < devices_ep - 1:
            backs.append(
                remote(
                    dx_sum.at[block], owned(slot_rows, s), back_send.at[n], back_recv.at[s],
                    (r, block),
                )
            )
        else:
            backs.append(local(dx_sum.at[block], owned(slot_rows, s), self_sem.at[2]))

    pass_on(0, None)
    for n in CORE + NEAR:
        pass_on(0, n)
    pass_on(0, 5)
    pass_on(0, 6)
    pass_on(1, None)
    pass_on(0, 3)
    pass_on(0, 4)

    @pl.when(jnp.logical_not(at_end))
    def _():
        send(1, FAR)

    @pl.when(at_end)
    def _():
        send(1, FAR[:1])

    for n in CORE + NEAR:
        pass_on(1, n)
    project(0, 0, 0)
    w_copies[0].wait_recv()
    project(0, 1, 0)
    hand_over(0, 0)
    project(0, 0, 1)
    send_pair(0, 0)
    for copy in passed[0]:
        copy.wait_recv()
    project(1, 0, 0)
    project(1, 1, 0)
    hand_over(1, 0)
    project(1, 0, 1)
    send_pair(1, 0)

    @pl.when(at_end)
    def _():
        send(1, FAR[1:])

    pass_on(1, 5)
    w_copies[1].wait_recv()
    project(0, 1, 1)
    hand_over(0, 1)
    project(1, 1, 1)
    hand_over(1, 1)
    pass_on(1, 6)
    send_pair(0, 1)
    send_pair(1, 1)
    pass_on(1, 3)
    pass_on(1, 4)
    project(0, 0, 2)
    make_hidden(0)
    make_hidden(1)
    w_copies[2].wait_recv()
    project(0, 1, 2)
    hand_over(0, 2)
    for copy in passed[1]:
        copy.wait_recv()
    project(1, 0, 2)
    project(1, 1, 2)
    hand_over(1, 2)
    send_pair(0, 2)
    for k in range(2):
        act_copies[k, 0].wait_recv()
    transpose(1, 0)
    send_term(2)
    send_pair(1, 2)
    transpose(0, 0)
    own_term(2)
    make_slopes(0)
    make_slopes(1)
    act_copies[0, 1].wait_recv()
    act_copies[1, 1].wait_recv()
    send_dx(1 - side, range(0, 4))
    send_dx(side, range(4, 8))
    transpose(1, 1)
    send_term(0)
    transpose(1, 2)
    send_term(1)
    own_dx(1 - side)
    for n in range(4):
        give_back(n)
    own_dx(side)
    finish(2)
    transpose(0, 1)
    own_term(0)
    transpose(0, 2)
    own_term(1)
    for n in range(4, 8):
        give_back(n)
    finish(0)
    backs[-1].wait()
    for origin in others:
        remote(
            dx_sum.at[0], owned(slot_rows, origin), back_send.at[0], back_recv.at[origin],
            (r, origin), start=False,
        ).wait_recv()

    def fill_in(at):
        in_grad[:, at] = jnp.dot(
            pick_t[...], slot_rows[:, at], preferred_element_type=jnp.float32
        ).astype(short)

    by_quarters(fill_in)
    finish(1)
    for kind in range(2):
        for n in range(devices_ep - 1):
            flow(kind, n).wait_send()
    sent = w_copies + passed[0] + passed[1] + list(give_copies.values())
    sent += list(pair_copies.values()) + list(act_copies.values())
    sent += list(term_copies.values()) + dx_copies + backs[:-1]
    for copy in sent:
        copy.wait_send()


def fast_body(tokens, out_grad, route_weight, expert_ids, w_gate, w_up, w_down):
    devices_ep = lax.axis_size("ep")
    experts = devices_ep // GROUP
    token_count = tokens.shape[0]
    capacity = 6 * GROUP * token_count * TOP // (8 * devices_ep)
    quarter = D // GROUP
    hidden = w_gate.shape[0]
    rows = devices_ep * capacity
    slots = experts * capacity
    short = jnp.bfloat16
    vmem = pl.BlockSpec(memory_space=pltpu.VMEM)
    hbm = pl.BlockSpec(memory_space=pl.ANY)
    grad = jax.ShapeDtypeStruct(w_gate.shape, short)
    dma = pltpu.SemaphoreType.DMA
    in_grad, grad_gate, grad_up, grad_down = pl.pallas_call(
        expert_kernel,
        out_shape=(jax.ShapeDtypeStruct(tokens.shape, short), grad, grad, grad),
        in_specs=[hbm, hbm, vmem, vmem, hbm, hbm, hbm],
        out_specs=(vmem, vmem, vmem, vmem),
        scratch_shapes=[
            pltpu.VMEM(tokens.shape, short),
            pltpu.VMEM(tokens.shape, short),
            pltpu.VMEM((slots, token_count), short),
            pltpu.VMEM((token_count, slots), short),
            pltpu.VMEM((slots, 1), jnp.float32),
            pltpu.VMEM((slots, D), short),
            pltpu.VMEM((slots, D), short),
            pltpu.VMEM((slots, D), short),
            pltpu.VMEM((2, devices_ep, capacity, quarter), short),
            pltpu.VMEM((2, devices_ep, capacity, quarter), short),
            pltpu.VMEM((2, 3, hidden, quarter), short),
            pltpu.VMEM((2, 2, 3, rows, hidden), short),
            pltpu.VMEM((2, 3, rows, hidden), short),
            pltpu.VMEM((2, 3, rows, hidden), short),
            pltpu.VMEM((2, 3, rows, hidden), short),
            pltpu.VMEM((2, 2, 3, rows, hidden), short),
            pltpu.VMEM((2, 3, hidden, 2 * rows), short),
            pltpu.VMEM((3, hidden, quarter), short),
            pltpu.VMEM((3, hidden, quarter), short),
            pltpu.VMEM((3, hidden, quarter), jnp.float32),
            pltpu.VMEM((devices_ep, capacity, quarter), short),
            pltpu.VMEM((devices_ep, capacity, quarter), short),
            pltpu.VMEM((devices_ep, capacity, quarter), jnp.float32),
            pltpu.VMEM((devices_ep, capacity, quarter), short),
        ]
        + [dma((2,))]
        + [dma((3,))] * 4
        + [dma((devices_ep,))] * 8
        + [dma((6,))] * 4
        + [dma((4,))] * 2
        + [dma((12,))] * 2
        + [dma((devices_ep,))] * 4,
        compiler_params=pltpu.CompilerParams(
            collective_id=0, has_side_effects=True, vmem_limit_bytes=60 * 2**20
        ),
    )(
        tokens, out_grad, route_weight.reshape(1, token_count),
        expert_ids.reshape(1, token_count), w_gate, w_up, w_down,
    )
    return (in_grad, grad_gate, grad_up, grad_down)


def solution(mesh):
    devices_ep = mesh.shape["ep"]

    def step(*arrays):
        token_count = arrays[0].shape[0]
        capacity = 6 * GROUP * token_count * TOP // (8 * devices_ep)
        hidden = arrays[4].shape[0]
        fits = capacity % 48 == 0 and hidden % 128 == 0 and token_count % 128 == 0
        fits = fits and mesh.shape["dp"] == 4 and devices_ep == 2 * GROUP
        return (fast_body if fits else body)(*arrays)

    placed = (
        P(("dp", "ep"), None),
        P(("dp", "ep"), None),
        P(("dp", "ep"), None),
        P(("dp", "ep"), None),
        P("dp", "ep"),
        P("dp", "ep"),
        P("dp", "ep"),
    )
    return jax.shard_map(
        step,
        mesh=mesh,
        in_specs=placed,
        out_specs=(P(("dp", "ep"), None), P("dp", "ep"), P("dp", "ep"), P("dp", "ep")),
        check_vma=False,
    )
```

```python
import jax
import jax.numpy as jnp
from jax import lax
from jax.experimental import pallas as pl
from jax.experimental.pallas import tpu as pltpu
from jax.sharding import PartitionSpec as P

D = 7168
GROUP = 4
TOP = 1


CONTRACT_LAST = (((1,), (1,)), ((), ()))
CONTRACT_FIRST = (((0,), (0,)), ((), ()))


def as_sent(value):

    def short(part):
        return part.astype(jnp.bfloat16) if part.dtype == jnp.float32 else part

    return jax.tree.map(short, value)


def from_partner(value, axis, distance):
    mask = 2**distance
    pairs = [(source, source ^ mask) for source in range(lax.axis_size(axis))]
    return lax.ppermute(value, axis, pairs)


def slot_tables(expert_ids, route_weight, experts, capacity):
    token_count, top_count = expert_ids.shape
    pair_count = token_count * top_count
    flat_ids = expert_ids.reshape(pair_count)
    onehot = (flat_ids[:, None] == jnp.arange(experts, dtype=jnp.int32)[None, :]).astype(jnp.int32)
    before = jnp.cumsum(onehot, axis=0) - onehot
    ranks = jnp.sum(before * onehot, axis=1)
    kept = ranks < capacity
    slots = jnp.where(kept, flat_ids * capacity + ranks, 0)
    slot_ids = jnp.arange(experts * capacity, dtype=jnp.int32)
    match = (slots[None, :] == slot_ids[:, None]) & kept[None, :]
    pair_ids = jnp.arange(pair_count, dtype=jnp.int32)
    pair_of_slot = jnp.sum(jnp.where(match, pair_ids[None, :], 0), axis=1)
    filled = jnp.any(match, axis=1)
    flat_weight = route_weight.reshape(pair_count)
    weight_of_slot = jnp.sum(jnp.where(match, flat_weight[None, :], jnp.float32(0.0)), axis=1)
    return (kept, slots, pair_of_slot // top_count, filled, weight_of_slot)


def activations(gate, up, back):
    logistic = jax.nn.sigmoid(gate)
    silu = gate * logistic
    hidden = (silu * up).astype(jnp.bfloat16)
    d_gate = (back * up * logistic * (1.0 + gate * (1.0 - logistic))).astype(jnp.bfloat16)
    d_up = (back * silu).astype(jnp.bfloat16)
    return (hidden, d_gate, d_up)


def swap(value, axis, distance):
    return from_partner(value, axis, distance)


def wide(value):
    return value.astype(jnp.float32)


def dot_last(left, right):
    return lax.dot_general(left, right, CONTRACT_LAST, preferred_element_type=jnp.float32)


def dot_first(left, right):
    return lax.dot_general(left, right, CONTRACT_FIRST, preferred_element_type=jnp.float32)


def body(tokens, out_grad, route_weight, expert_ids, w_gate, w_up, w_down):
    devices_ep = lax.axis_size("ep")
    experts = devices_ep // GROUP
    token_count = tokens.shape[0]
    capacity = 6 * GROUP * token_count * TOP // (8 * devices_ep)
    quarter = D // GROUP
    short = jnp.bfloat16
    kept, slots, token_of_slot, filled, weight_of_slot = slot_tables(
        expert_ids, route_weight, experts, capacity
    )
    other_w = tuple(swap(w, "dp", 1) for w in (w_gate, w_up, w_down))
    token_ids = jnp.arange(token_count, dtype=jnp.int32)
    pick = ((token_of_slot[:, None] == token_ids[None, :]) & filled[:, None]).astype(short)
    x_slots = jnp.dot(pick, tokens, preferred_element_type=jnp.float32).astype(short)
    d_slots = (
        jnp.dot(pick, out_grad, preferred_element_type=jnp.float32) * weight_of_slot[:, None]
    ).astype(short)

    def to_owners(rows):
        shaped = rows.reshape(experts, capacity, GROUP, quarter).transpose(0, 2, 1, 3)
        return shaped.reshape(devices_ep, capacity, quarter)

    def sent(rows):
        return lax.all_to_all(to_owners(rows), "ep", split_axis=0, concat_axis=0, tiled=True)

    row_count = devices_ep * capacity
    x_own = sent(x_slots).reshape(row_count, quarter)
    d_own = sent(d_slots).reshape(row_count, quarter)
    x_other, d_other = swap(x_own, "dp", 0), swap(d_own, "dp", 0)
    core = lax.axis_index("ep") % 2
    weights = ((w_gate, w_up, w_down), other_w)
    acts = []
    for x_rows, d_rows in ((x_own, d_own), (x_other, d_other)):
        terms = [
            jnp.concatenate(
                [dot_last(x_rows, wg), dot_last(x_rows, wu), dot_last(d_rows, wd)], axis=1
            ).astype(short)
            for wg, wu, wd in weights
        ]
        give = jnp.where(core == 0, terms[1], terms[0])
        keep = jnp.where(core == 0, terms[0], terms[1])
        pair = (wide(keep) + wide(swap(give, "ep", 0))).astype(short)
        total = wide(pair) + wide(swap(pair, "ep", 1))
        width = total.shape[1] // 3
        mine = jnp.concatenate(
            activations(total[:, :width], total[:, width : 2 * width], total[:, 2 * width :]), axis=1
        )
        theirs = swap(mine, "ep", 0)
        first = jnp.where(core == 0, mine, theirs)
        second = jnp.where(core == 0, theirs, mine)
        acts.append(
            tuple(
                tuple(half[:, piece * width : (piece + 1) * width] for piece in range(3))
                for half in (first, second)
            )
        )

    def grads(half):
        (h0, g0, u0), (h1, g1, u1) = acts[0][half], acts[1][half]
        return (
            dot_first(g0, x_own) + dot_first(g1, x_other),
            dot_first(u0, x_own) + dot_first(u1, x_other),
            dot_first(h0, d_own) + dot_first(h1, d_other),
        )

    def dx(rows):
        return sum(
            jnp.dot(acts[rows][half][1], weights[half][0], preferred_element_type=jnp.float32)
            + jnp.dot(acts[rows][half][2], weights[half][1], preferred_element_type=jnp.float32)
            for half in range(2)
        )

    dx_in = swap(dx(1).astype(short), "dp", 0)
    away = tuple(swap(term.astype(short), "dp", 1) for term in grads(1))
    expert_dx = (dx(0) + wide(dx_in)).astype(short)
    grad_gate, grad_up, grad_down = (
        (own + wide(term)).astype(short) for own, term in zip(grads(0), away)
    )
    returned = lax.all_to_all(
        expert_dx.reshape(devices_ep, capacity, quarter),
        "ep",
        split_axis=0,
        concat_axis=0,
        tiled=True,
    )
    slot_rows = (
        returned.reshape(experts, GROUP, capacity, quarter)
        .transpose(0, 2, 1, 3)
        .reshape(experts * capacity, D)
    )
    in_grad = dot_first(pick, slot_rows).astype(short)
    return (in_grad, grad_gate, grad_up, grad_down)

MESH = pl.DeviceIdType.MESH


def flip(index, bit):
    size = 1 << bit
    return index + size - 2 * size * lax.rem(lax.div(index, size), 2)


def expert_kernel(
    tokens, out_grad, route, ids, wg, wu, wd, in_grad, grad_gate, grad_up, grad_down,
    named, paid, tok, ogr, pick, pick_t, scale, xs, ds, slot_rows, x_all, d_all, w_all, part, got, pair, across,
    act, act_t, term_out, term_in, term_own, dx_out, dx_in, dx_own, dx_sum,
    in_sem, w_local, w_send, w_recv, self_sem, x_send, x_recv, d_send, d_recv,
    fx_send, fx_recv, fd_send, fd_recv, give_send, give_recv, pair_send, pair_recv,
    act_send, act_recv, term_send, term_recv, dx_send, dx_recv, back_send, back_recv,
):
    devices_ep, capacity, quarter = dx_sum.shape
    rows = devices_ep * capacity
    half_rows = rows // 2
    hidden = wg.shape[0]
    slots, token_count = pick.shape
    experts = slots // capacity
    short = jnp.bfloat16
    r, s = lax.axis_index("dp"), lax.axis_index("ep")
    core, z = lax.rem(s, 2), lax.div(s, 2)
    side = lax.div(z, 2)
    end = 1 - lax.rem(z + side, 2)
    at_end = end == 1
    row_mate, weight_mate = (flip(r, 0), s), (flip(r, 1), s)
    core_mate, chip_mate = (r, flip(s, 0)), (r, flip(s, 1))
    far_mid, far_end = 2 * (2 - side), 2 * (3 - 3 * side)
    near = [flip(s, 1), flip(flip(s, 1), 0)]
    mids = [far_mid + core, far_mid + 1 - core]
    ends = [far_end + core, far_end + 1 - core]
    others = [flip(s, 0)] + near + ends + mids
    CORE, NEAR, FAR = [0], [1, 2], [3, 4, 5, 6]

    def local(source, target, sem):
        copy = pltpu.make_async_copy(source, target, sem)
        copy.start()
        return copy

    small = [local(ids, named, in_sem.at[2]), local(route, paid, in_sem.at[3])]
    weights = (wg, wu, wd)
    own_w = [local(w, w_all.at[i, 0], w_local.at[i]) for i, w in enumerate(weights)]
    tok_copy = local(tokens, tok, in_sem.at[0])
    ogr_copy = local(out_grad, ogr, in_sem.at[1])

    barrier = pltpu.get_barrier_semaphore()
    peers = [row_mate, weight_mate] + [(r, other) for other in others]
    for peer in peers:
        pl.semaphore_signal(barrier, inc=1, device_id=peer, device_id_type=MESH)

    for copy in small:
        copy.wait()
    name = named[...]
    wide_rows = max(8, experts)
    expert_row = lax.broadcasted_iota(jnp.int32, (wide_rows, token_count), 0)
    onehot = jnp.where(expert_row == name, 1.0, 0.0)
    earlier = lax.broadcasted_iota(jnp.int32, (token_count, token_count), 0) < (
        lax.broadcasted_iota(jnp.int32, (token_count, token_count), 1)
    )
    before = jnp.dot(
        onehot.astype(short), jnp.where(earlier, 1.0, 0.0).astype(short),
        preferred_element_type=jnp.float32,
    )
    rank = jnp.sum(before * onehot, axis=0, keepdims=True)
    slot = jnp.where(rank < capacity, name.astype(jnp.float32) * capacity + rank, -1.0)
    slot_row = lax.broadcasted_iota(jnp.int32, (slots, token_count), 0).astype(jnp.float32)
    match = jnp.where(slot_row == slot, 1.0, 0.0)
    pick[...] = match.astype(short)
    scale[...] = jnp.sum(match * paid[...], axis=1, keepdims=True)
    pick_t[...] = match.T.astype(short)

    pl.semaphore_wait(barrier, len(peers))

    def remote(source, target, send, recv, peer, start=True):
        copy = pltpu.make_async_remote_copy(
            src_ref=source, dst_ref=target, send_sem=send, recv_sem=recv,
            device_id=peer, device_id_type=MESH,
        )
        if start:
            copy.start()
        return copy

    def owned(ref, device):
        row = pl.multiple_of(lax.div(device, GROUP) * capacity, capacity)
        column = pl.multiple_of(lax.rem(device, GROUP) * quarter, 128)
        return ref.at[pl.ds(row, capacity), pl.ds(column, quarter)]

    w_copies = []
    for i in range(3):
        own_w[i].wait()
        w_copies.append(
            remote(w_all.at[i, 0], w_all.at[i, 1], w_send.at[i], w_recv.at[i], weight_mate)
        )

    def by_quarters(fn):
        def one(n, carry):
            fn(pl.ds(pl.multiple_of(n * quarter, quarter), quarter))
            return carry

        lax.fori_loop(0, GROUP, one, 0)

    def fill_x(at):
        xs[:, at] = jnp.dot(
            pick[...], tok[:, at], preferred_element_type=jnp.float32
        ).astype(short)

    def fill_d(at):
        ds[:, at] = (
            jnp.dot(pick[...], ogr[:, at], preferred_element_type=jnp.float32) * scale[...]
        ).astype(short)

    kinds = ((xs, x_all, x_send, x_recv), (ds, d_all, d_send, d_recv))

    def flow(kind, n):
        source, target, send, recv = kinds[kind]
        peer = others[n]
        return remote(
            owned(source, peer), target.at[0, s], send.at[n], recv.at[s], (r, peer), start=False
        )

    def send(kind, which):
        for n in which:
            flow(kind, n).start()

    self_copies = []
    tok_copy.wait()
    by_quarters(fill_x)
    send(0, CORE + NEAR)
    self_copies.append(local(owned(xs, s), x_all.at[0, s], self_sem.at[0]))

    @pl.when(jnp.logical_not(at_end))
    def _():
        send(0, FAR)

    ogr_copy.wait()
    by_quarters(fill_d)
    send(1, CORE + NEAR)
    self_copies.append(local(owned(ds, s), d_all.at[0, s], self_sem.at[1]))

    @pl.when(at_end)
    def _():
        send(0, FAR)

    passed = ([], [])

    def pass_on(kind, n):
        _, target, _, recv = kinds[kind]
        if n is None:
            origin = s
            self_copies[kind].wait()
        else:
            origin = others[n]
            remote(
                target.at[0, origin], target.at[0, origin], x_send.at[0], recv.at[origin],
                (r, origin), start=False,
            ).wait_recv()
        to_send, to_recv = ((fx_send, fx_recv), (fd_send, fd_recv))[kind]
        passed[kind].append(
            remote(
                target.at[0, origin], target.at[1, origin], to_send.at[origin],
                to_recv.at[origin], row_mate,
            )
        )

    def project(k, i):
        block = (x_all if i < 2 else d_all)[k].reshape(rows, quarter)
        both = dot_last(block, w_all[i].reshape(2 * hidden, quarter)).astype(short)
        for which in range(2):
            part[k, which, i] = both[:, which * hidden : (which + 1) * hidden]

    STEP = 48

    def by_rows(fn):
        def one(n, carry):
            fn(pl.ds(pl.multiple_of(n * STEP, STEP), STEP))
            return carry

        lax.fori_loop(0, rows // STEP, one, 0)

    give_copies, pair_copies, act_copies = {}, {}, {}

    def hand_over(k, i):
        give_copies[k, i] = remote(
            part.at[k, 1 - core, i], got.at[k, i],
            give_send.at[3 * k + i], give_recv.at[3 * k + i], core_mate,
        )

    def send_pair(k, i):
        give_copies[k, i].wait_recv()

        def add_pair(at):
            pair[k, i, at, :] = (wide(part[k, core, i, at, :]) + wide(got[k, i, at, :])).astype(
                short
            )

        by_rows(add_pair)
        pair_copies[k, i] = remote(
            pair.at[k, i], across.at[k, i],
            pair_send.at[3 * k + i], pair_recv.at[3 * k + i], chip_mate,
        )

    def total(k, i, at):
        return wide(pair[k, i, at, :]) + wide(across[k, i, at, :])

    def make_hidden(k):
        for i in range(2):
            pair_copies[k, i].wait_recv()

        def one(at):
            gate, up = total(k, 0, at), total(k, 1, at)
            act[k, core, 0, at, :] = (gate * jax.nn.sigmoid(gate) * up).astype(short)

        by_rows(one)
        act_copies[k, 0] = remote(
            act.at[k, core, 0], act.at[k, core, 0],
            act_send.at[2 * k], act_recv.at[2 * k], core_mate,
        )

    def make_slopes(k):
        pair_copies[k, 2].wait_recv()

        def one(at):
            made = activations(total(k, 0, at), total(k, 1, at), total(k, 2, at))
            act[k, core, 1, at, :] = made[1]
            act[k, core, 2, at, :] = made[2]

        by_rows(one)
        act_copies[k, 1] = remote(
            act.at[k, core, pl.ds(1, 2)], act.at[k, core, pl.ds(1, 2)],
            act_send.at[2 * k + 1], act_recv.at[2 * k + 1], core_mate,
        )

    def transpose(which, piece):
        for k in range(2):
            act_t[which, piece, :, k * rows : (k + 1) * rows] = act[k, which, piece].T

    LANES = 896

    def by_columns(fn):
        def one(n, carry):
            fn(pl.ds(pl.multiple_of(n * LANES, LANES), LANES))
            return carry

        lax.fori_loop(0, quarter // LANES, one, 0)

    def term(which, i, cut, at):
        block = (x_all if i < 2 else d_all)[:, :, :, at].reshape(2 * rows, LANES)
        return jnp.dot(
            act_t[which, (i + 1) % 3, cut, :], block, preferred_element_type=jnp.float32
        )

    CUTS = 2
    cuts = [pl.ds(n * (hidden // CUTS), hidden // CUTS) for n in range(CUTS)]
    term_copies = {}

    def send_term(i):
        for n, cut in enumerate(cuts):

            def make(at, cut=cut):
                term_out[i, cut, at] = term(1, i, cut, at).astype(short)

            by_columns(make)
            term_copies[i, n] = remote(
                term_out.at[i, cut], term_in.at[i, cut],
                term_send.at[CUTS * i + n], term_recv.at[CUTS * i + n], weight_mate,
            )

    def own_term(i):
        def make(at):
            term_own[i, :, at] = term(0, i, slice(None), at)

        by_columns(make)

    def finish(i):
        out = (grad_gate, grad_up, grad_down)[i]
        for n, cut in enumerate(cuts):
            term_copies[i, n].wait_recv()
            out[cut, :] = (term_own[i, cut, :] + wide(term_in[i, cut, :])).astype(short)

    def expert_dx(k, part_of, at):
        here = pl.ds(pl.multiple_of(part_of * half_rows, half_rows), half_rows)
        return sum(
            jnp.dot(
                act[k, which, i + 1, here, :], w_all[i, which, :, at],
                preferred_element_type=jnp.float32,
            )
            for which in range(2)
            for i in range(2)
        ).reshape(devices_ep // 2, capacity, LANES)

    dx_blocks = ends + mids + near + [flip(s, 0), s]
    dx_copies = []

    def send_dx(part_of, blocks):
        here = pl.ds(part_of * (devices_ep // 2), devices_ep // 2)

        def make(at):
            dx_out[here, :, at] = expert_dx(1, part_of, at).astype(short)

        by_columns(make)
        for n in blocks:
            block = dx_blocks[n]
            dx_copies.append(
                remote(
                    dx_out.at[block], dx_in.at[block], dx_send.at[n], dx_recv.at[n], row_mate
                )
            )

    def own_dx(part_of):
        here = pl.ds(part_of * (devices_ep // 2), devices_ep // 2)

        def make(at):
            dx_own[here, :, at] = expert_dx(0, part_of, at)

        by_columns(make)

    backs = []

    def give_back(n):
        block = dx_blocks[n]
        dx_copies[n].wait_recv()
        dx_sum[block] = (dx_own[block] + wide(dx_in[block])).astype(short)
        if n < devices_ep - 1:
            backs.append(
                remote(
                    dx_sum.at[block], owned(slot_rows, s), back_send.at[n], back_recv.at[s],
                    (r, block),
                )
            )
        else:
            backs.append(local(dx_sum.at[block], owned(slot_rows, s), self_sem.at[2]))

    for kind in range(2):
        pass_on(kind, None)
        for n in CORE:
            pass_on(kind, n)
    for n in (1, 2, 5, 6, 3, 4):
        pass_on(0, n)

    @pl.when(jnp.logical_not(at_end))
    def _():
        send(1, (3, 4, 5, 6))

    @pl.when(at_end)
    def _():
        send(1, (3, 4))

    for n in NEAR:
        pass_on(1, n)
    w_copies[0].wait_recv()
    project(0, 0)
    hand_over(0, 0)
    send_pair(0, 0)

    @pl.when(at_end)
    def _():
        send(1, (5,))

    for copy in passed[0]:
        copy.wait_recv()
    project(1, 0)
    hand_over(1, 0)
    w_copies[1].wait_recv()
    project(0, 1)
    hand_over(0, 1)
    send_pair(1, 0)
    project(1, 1)
    hand_over(1, 1)
    send_pair(0, 1)

    @pl.when(at_end)
    def _():
        send(1, (6,))

    send_pair(1, 1)
    for n in (3, 5, 4, 6):
        pass_on(1, n)
    w_copies[2].wait_recv()
    project(0, 2)
    hand_over(0, 2)
    make_hidden(0)
    make_hidden(1)
    send_pair(0, 2)
    for k in range(2):
        act_copies[k, 0].wait_recv()
    transpose(1, 0)
    for copy in passed[1]:
        copy.wait_recv()
    send_term(2)
    project(1, 2)
    hand_over(1, 2)
    transpose(0, 0)
    send_pair(1, 2)
    own_term(2)
    make_slopes(0)
    make_slopes(1)
    act_copies[0, 1].wait_recv()
    act_copies[1, 1].wait_recv()
    send_dx(1 - side, range(0, 4))
    send_dx(side, range(4, 8))
    transpose(1, 1)
    send_term(0)
    transpose(1, 2)
    send_term(1)
    own_dx(1 - side)
    for n in range(4):
        give_back(n)
    own_dx(side)
    finish(2)
    transpose(0, 1)
    own_term(0)
    transpose(0, 2)
    own_term(1)
    for n in range(4, 8):
        give_back(n)
    finish(0)
    backs[-1].wait()
    for origin in others:
        remote(
            dx_sum.at[0], owned(slot_rows, origin), back_send.at[0], back_recv.at[origin],
            (r, origin), start=False,
        ).wait_recv()

    def fill_in(at):
        in_grad[:, at] = jnp.dot(
            pick_t[...], slot_rows[:, at], preferred_element_type=jnp.float32
        ).astype(short)

    by_quarters(fill_in)
    finish(1)
    for kind in range(2):
        for n in range(devices_ep - 1):
            flow(kind, n).wait_send()
    sent = w_copies + passed[0] + passed[1] + list(give_copies.values())
    sent += list(pair_copies.values()) + list(act_copies.values())
    sent += list(term_copies.values()) + dx_copies + backs[:-1]
    for copy in sent:
        copy.wait_send()


def store_kernel(*refs):
    count = len(refs) // 2
    copies = [
        pltpu.make_async_copy(refs[i], refs[count + i], refs[-1].at[i]) for i in range(count)
    ]
    for copy in copies:
        copy.start()
    for copy in copies:
        copy.wait()


def fast_body(tokens, out_grad, route_weight, expert_ids, w_gate, w_up, w_down):
    devices_ep = lax.axis_size("ep")
    experts = devices_ep // GROUP
    token_count = tokens.shape[0]
    capacity = 6 * GROUP * token_count * TOP // (8 * devices_ep)
    quarter = D // GROUP
    hidden = w_gate.shape[0]
    rows = devices_ep * capacity
    slots = experts * capacity
    short = jnp.bfloat16
    vmem = pl.BlockSpec(memory_space=pltpu.VMEM)
    far = pl.BlockSpec(memory_space=pltpu.HBM)
    grad = jax.ShapeDtypeStruct(w_gate.shape, short)
    dma = pltpu.SemaphoreType.DMA
    results = pl.pallas_call(
        expert_kernel,
        out_shape=(jax.ShapeDtypeStruct(tokens.shape, short), grad, grad, grad),
        in_specs=[far] * 7,
        out_specs=(vmem, vmem, vmem, vmem),
        scratch_shapes=[
            pltpu.VMEM((1, token_count), jnp.int32),
            pltpu.VMEM((1, token_count), jnp.float32),
            pltpu.VMEM(tokens.shape, short),
            pltpu.VMEM(tokens.shape, short),
            pltpu.VMEM((slots, token_count), short),
            pltpu.VMEM((token_count, slots), short),
            pltpu.VMEM((slots, 1), jnp.float32),
            pltpu.VMEM((slots, D), short),
            pltpu.VMEM((slots, D), short),
            pltpu.VMEM((slots, D), short),
            pltpu.VMEM((2, devices_ep, capacity, quarter), short),
            pltpu.VMEM((2, devices_ep, capacity, quarter), short),
            pltpu.VMEM((3, 2, hidden, quarter), short),
            pltpu.VMEM((2, 2, 3, rows, hidden), short),
            pltpu.VMEM((2, 3, rows, hidden), short),
            pltpu.VMEM((2, 3, rows, hidden), short),
            pltpu.VMEM((2, 3, rows, hidden), short),
            pltpu.VMEM((2, 2, 3, rows, hidden), short),
            pltpu.VMEM((2, 3, hidden, 2 * rows), short),
            pltpu.VMEM((3, hidden, quarter), short),
            pltpu.VMEM((3, hidden, quarter), short),
            pltpu.VMEM((3, hidden, quarter), jnp.float32),
            pltpu.VMEM((devices_ep, capacity, quarter), short),
            pltpu.VMEM((devices_ep, capacity, quarter), short),
            pltpu.VMEM((devices_ep, capacity, quarter), jnp.float32),
            pltpu.VMEM((devices_ep, capacity, quarter), short),
        ]
        + [dma((4,))]
        + [dma((3,))] * 4
        + [dma((devices_ep,))] * 8
        + [dma((6,))] * 4
        + [dma((4,))] * 2
        + [dma((6,))] * 2
        + [dma((devices_ep,))] * 4,
        compiler_params=pltpu.CompilerParams(
            collective_id=0, has_side_effects=True, vmem_limit_bytes=52 * 2**20
        ),
    )(
        tokens, out_grad, route_weight.reshape(1, token_count),
        expert_ids.reshape(1, token_count), w_gate, w_up, w_down,
    )
    return tuple(
        pl.pallas_call(
            store_kernel,
            out_shape=tuple(jax.ShapeDtypeStruct(v.shape, v.dtype) for v in results),
            in_specs=[vmem] * len(results),
            out_specs=(far,) * len(results),
            scratch_shapes=[dma((len(results),))],
            compiler_params=pltpu.CompilerParams(vmem_limit_bytes=8 * 2**20),
        )(*results)
    )


def solution(mesh):
    devices_ep = mesh.shape["ep"]

    def step(*arrays):
        token_count = arrays[0].shape[0]
        capacity = 6 * GROUP * token_count * TOP // (8 * devices_ep)
        hidden = arrays[4].shape[0]
        fits = capacity % 48 == 0 and hidden % 128 == 0 and token_count % 128 == 0
        fits = fits and mesh.shape["dp"] == 4 and devices_ep == 2 * GROUP
        return (fast_body if fits else body)(*arrays)

    placed = (
        P(("dp", "ep"), None),
        P(("dp", "ep"), None),
        P(("dp", "ep"), None),
        P(("dp", "ep"), None),
        P("dp", "ep"),
        P("dp", "ep"),
        P("dp", "ep"),
    )
    return jax.shard_map(
        step,
        mesh=mesh,
        in_specs=placed,
        out_specs=(P(("dp", "ep"), None), P("dp", "ep"), P("dp", "ep"), P("dp", "ep")),
        check_vma=False,
    )
```

```python
import jax
import jax.numpy as jnp
from jax import lax
from jax.experimental import pallas as pl
from jax.experimental.pallas import tpu as pltpu
from jax.sharding import PartitionSpec as P

D = 7168
GROUP = 4
TOP = 1


CONTRACT_LAST = (((1,), (1,)), ((), ()))
CONTRACT_FIRST = (((0,), (0,)), ((), ()))


def as_sent(value):

    def short(part):
        return part.astype(jnp.bfloat16) if part.dtype == jnp.float32 else part

    return jax.tree.map(short, value)


def from_partner(value, axis, distance):
    mask = 2**distance
    pairs = [(source, source ^ mask) for source in range(lax.axis_size(axis))]
    return lax.ppermute(value, axis, pairs)


def slot_tables(expert_ids, route_weight, experts, capacity):
    token_count, top_count = expert_ids.shape
    pair_count = token_count * top_count
    flat_ids = expert_ids.reshape(pair_count)
    onehot = (flat_ids[:, None] == jnp.arange(experts, dtype=jnp.int32)[None, :]).astype(jnp.int32)
    before = jnp.cumsum(onehot, axis=0) - onehot
    ranks = jnp.sum(before * onehot, axis=1)
    kept = ranks < capacity
    slots = jnp.where(kept, flat_ids * capacity + ranks, 0)
    slot_ids = jnp.arange(experts * capacity, dtype=jnp.int32)
    match = (slots[None, :] == slot_ids[:, None]) & kept[None, :]
    pair_ids = jnp.arange(pair_count, dtype=jnp.int32)
    pair_of_slot = jnp.sum(jnp.where(match, pair_ids[None, :], 0), axis=1)
    filled = jnp.any(match, axis=1)
    flat_weight = route_weight.reshape(pair_count)
    weight_of_slot = jnp.sum(jnp.where(match, flat_weight[None, :], jnp.float32(0.0)), axis=1)
    return (kept, slots, pair_of_slot // top_count, filled, weight_of_slot)


def activations(gate, up, back):
    logistic = jax.nn.sigmoid(gate)
    silu = gate * logistic
    hidden = (silu * up).astype(jnp.bfloat16)
    d_gate = (back * up * logistic * (1.0 + gate * (1.0 - logistic))).astype(jnp.bfloat16)
    d_up = (back * silu).astype(jnp.bfloat16)
    return (hidden, d_gate, d_up)


def swap(value, axis, distance):
    return from_partner(value, axis, distance)


def wide(value):
    return value.astype(jnp.float32)


def dot_last(left, right):
    return lax.dot_general(left, right, CONTRACT_LAST, preferred_element_type=jnp.float32)


def dot_first(left, right):
    return lax.dot_general(left, right, CONTRACT_FIRST, preferred_element_type=jnp.float32)


def body(tokens, out_grad, route_weight, expert_ids, w_gate, w_up, w_down):
    devices_ep = lax.axis_size("ep")
    experts = devices_ep // GROUP
    token_count = tokens.shape[0]
    capacity = 6 * GROUP * token_count * TOP // (8 * devices_ep)
    quarter = D // GROUP
    short = jnp.bfloat16
    kept, slots, token_of_slot, filled, weight_of_slot = slot_tables(
        expert_ids, route_weight, experts, capacity
    )
    other_w = tuple(swap(w, "dp", 1) for w in (w_gate, w_up, w_down))
    token_ids = jnp.arange(token_count, dtype=jnp.int32)
    pick = ((token_of_slot[:, None] == token_ids[None, :]) & filled[:, None]).astype(short)
    x_slots = jnp.dot(pick, tokens, preferred_element_type=jnp.float32).astype(short)
    d_slots = (
        jnp.dot(pick, out_grad, preferred_element_type=jnp.float32) * weight_of_slot[:, None]
    ).astype(short)

    def to_owners(rows):
        shaped = rows.reshape(experts, capacity, GROUP, quarter).transpose(0, 2, 1, 3)
        return shaped.reshape(devices_ep, capacity, quarter)

    def sent(rows):
        return lax.all_to_all(to_owners(rows), "ep", split_axis=0, concat_axis=0, tiled=True)

    row_count = devices_ep * capacity
    x_own = sent(x_slots).reshape(row_count, quarter)
    d_own = sent(d_slots).reshape(row_count, quarter)
    x_other, d_other = swap(x_own, "dp", 0), swap(d_own, "dp", 0)
    core = lax.axis_index("ep") % 2
    weights = ((w_gate, w_up, w_down), other_w)
    acts = []
    for x_rows, d_rows in ((x_own, d_own), (x_other, d_other)):
        terms = [
            jnp.concatenate(
                [dot_last(x_rows, wg), dot_last(x_rows, wu), dot_last(d_rows, wd)], axis=1
            ).astype(short)
            for wg, wu, wd in weights
        ]
        give = jnp.where(core == 0, terms[1], terms[0])
        keep = jnp.where(core == 0, terms[0], terms[1])
        pair = (wide(keep) + wide(swap(give, "ep", 0))).astype(short)
        total = wide(pair) + wide(swap(pair, "ep", 1))
        width = total.shape[1] // 3
        mine = jnp.concatenate(
            activations(total[:, :width], total[:, width : 2 * width], total[:, 2 * width :]), axis=1
        )
        theirs = swap(mine, "ep", 0)
        first = jnp.where(core == 0, mine, theirs)
        second = jnp.where(core == 0, theirs, mine)
        acts.append(
            tuple(
                tuple(half[:, piece * width : (piece + 1) * width] for piece in range(3))
                for half in (first, second)
            )
        )

    def grads(half):
        (h0, g0, u0), (h1, g1, u1) = acts[0][half], acts[1][half]
        return (
            dot_first(g0, x_own) + dot_first(g1, x_other),
            dot_first(u0, x_own) + dot_first(u1, x_other),
            dot_first(h0, d_own) + dot_first(h1, d_other),
        )

    def dx(rows):
        return sum(
            jnp.dot(acts[rows][half][1], weights[half][0], preferred_element_type=jnp.float32)
            + jnp.dot(acts[rows][half][2], weights[half][1], preferred_element_type=jnp.float32)
            for half in range(2)
        )

    dx_in = swap(dx(1).astype(short), "dp", 0)
    away = tuple(swap(term.astype(short), "dp", 1) for term in grads(1))
    expert_dx = (dx(0) + wide(dx_in)).astype(short)
    grad_gate, grad_up, grad_down = (
        (own + wide(term)).astype(short) for own, term in zip(grads(0), away)
    )
    returned = lax.all_to_all(
        expert_dx.reshape(devices_ep, capacity, quarter),
        "ep",
        split_axis=0,
        concat_axis=0,
        tiled=True,
    )
    slot_rows = (
        returned.reshape(experts, GROUP, capacity, quarter)
        .transpose(0, 2, 1, 3)
        .reshape(experts * capacity, D)
    )
    in_grad = dot_first(pick, slot_rows).astype(short)
    return (in_grad, grad_gate, grad_up, grad_down)

MESH = pl.DeviceIdType.MESH


def flip(index, bit):
    size = 1 << bit
    return index + size - 2 * size * lax.rem(lax.div(index, size), 2)


def expert_kernel(
    tokens, out_grad, route, ids, wg, wu, wd, in_0, in_1, in_2, in_3, grad_gate, grad_up, grad_down,
    named, paid, tok, ogr, pick, pick_t, scale, xs, ds, slot_rows, x_all, d_all, w_all, part, got, pair, across,
    act, act_t, term_out, term_in, term_own, dx_out, dx_in, dx_own, dx_sum,
    in_sem, tok_sem, w_local, w_send, w_recv, self_sem, x_send, x_recv, d_send, d_recv,
    fx_send, fx_recv, fd_send, fd_recv, give_send, give_recv, pair_send, pair_recv,
    act_send, act_recv, term_send, term_recv, dx_send, dx_recv, back_send, back_recv,
):
    devices_ep, capacity, quarter = dx_sum.shape
    rows = devices_ep * capacity
    half_rows = rows // 2
    hidden = wg.shape[0]
    slots, token_count = pick.shape
    experts = slots // capacity
    short = jnp.bfloat16
    r, s = lax.axis_index("dp"), lax.axis_index("ep")
    core, z = lax.rem(s, 2), lax.div(s, 2)
    side = lax.div(z, 2)
    end = 1 - lax.rem(z + side, 2)
    at_end = end == 1
    row_mate, weight_mate = (flip(r, 0), s), (flip(r, 1), s)
    core_mate, chip_mate = (r, flip(s, 0)), (r, flip(s, 1))
    far_mid, far_end = 2 * (2 - side), 2 * (3 - 3 * side)
    near = [flip(s, 1), flip(flip(s, 1), 0)]
    mids = [far_mid + core, far_mid + 1 - core]
    ends = [far_end + core, far_end + 1 - core]
    others = [flip(s, 0)] + near + ends + mids
    CORE, NEAR, FAR = [0], [1, 2], [3, 4, 5, 6]

    def local(source, target, sem):
        copy = pltpu.make_async_copy(source, target, sem)
        copy.start()
        return copy

    small = [local(ids, named, in_sem.at[2]), local(route, paid, in_sem.at[3])]
    order = (5, 6, 3, 4)
    columns = [
        pl.ds(pl.multiple_of(lax.rem(others[n], GROUP) * quarter, 128), quarter) for n in order
    ]
    tok_copies = [
        local(tokens.at[:, at], tok.at[:, at], tok_sem.at[n]) for n, at in enumerate(columns)
    ]
    own_w = [local(wg, w_all.at[0, 0], w_local.at[0])]

    barrier = pltpu.get_barrier_semaphore()
    peers = [row_mate, weight_mate] + [(r, other) for other in others]
    for peer in peers:
        pl.semaphore_signal(barrier, inc=1, device_id=peer, device_id_type=MESH)

    for copy in small:
        copy.wait()
    name = named[...]
    wide_rows = max(8, experts)
    expert_row = lax.broadcasted_iota(jnp.int32, (wide_rows, token_count), 0)
    onehot = jnp.where(expert_row == name, 1.0, 0.0)
    earlier = lax.broadcasted_iota(jnp.int32, (token_count, token_count), 0) < (
        lax.broadcasted_iota(jnp.int32, (token_count, token_count), 1)
    )
    before = jnp.dot(
        onehot.astype(short), jnp.where(earlier, 1.0, 0.0).astype(short),
        preferred_element_type=jnp.float32,
    )
    rank = jnp.sum(before * onehot, axis=0, keepdims=True)
    slot = jnp.where(rank < capacity, name.astype(jnp.float32) * capacity + rank, -1.0)
    slot_row = lax.broadcasted_iota(jnp.int32, (slots, token_count), 0).astype(jnp.float32)
    match = jnp.where(slot_row == slot, 1.0, 0.0)
    pick[...] = match.astype(short)
    scale[...] = jnp.sum(match * paid[...], axis=1, keepdims=True)
    pick_t[...] = match.T.astype(short)

    def by_quarters(fn):
        def one(n, carry):
            fn(pl.ds(pl.multiple_of(n * quarter, quarter), quarter))
            return carry

        lax.fori_loop(0, GROUP, one, 0)

    def fill_x(at):
        xs[:, at] = jnp.dot(
            pick[...], tok[:, at], preferred_element_type=jnp.float32
        ).astype(short)

    def fill_d(at):
        ds[:, at] = (
            jnp.dot(pick[...], ogr[:, at], preferred_element_type=jnp.float32) * scale[...]
        ).astype(short)

    tok_copies[0].wait()
    ogr_copy = local(out_grad, ogr, in_sem.at[1])
    own_w += [local(w, w_all.at[i, 0], w_local.at[i]) for i, w in ((1, wu), (2, wd))]

    def remote(source, target, send, recv, peer, start=True):
        copy = pltpu.make_async_remote_copy(
            src_ref=source, dst_ref=target, send_sem=send, recv_sem=recv,
            device_id=peer, device_id_type=MESH,
        )
        if start:
            copy.start()
        return copy

    def owned(ref, device, part=slice(None)):
        first, size = (0, capacity) if part == slice(None) else part
        row = pl.multiple_of(lax.div(device, GROUP) * capacity, 16) + first
        column = pl.multiple_of(lax.rem(device, GROUP) * quarter, 128)
        return ref.at[pl.ds(pl.multiple_of(row, 16), size), pl.ds(column, quarter)]

    w_copies = []

    def send_weight(i):
        if i:
            own_w[i].wait()
        w_copies.append(
            remote(w_all.at[i, 0], w_all.at[i, 1], w_send.at[0], w_recv.at[i], weight_mate)
        )

    LAST = 16
    WHOLE = ((0, capacity),)
    SPLIT = ((0, capacity - LAST), (capacity - LAST, LAST))
    kinds = ((xs, x_all, x_send, x_recv), (ds, d_all, d_send, d_recv))

    def parts_of(kind, n):
        return SPLIT if kind and n is not None and n in FAR else WHOLE

    def flow(kind, n, piece):
        source, target, send, recv = kinds[kind]
        peer = others[n]
        part = parts_of(kind, n)[piece]
        return remote(
            owned(source, peer, part), target.at[0, s, pl.ds(*part)], send.at[0],
            recv.at[piece, s], (r, peer), start=False,
        )

    def send(kind, which):
        for n in which:
            for piece in range(len(parts_of(kind, n))):
                flow(kind, n, piece).start()

    self_copies = []

    fill_x(columns[0])
    own_w[0].wait()
    pl.semaphore_wait(barrier, len(peers))
    send_weight(0)
    for n, peer in enumerate(order):
        if n:
            tok_copies[n].wait()
            fill_x(columns[n])

        @pl.when(jnp.logical_not(at_end))
        def _(peer=peer):
            send(0, (peer,))

    send(0, CORE + NEAR)
    self_copies.append(local(owned(xs, s), x_all.at[0, s], self_sem.at[0]))
    ogr_copy.wait()
    by_quarters(fill_d)
    send_weight(1)
    send_weight(2)
    send(1, CORE + NEAR)
    self_copies.append(local(owned(ds, s), d_all.at[0, s], self_sem.at[1]))

    @pl.when(at_end)
    def _():
        send(0, FAR)

    def landed(ref, sem):
        pltpu.make_async_copy(ref, ref, sem.at[0]).wait()


    def pass_on(kind, n, at_middle=None):
        _, target, _, recv = kinds[kind]
        origin = s if n is None else others[n]
        if at_middle is not None:
            origin = end * origin + (1 - end) * others[at_middle]
        to_send, to_recv = ((fx_send, fx_recv), (fd_send, fd_recv))[kind]
        if n is None:
            self_copies[kind].wait()
        for piece, part in enumerate(parts_of(kind, n)):
            here = target.at[0, origin, pl.ds(*part)]
            if n is not None:
                remote(
                    here, here, x_send.at[0], recv.at[piece, origin], (r, origin), start=False
                ).wait_recv()
            remote(
                here, target.at[1, origin, pl.ds(*part)], to_send.at[0], to_recv.at[0], row_mate
            )

    def project(k, i):
        block = (x_all if i < 2 else d_all)[k].reshape(rows, quarter)
        both = dot_last(block, w_all[i].reshape(2 * hidden, quarter)).astype(short)
        for which in range(2):
            part[k, which, i] = both[:, which * hidden : (which + 1) * hidden]

    STEP = 48

    def by_rows(fn):
        def one(n, carry):
            fn(pl.ds(pl.multiple_of(n * STEP, STEP), STEP))
            return carry

        lax.fori_loop(0, rows // STEP, one, 0)

    give_copies, pair_copies, act_copies = {}, {}, {}

    def hand_over(k, i):
        give_copies[k, i] = remote(
            part.at[k, 1 - core, i], got.at[k, i],
            give_send.at[0], give_recv.at[3 * k + i], core_mate,
        )

    def send_pair(k, i):
        give_copies[k, i].wait_recv()

        def add_pair(at):
            pair[k, i, at, :] = (wide(part[k, core, i, at, :]) + wide(got[k, i, at, :])).astype(
                short
            )

        by_rows(add_pair)
        pair_copies[k, i] = remote(
            pair.at[k, i], across.at[k, i],
            pair_send.at[0], pair_recv.at[3 * k + i], chip_mate,
        )

    def total(k, i, at):
        return wide(pair[k, i, at, :]) + wide(across[k, i, at, :])

    def make_hidden(k):
        for i in range(2):
            pair_copies[k, i].wait_recv()

        def one(at):
            gate, up = total(k, 0, at), total(k, 1, at)
            act[k, core, 0, at, :] = (gate * jax.nn.sigmoid(gate) * up).astype(short)

        by_rows(one)
        act_copies[k, 0] = remote(
            act.at[k, core, 0], act.at[k, core, 0],
            act_send.at[0], act_recv.at[2 * k], core_mate,
        )

    def make_slopes(k):
        pair_copies[k, 2].wait_recv()

        def one(at):
            made = activations(total(k, 0, at), total(k, 1, at), total(k, 2, at))
            act[k, core, 1, at, :] = made[1]
            act[k, core, 2, at, :] = made[2]

        by_rows(one)
        act_copies[k, 1] = remote(
            act.at[k, core, pl.ds(1, 2)], act.at[k, core, pl.ds(1, 2)],
            act_send.at[0], act_recv.at[2 * k + 1], core_mate,
        )

    def transpose(which, piece):
        for k in range(2):
            act_t[which, piece, :, k * rows : (k + 1) * rows] = act[k, which, piece].T

    LANES = 896

    def by_columns(fn):
        def one(n, carry):
            fn(pl.ds(pl.multiple_of(n * LANES, LANES), LANES))
            return carry

        lax.fori_loop(0, quarter // LANES, one, 0)

    def term(which, i, cut, at):
        block = (x_all if i < 2 else d_all)[:, :, :, at].reshape(2 * rows, LANES)
        return jnp.dot(
            act_t[which, (i + 1) % 3, cut, :], block, preferred_element_type=jnp.float32
        )

    CUTS = 2
    FIRST = hidden // 4
    cuts = [pl.ds(0, FIRST), pl.ds(FIRST, hidden - FIRST)]
    term_copies = {}

    def send_term(i):
        for n, cut in enumerate(cuts):

            def make(at, cut=cut):
                term_out[i, cut, at] = term(1, i, cut, at).astype(short)

            by_columns(make)
            term_copies[i, n] = remote(
                term_out.at[i, cut], term_in.at[i, cut],
                term_send.at[0], term_recv.at[CUTS * i + n], weight_mate,
            )

    def own_term(i):
        def make(at):
            term_own[i, :, at] = term(0, i, slice(None), at)

        by_columns(make)

    def finish(i):
        out = (grad_gate, grad_up, grad_down)[i]
        for n, cut in enumerate(cuts):
            term_copies[i, n].wait_recv()
            out[cut, :] = (term_own[i, cut, :] + wide(term_in[i, cut, :])).astype(short)

    def expert_dx(k, part_of, at):
        here = pl.ds(pl.multiple_of(part_of * half_rows, half_rows), half_rows)
        return sum(
            jnp.dot(
                act[k, which, i + 1, here, :], w_all[i, which, :, at],
                preferred_element_type=jnp.float32,
            )
            for which in range(2)
            for i in range(2)
        ).reshape(devices_ep // 2, capacity, LANES)

    dx_blocks = ends + mids + near + [flip(s, 0), s]
    dx_copies = []

    def send_dx(part_of, blocks):
        here = pl.ds(part_of * (devices_ep // 2), devices_ep // 2)

        def make(at):
            dx_out[here, :, at] = expert_dx(1, part_of, at).astype(short)

        by_columns(make)
        for n in blocks:
            block = dx_blocks[n]
            dx_copies.append(
                remote(
                    dx_out.at[block], dx_in.at[block], dx_send.at[0], dx_recv.at[n], row_mate
                )
            )

    def own_dx(part_of):
        here = pl.ds(part_of * (devices_ep // 2), devices_ep // 2)

        def make(at):
            dx_own[here, :, at] = expert_dx(0, part_of, at)

        by_columns(make)

    backs = []

    def give_back(n):
        block = dx_blocks[n]
        dx_copies[n].wait_recv()
        dx_sum[block] = (dx_own[block] + wide(dx_in[block])).astype(short)
        if n < devices_ep - 1:
            backs.append(
                remote(
                    dx_sum.at[block], owned(slot_rows, s), back_send.at[0], back_recv.at[0],
                    (r, block),
                )
            )
        else:
            backs.append(local(dx_sum.at[block], owned(slot_rows, s), self_sem.at[2]))

    for kind in range(2):
        pass_on(kind, None)
        for n in CORE:
            pass_on(kind, n)
    pass_on(0, 1)
    pass_on(0, 2)
    pass_on(0, 5)
    pass_on(0, 6)
    pass_on(0, 3)
    pass_on(0, 4)

    @pl.when(jnp.logical_not(at_end))
    def _():
        send(1, (3, 4, 5, 6))

    @pl.when(at_end)
    def _():
        send(1, (3, 5))

    for n in NEAR:
        pass_on(1, n)
    w_copies[0].wait_recv()
    project(0, 0)
    hand_over(0, 0)
    send_pair(0, 0)

    @pl.when(at_end)
    def _():
        send(1, (6,))

    landed(x_all.at[1], fx_recv)
    project(1, 0)
    hand_over(1, 0)
    w_copies[1].wait_recv()
    project(0, 1)
    hand_over(0, 1)
    send_pair(1, 0)
    project(1, 1)
    hand_over(1, 1)
    send_pair(0, 1)

    @pl.when(at_end)
    def _():
        send(1, (4,))

    send_pair(1, 1)
    pass_on(1, 3)
    pass_on(1, 5, 4)
    pass_on(1, 6, 5)
    pass_on(1, 4, 6)
    make_hidden(0)
    w_copies[2].wait_recv()
    project(0, 2)
    hand_over(0, 2)
    make_hidden(1)
    send_pair(0, 2)
    for k in range(2):
        act_copies[k, 0].wait_recv()
    transpose(1, 0)
    landed(d_all.at[1], fd_recv)
    send_term(2)
    project(1, 2)
    hand_over(1, 2)
    transpose(0, 0)
    send_pair(1, 2)
    own_term(2)
    make_slopes(0)
    make_slopes(1)
    act_copies[0, 1].wait_recv()
    act_copies[1, 1].wait_recv()
    send_dx(1 - side, range(0, 4))
    send_dx(side, range(4, 8))
    transpose(1, 1)
    send_term(0)
    transpose(1, 2)
    send_term(1)
    own_dx(1 - side)
    for n in range(4):
        give_back(n)
    own_dx(side)
    finish(2)
    transpose(0, 1)
    own_term(0)
    transpose(0, 2)
    own_term(1)
    for n in range(4, 8):
        give_back(n)
    finish(0)
    backs[-1].wait()
    landed(dx_sum.at[pl.ds(0, devices_ep - 1)], back_recv)

    for n, out in enumerate((in_0, in_1, in_2, in_3)):
        out[...] = jnp.dot(
            pick_t[...], slot_rows[:, n * quarter : (n + 1) * quarter],
            preferred_element_type=jnp.float32,
        ).astype(short)
    finish(1)
    most = pl.ds(0, devices_ep - 1)
    for sem in (x_send, d_send, back_send):
        landed(dx_sum.at[most], sem)
    for sem in (fx_send, fd_send, dx_send):
        landed(dx_sum, sem)
    for sem in (give_send, pair_send, act_send):
        landed(got, sem)
    for sem in (w_send, term_send):
        landed(term_in, sem)


def store_kernel(*refs):
    grads = refs[GROUP : GROUP + 3]
    whole, outs, sem = refs[GROUP + 3], refs[GROUP + 4 : GROUP + 7], refs[-1]
    quarter = whole.shape[1] // GROUP
    stores = [
        pltpu.make_async_copy(part, whole.at[:, pl.ds(n * quarter, quarter)], sem.at[n])
        for n, part in enumerate(refs[:GROUP])
    ]
    stores += [
        pltpu.make_async_copy(grad, out, sem.at[GROUP + n])
        for n, (grad, out) in enumerate(zip(grads, outs))
    ]
    for store in stores:
        store.start()
    for store in stores:
        store.wait()


def fast_body(tokens, out_grad, route_weight, expert_ids, w_gate, w_up, w_down):
    devices_ep = lax.axis_size("ep")
    experts = devices_ep // GROUP
    token_count = tokens.shape[0]
    capacity = 6 * GROUP * token_count * TOP // (8 * devices_ep)
    quarter = D // GROUP
    hidden = w_gate.shape[0]
    rows = devices_ep * capacity
    slots = experts * capacity
    short = jnp.bfloat16
    vmem = pl.BlockSpec(memory_space=pltpu.VMEM)
    far = pl.BlockSpec(memory_space=pltpu.HBM)
    grad = jax.ShapeDtypeStruct(w_gate.shape, short)
    dma = pltpu.SemaphoreType.DMA
    results = pl.pallas_call(
        expert_kernel,
        out_shape=(jax.ShapeDtypeStruct((token_count, quarter), short),) * GROUP + (grad,) * 3,
        in_specs=[far] * 7,
        out_specs=(vmem,) * (GROUP + 3),
        scratch_shapes=[
            pltpu.VMEM((1, token_count), jnp.int32),
            pltpu.VMEM((1, token_count), jnp.float32),
            pltpu.VMEM(tokens.shape, short),
            pltpu.VMEM(tokens.shape, short),
            pltpu.VMEM((slots, token_count), short),
            pltpu.VMEM((token_count, slots), short),
            pltpu.VMEM((slots, 1), jnp.float32),
            pltpu.VMEM((slots, D), short),
            pltpu.VMEM((slots, D), short),
            pltpu.VMEM((slots, D), short),
            pltpu.VMEM((2, devices_ep, capacity, quarter), short),
            pltpu.VMEM((2, devices_ep, capacity, quarter), short),
            pltpu.VMEM((3, 2, hidden, quarter), short),
            pltpu.VMEM((2, 2, 3, rows, hidden), short),
            pltpu.VMEM((2, 3, rows, hidden), short),
            pltpu.VMEM((2, 3, rows, hidden), short),
            pltpu.VMEM((2, 3, rows, hidden), short),
            pltpu.VMEM((2, 2, 3, rows, hidden), short),
            pltpu.VMEM((2, 3, hidden, 2 * rows), short),
            pltpu.VMEM((3, hidden, quarter), short),
            pltpu.VMEM((3, hidden, quarter), short),
            pltpu.VMEM((3, hidden, quarter), jnp.float32),
            pltpu.VMEM((devices_ep, capacity, quarter), short),
            pltpu.VMEM((devices_ep, capacity, quarter), short),
            pltpu.VMEM((devices_ep, capacity, quarter), jnp.float32),
            pltpu.VMEM((devices_ep, capacity, quarter), short),
        ]
        + [dma((4,)), dma((GROUP,)), dma((3,)), dma((1,)), dma((3,)), dma((3,))]
        + [dma((1,)), dma((1, devices_ep)), dma((1,)), dma((2, devices_ep))]
        + [dma((1,))] * 4
        + [dma((1,)), dma((6,))] * 2
        + [dma((1,)), dma((4,)), dma((1,)), dma((6,)), dma((1,)), dma((devices_ep,))]
        + [dma((1,))] * 2,
        compiler_params=pltpu.CompilerParams(
            collective_id=0, has_side_effects=True, vmem_limit_bytes=51904512
        ),
    )(
        tokens, out_grad, route_weight.reshape(1, token_count),
        expert_ids.reshape(1, token_count), w_gate, w_up, w_down,
    )
    return tuple(
        pl.pallas_call(
            store_kernel,
            out_shape=(jax.ShapeDtypeStruct(tokens.shape, short), grad, grad, grad),
            in_specs=[vmem] * len(results),
            out_specs=(far,) * 4,
            scratch_shapes=[dma((len(results),))],
            compiler_params=pltpu.CompilerParams(vmem_limit_bytes=40 * 2**20),
        )(*results)
    )


def solution(mesh):
    devices_ep = mesh.shape["ep"]

    def step(*arrays):
        token_count = arrays[0].shape[0]
        capacity = 6 * GROUP * token_count * TOP // (8 * devices_ep)
        hidden = arrays[4].shape[0]
        fits = capacity % 48 == 0 and hidden % 128 == 0 and token_count % 128 == 0
        fits = fits and mesh.shape["dp"] == 4 and devices_ep == 2 * GROUP
        return (fast_body if fits else body)(*arrays)

    placed = (
        P(("dp", "ep"), None),
        P(("dp", "ep"), None),
        P(("dp", "ep"), None),
        P(("dp", "ep"), None),
        P("dp", "ep"),
        P("dp", "ep"),
        P("dp", "ep"),
    )
    return jax.shard_map(
        step,
        mesh=mesh,
        in_specs=placed,
        out_specs=(P(("dp", "ep"), None), P("dp", "ep"), P("dp", "ep"), P("dp", "ep")),
        check_vma=False,
    )
```

```python
import jax
import jax.numpy as jnp
from jax import lax
from jax.experimental import pallas as pl
from jax.experimental.pallas import tpu as pltpu
from jax.sharding import PartitionSpec as P

D = 7168
GROUP = 4
TOP = 1


CONTRACT_LAST = (((1,), (1,)), ((), ()))
CONTRACT_FIRST = (((0,), (0,)), ((), ()))


def as_sent(value):

    def short(part):
        return part.astype(jnp.bfloat16) if part.dtype == jnp.float32 else part

    return jax.tree.map(short, value)


def from_partner(value, axis, distance):
    mask = 2**distance
    pairs = [(source, source ^ mask) for source in range(lax.axis_size(axis))]
    return lax.ppermute(value, axis, pairs)


def slot_tables(expert_ids, route_weight, experts, capacity):
    token_count, top_count = expert_ids.shape
    pair_count = token_count * top_count
    flat_ids = expert_ids.reshape(pair_count)
    onehot = (flat_ids[:, None] == jnp.arange(experts, dtype=jnp.int32)[None, :]).astype(jnp.int32)
    before = jnp.cumsum(onehot, axis=0) - onehot
    ranks = jnp.sum(before * onehot, axis=1)
    kept = ranks < capacity
    slots = jnp.where(kept, flat_ids * capacity + ranks, 0)
    slot_ids = jnp.arange(experts * capacity, dtype=jnp.int32)
    match = (slots[None, :] == slot_ids[:, None]) & kept[None, :]
    pair_ids = jnp.arange(pair_count, dtype=jnp.int32)
    pair_of_slot = jnp.sum(jnp.where(match, pair_ids[None, :], 0), axis=1)
    filled = jnp.any(match, axis=1)
    flat_weight = route_weight.reshape(pair_count)
    weight_of_slot = jnp.sum(jnp.where(match, flat_weight[None, :], jnp.float32(0.0)), axis=1)
    return (kept, slots, pair_of_slot // top_count, filled, weight_of_slot)


def activations(gate, up, back):
    logistic = jax.nn.sigmoid(gate)
    silu = gate * logistic
    hidden = (silu * up).astype(jnp.bfloat16)
    d_gate = (back * up * logistic * (1.0 + gate * (1.0 - logistic))).astype(jnp.bfloat16)
    d_up = (back * silu).astype(jnp.bfloat16)
    return (hidden, d_gate, d_up)


def swap(value, axis, distance):
    return from_partner(value, axis, distance)


def wide(value):
    return value.astype(jnp.float32)


def dot_last(left, right):
    return lax.dot_general(left, right, CONTRACT_LAST, preferred_element_type=jnp.float32)


def dot_first(left, right):
    return lax.dot_general(left, right, CONTRACT_FIRST, preferred_element_type=jnp.float32)


def body(tokens, out_grad, route_weight, expert_ids, w_gate, w_up, w_down):
    devices_ep = lax.axis_size("ep")
    experts = devices_ep // GROUP
    token_count = tokens.shape[0]
    capacity = 6 * GROUP * token_count * TOP // (8 * devices_ep)
    quarter = D // GROUP
    short = jnp.bfloat16
    kept, slots, token_of_slot, filled, weight_of_slot = slot_tables(
        expert_ids, route_weight, experts, capacity
    )
    other_w = tuple(swap(w, "dp", 1) for w in (w_gate, w_up, w_down))
    token_ids = jnp.arange(token_count, dtype=jnp.int32)
    pick = ((token_of_slot[:, None] == token_ids[None, :]) & filled[:, None]).astype(short)
    x_slots = jnp.dot(pick, tokens, preferred_element_type=jnp.float32).astype(short)
    d_slots = (
        jnp.dot(pick, out_grad, preferred_element_type=jnp.float32) * weight_of_slot[:, None]
    ).astype(short)

    def to_owners(rows):
        shaped = rows.reshape(experts, capacity, GROUP, quarter).transpose(0, 2, 1, 3)
        return shaped.reshape(devices_ep, capacity, quarter)

    def sent(rows):
        return lax.all_to_all(to_owners(rows), "ep", split_axis=0, concat_axis=0, tiled=True)

    row_count = devices_ep * capacity
    x_own = sent(x_slots).reshape(row_count, quarter)
    d_own = sent(d_slots).reshape(row_count, quarter)
    x_other, d_other = swap(x_own, "dp", 0), swap(d_own, "dp", 0)
    core = lax.axis_index("ep") % 2
    weights = ((w_gate, w_up, w_down), other_w)
    acts = []
    for x_rows, d_rows in ((x_own, d_own), (x_other, d_other)):
        terms = [
            jnp.concatenate(
                [dot_last(x_rows, wg), dot_last(x_rows, wu), dot_last(d_rows, wd)], axis=1
            ).astype(short)
            for wg, wu, wd in weights
        ]
        give = jnp.where(core == 0, terms[1], terms[0])
        keep = jnp.where(core == 0, terms[0], terms[1])
        pair = (wide(keep) + wide(swap(give, "ep", 0))).astype(short)
        total = wide(pair) + wide(swap(pair, "ep", 1))
        width = total.shape[1] // 3
        mine = jnp.concatenate(
            activations(total[:, :width], total[:, width : 2 * width], total[:, 2 * width :]), axis=1
        )
        theirs = swap(mine, "ep", 0)
        first = jnp.where(core == 0, mine, theirs)
        second = jnp.where(core == 0, theirs, mine)
        acts.append(
            tuple(
                tuple(half[:, piece * width : (piece + 1) * width] for piece in range(3))
                for half in (first, second)
            )
        )

    def grads(half):
        (h0, g0, u0), (h1, g1, u1) = acts[0][half], acts[1][half]
        return (
            dot_first(g0, x_own) + dot_first(g1, x_other),
            dot_first(u0, x_own) + dot_first(u1, x_other),
            dot_first(h0, d_own) + dot_first(h1, d_other),
        )

    def dx(rows):
        return sum(
            jnp.dot(acts[rows][half][1], weights[half][0], preferred_element_type=jnp.float32)
            + jnp.dot(acts[rows][half][2], weights[half][1], preferred_element_type=jnp.float32)
            for half in range(2)
        )

    dx_in = swap(dx(1).astype(short), "dp", 0)
    away = tuple(swap(term.astype(short), "dp", 1) for term in grads(1))
    expert_dx = (dx(0) + wide(dx_in)).astype(short)
    grad_gate, grad_up, grad_down = (
        (own + wide(term)).astype(short) for own, term in zip(grads(0), away)
    )
    returned = lax.all_to_all(
        expert_dx.reshape(devices_ep, capacity, quarter),
        "ep",
        split_axis=0,
        concat_axis=0,
        tiled=True,
    )
    slot_rows = (
        returned.reshape(experts, GROUP, capacity, quarter)
        .transpose(0, 2, 1, 3)
        .reshape(experts * capacity, D)
    )
    in_grad = dot_first(pick, slot_rows).astype(short)
    return (in_grad, grad_gate, grad_up, grad_down)

MESH = pl.DeviceIdType.MESH


def flip(index, bit):
    size = 1 << bit
    return index + size - 2 * size * lax.rem(lax.div(index, size), 2)


def expert_kernel(
    tokens, out_grad, route, ids, wg, wu, wd, in_0, in_1, in_2, in_3, grad_gate, grad_up, grad_down,
    named, paid, tok, ogr, pick, pick_t, scale, xs, ds, slot_rows, x_all, d_all, w_all, part, got, pair, across,
    act, act_t, term_out, term_in, term_own, dx_out, dx_in, dx_own, dx_sum,
    in_sem, tok_sem, w_local, w_send, w_recv, self_sem, x_send, x_recv, d_send, d_recv,
    fx_send, fx_recv, fd_send, fd_recv, give_send, give_recv, pair_send, pair_recv,
    act_send, act_recv, term_send, term_recv, dx_send, dx_recv, back_send, back_recv,
):
    devices_ep, capacity, quarter = dx_sum.shape
    rows = devices_ep * capacity
    half_rows = rows // 2
    hidden = wg.shape[0]
    slots, token_count = pick.shape
    experts = slots // capacity
    short = jnp.bfloat16
    r, s = lax.axis_index("dp"), lax.axis_index("ep")
    core, z = lax.rem(s, 2), lax.div(s, 2)
    side = lax.div(z, 2)
    end = 1 - lax.rem(z + side, 2)
    at_end = end == 1
    row_mate, weight_mate = (flip(r, 0), s), (flip(r, 1), s)
    core_mate, chip_mate = (r, flip(s, 0)), (r, flip(s, 1))
    far_mid, far_end = 2 * (2 - side), 2 * (3 - 3 * side)
    near = [flip(s, 1), flip(flip(s, 1), 0)]
    mids = [far_mid + core, far_mid + 1 - core]
    ends = [far_end + core, far_end + 1 - core]
    others = [flip(s, 0)] + near + ends + mids
    CORE, NEAR, FAR = [0], [1, 2], [3, 4, 5, 6]

    def local(source, target, sem):
        copy = pltpu.make_async_copy(source, target, sem)
        copy.start()
        return copy

    small = [local(ids, named, in_sem.at[2]), local(route, paid, in_sem.at[3])]
    order = (5, 6, 3, 4)
    columns = [
        pl.ds(pl.multiple_of(lax.rem(others[n], GROUP) * quarter, 128), quarter) for n in order
    ]
    tok_copies = [
        local(tokens.at[:, at], tok.at[:, at], tok_sem.at[n]) for n, at in enumerate(columns)
    ]
    own_w = [local(wg, w_all.at[0, 0], w_local.at[0])]

    barrier = pltpu.get_barrier_semaphore()
    peers = [row_mate, weight_mate] + [(r, other) for other in others]
    for peer in peers:
        pl.semaphore_signal(barrier, inc=1, device_id=peer, device_id_type=MESH)

    for copy in small:
        copy.wait()
    name = named[...]
    wide_rows = max(8, experts)
    expert_row = lax.broadcasted_iota(jnp.int32, (wide_rows, token_count), 0)
    onehot = jnp.where(expert_row == name, 1.0, 0.0)
    earlier = lax.broadcasted_iota(jnp.int32, (token_count, token_count), 0) < (
        lax.broadcasted_iota(jnp.int32, (token_count, token_count), 1)
    )
    before = jnp.dot(
        onehot.astype(short), jnp.where(earlier, 1.0, 0.0).astype(short),
        preferred_element_type=jnp.float32,
    )
    rank = jnp.sum(before * onehot, axis=0, keepdims=True)
    slot = jnp.where(rank < capacity, name.astype(jnp.float32) * capacity + rank, -1.0)
    slot_row = lax.broadcasted_iota(jnp.int32, (slots, token_count), 0).astype(jnp.float32)
    match = jnp.where(slot_row == slot, 1.0, 0.0)
    pick[...] = match.astype(short)
    scale[...] = jnp.sum(match * paid[...], axis=1, keepdims=True)
    pick_t[...] = match.T.astype(short)

    def by_quarters(fn):
        def one(n, carry):
            fn(pl.ds(pl.multiple_of(n * quarter, quarter), quarter))
            return carry

        lax.fori_loop(0, GROUP, one, 0)

    def fill_x(at):
        xs[:, at] = jnp.dot(
            pick[...], tok[:, at], preferred_element_type=jnp.float32
        ).astype(short)

    def fill_d(at):
        ds[:, at] = (
            jnp.dot(pick[...], ogr[:, at], preferred_element_type=jnp.float32) * scale[...]
        ).astype(short)

    tok_copies[0].wait()
    ogr_copy = local(out_grad, ogr, in_sem.at[1])
    own_w += [local(w, w_all.at[i, 0], w_local.at[i]) for i, w in ((1, wu), (2, wd))]

    def remote(source, target, send, recv, peer, start=True):
        copy = pltpu.make_async_remote_copy(
            src_ref=source, dst_ref=target, send_sem=send, recv_sem=recv,
            device_id=peer, device_id_type=MESH,
        )
        if start:
            copy.start()
        return copy

    def owned(ref, device, part=slice(None)):
        first, size = (0, capacity) if part == slice(None) else part
        row = pl.multiple_of(lax.div(device, GROUP) * capacity, 16) + first
        column = pl.multiple_of(lax.rem(device, GROUP) * quarter, 128)
        return ref.at[pl.ds(pl.multiple_of(row, 16), size), pl.ds(column, quarter)]

    w_copies = []

    def send_weight(i):
        if i:
            own_w[i].wait()
        w_copies.append(
            remote(w_all.at[i, 0], w_all.at[i, 1], w_send.at[0], w_recv.at[i], weight_mate)
        )

    SLICE = 16
    WHOLE = ((0, capacity),)
    SPLIT = tuple((first, SLICE) for first in range(0, capacity, SLICE))
    kinds = ((xs, x_all, x_send, x_recv), (ds, d_all, d_send, d_recv))

    def parts_of(kind, n):
        return SPLIT if kind and n is not None and n in FAR else WHOLE

    def flow(kind, n, piece):
        source, target, send, recv = kinds[kind]
        peer = others[n]
        part = parts_of(kind, n)[piece]
        return remote(
            owned(source, peer, part), target.at[0, s, pl.ds(*part)], send.at[0],
            recv.at[piece, s], (r, peer), start=False,
        )

    def send(kind, which):
        for n in which:
            for piece in range(len(parts_of(kind, n))):
                flow(kind, n, piece).start()

    self_copies = []

    fill_x(columns[0])
    own_w[0].wait()
    pl.semaphore_wait(barrier, len(peers))
    send_weight(0)
    for n, peer in enumerate(order):
        if n:
            tok_copies[n].wait()
            fill_x(columns[n])

        @pl.when(jnp.logical_not(at_end))
        def _(peer=peer):
            send(0, (peer,))

    send(0, CORE + NEAR)
    self_copies.append(local(owned(xs, s), x_all.at[0, s], self_sem.at[0]))
    ogr_copy.wait()
    by_quarters(fill_d)
    send_weight(1)
    send_weight(2)
    send(1, CORE + NEAR)
    self_copies.append(local(owned(ds, s), d_all.at[0, s], self_sem.at[1]))

    @pl.when(at_end)
    def _():
        send(0, FAR)

    def landed(ref, sem):
        pltpu.make_async_copy(ref, ref, sem.at[0]).wait()


    def pass_on(kind, n, at_middle=None):
        _, target, _, recv = kinds[kind]
        origin = s if n is None else others[n]
        if at_middle is not None:
            origin = end * origin + (1 - end) * others[at_middle]
        to_send, to_recv = ((fx_send, fx_recv), (fd_send, fd_recv))[kind]
        if n is None:
            self_copies[kind].wait()
        for piece, part in enumerate(parts_of(kind, n)):
            here = target.at[0, origin, pl.ds(*part)]
            if n is not None:
                remote(
                    here, here, x_send.at[0], recv.at[piece, origin], (r, origin), start=False
                ).wait_recv()
            remote(
                here, target.at[1, origin, pl.ds(*part)], to_send.at[0], to_recv.at[0], row_mate
            )

    def project(k, i):
        block = (x_all if i < 2 else d_all)[k].reshape(rows, quarter)
        both = dot_last(block, w_all[i].reshape(2 * hidden, quarter)).astype(short)
        for which in range(2):
            part[k, which, i] = both[:, which * hidden : (which + 1) * hidden]

    STEP = 48

    def by_rows(fn):
        def one(n, carry):
            fn(pl.ds(pl.multiple_of(n * STEP, STEP), STEP))
            return carry

        lax.fori_loop(0, rows // STEP, one, 0)

    give_copies, pair_copies, act_copies = {}, {}, {}

    def hand_over(k, i):
        give_copies[k, i] = remote(
            part.at[k, 1 - core, i], got.at[k, i],
            give_send.at[0], give_recv.at[3 * k + i], core_mate,
        )

    def send_pair(k, i):
        give_copies[k, i].wait_recv()

        def add_pair(at):
            pair[k, i, at, :] = (wide(part[k, core, i, at, :]) + wide(got[k, i, at, :])).astype(
                short
            )

        by_rows(add_pair)
        pair_copies[k, i] = remote(
            pair.at[k, i], across.at[k, i],
            pair_send.at[0], pair_recv.at[3 * k + i], chip_mate,
        )

    def total(k, i, at):
        return wide(pair[k, i, at, :]) + wide(across[k, i, at, :])

    def make_hidden(k):
        for i in range(2):
            pair_copies[k, i].wait_recv()

        def one(at):
            gate, up = total(k, 0, at), total(k, 1, at)
            act[k, core, 0, at, :] = (gate * jax.nn.sigmoid(gate) * up).astype(short)

        by_rows(one)
        act_copies[k, 0] = remote(
            act.at[k, core, 0], act.at[k, core, 0],
            act_send.at[0], act_recv.at[2 * k], core_mate,
        )

    def make_slopes(k):
        pair_copies[k, 2].wait_recv()

        def one(at):
            made = activations(total(k, 0, at), total(k, 1, at), total(k, 2, at))
            act[k, core, 1, at, :] = made[1]
            act[k, core, 2, at, :] = made[2]

        by_rows(one)
        act_copies[k, 1] = remote(
            act.at[k, core, pl.ds(1, 2)], act.at[k, core, pl.ds(1, 2)],
            act_send.at[0], act_recv.at[2 * k + 1], core_mate,
        )

    def transpose(which, piece):
        for k in range(2):
            act_t[which, piece, :, k * rows : (k + 1) * rows] = act[k, which, piece].T

    LANES = 896

    def by_columns(fn):
        def one(n, carry):
            fn(pl.ds(pl.multiple_of(n * LANES, LANES), LANES))
            return carry

        lax.fori_loop(0, quarter // LANES, one, 0)

    def term(which, i, cut, at):
        block = (x_all if i < 2 else d_all)[:, :, :, at].reshape(2 * rows, LANES)
        return jnp.dot(
            act_t[which, (i + 1) % 3, cut, :], block, preferred_element_type=jnp.float32
        )

    CUTS = 2
    FIRST = hidden // 4
    cuts = [pl.ds(0, FIRST), pl.ds(FIRST, hidden - FIRST)]
    term_copies = {}

    def send_term(i):
        for n, cut in enumerate(cuts):

            def make(at, cut=cut):
                term_out[i, cut, at] = term(1, i, cut, at).astype(short)

            by_columns(make)
            term_copies[i, n] = remote(
                term_out.at[i, cut], term_in.at[i, cut],
                term_send.at[0], term_recv.at[CUTS * i + n], weight_mate,
            )

    def own_term(i):
        def make(at):
            term_own[i, :, at] = term(0, i, slice(None), at)

        by_columns(make)

    def finish(i):
        out = (grad_gate, grad_up, grad_down)[i]
        for n, cut in enumerate(cuts):
            term_copies[i, n].wait_recv()
            out[cut, :] = (term_own[i, cut, :] + wide(term_in[i, cut, :])).astype(short)

    def expert_dx(k, part_of, at):
        here = pl.ds(pl.multiple_of(part_of * half_rows, half_rows), half_rows)
        return sum(
            jnp.dot(
                act[k, which, i + 1, here, :], w_all[i, which, :, at],
                preferred_element_type=jnp.float32,
            )
            for which in range(2)
            for i in range(2)
        ).reshape(devices_ep // 2, capacity, LANES)

    dx_blocks = ends + mids + near + [flip(s, 0), s]
    dx_copies = []

    def send_dx(part_of, blocks):
        here = pl.ds(part_of * (devices_ep // 2), devices_ep // 2)

        def make(at):
            dx_out[here, :, at] = expert_dx(1, part_of, at).astype(short)

        by_columns(make)
        for n in blocks:
            block = dx_blocks[n]
            dx_copies.append(
                remote(
                    dx_out.at[block], dx_in.at[block], dx_send.at[0], dx_recv.at[n], row_mate
                )
            )

    def own_dx(part_of):
        here = pl.ds(part_of * (devices_ep // 2), devices_ep // 2)

        def make(at):
            dx_own[here, :, at] = expert_dx(0, part_of, at)

        by_columns(make)

    backs = []

    def give_back(n):
        block = dx_blocks[n]
        dx_copies[n].wait_recv()
        dx_sum[block] = (dx_own[block] + wide(dx_in[block])).astype(short)
        if n < devices_ep - 1:
            backs.append(
                remote(
                    dx_sum.at[block], owned(slot_rows, s), back_send.at[0], back_recv.at[0],
                    (r, block),
                )
            )
        else:
            backs.append(local(dx_sum.at[block], owned(slot_rows, s), self_sem.at[2]))

    pass_on(0, None)
    pass_on(0, 0)
    pass_on(0, 1)
    pass_on(1, None)
    pass_on(0, 2)
    pass_on(0, 5)
    pass_on(0, 6)
    pass_on(0, 3)
    pass_on(0, 4)

    @pl.when(jnp.logical_not(at_end))
    def _():
        send(1, (3, 4, 5, 6))

    @pl.when(at_end)
    def _():
        send(1, (3, 5))

    for n in CORE + NEAR:
        pass_on(1, n)
    w_copies[0].wait_recv()
    project(0, 0)
    hand_over(0, 0)
    send_pair(0, 0)

    @pl.when(at_end)
    def _():
        send(1, (6,))

    landed(x_all.at[1], fx_recv)
    project(1, 0)
    hand_over(1, 0)
    send_pair(1, 0)
    w_copies[1].wait_recv()
    project(0, 1)
    hand_over(0, 1)
    project(1, 1)
    hand_over(1, 1)
    send_pair(0, 1)

    @pl.when(at_end)
    def _():
        send(1, (4,))

    send_pair(1, 1)
    pass_on(1, 3)
    pass_on(1, 5, 4)
    pass_on(1, 6, 5)
    pass_on(1, 4, 6)
    make_hidden(0)
    w_copies[2].wait_recv()
    project(0, 2)
    hand_over(0, 2)
    make_hidden(1)
    send_pair(0, 2)
    for k in range(2):
        act_copies[k, 0].wait_recv()
    transpose(1, 0)
    landed(d_all.at[1], fd_recv)
    send_term(2)
    project(1, 2)
    hand_over(1, 2)
    transpose(0, 0)
    send_pair(1, 2)
    own_term(2)
    make_slopes(0)
    make_slopes(1)
    act_copies[0, 1].wait_recv()
    act_copies[1, 1].wait_recv()
    send_dx(1 - side, range(0, 4))
    send_dx(side, range(4, 8))
    transpose(1, 1)
    send_term(0)
    transpose(1, 2)
    send_term(1)
    own_dx(1 - side)
    for n in range(4):
        give_back(n)
    own_dx(side)
    finish(2)
    transpose(0, 1)
    own_term(0)
    transpose(0, 2)
    own_term(1)
    for n in range(4, 8):
        give_back(n)
    finish(0)
    backs[-1].wait()
    landed(dx_sum.at[pl.ds(0, devices_ep - 1)], back_recv)

    for n, out in enumerate((in_0, in_1, in_2, in_3)):
        out[...] = jnp.dot(
            pick_t[...], slot_rows[:, n * quarter : (n + 1) * quarter],
            preferred_element_type=jnp.float32,
        ).astype(short)
    finish(1)
    most = pl.ds(0, devices_ep - 1)
    for sem in (x_send, d_send, back_send):
        landed(dx_sum.at[most], sem)
    for sem in (fx_send, fd_send, dx_send):
        landed(dx_sum, sem)
    for sem in (give_send, pair_send, act_send):
        landed(got, sem)
    for sem in (w_send, term_send):
        landed(term_in, sem)


def store_kernel(*refs):
    grads = refs[GROUP : GROUP + 3]
    whole, outs, sem = refs[GROUP + 3], refs[GROUP + 4 : GROUP + 7], refs[-1]
    quarter = whole.shape[1] // GROUP
    stores = [
        pltpu.make_async_copy(part, whole.at[:, pl.ds(n * quarter, quarter)], sem.at[n])
        for n, part in enumerate(refs[:GROUP])
    ]
    stores += [
        pltpu.make_async_copy(grad, out, sem.at[GROUP + n])
        for n, (grad, out) in enumerate(zip(grads, outs))
    ]
    for store in stores:
        store.start()
    for store in stores:
        store.wait()


def fast_body(tokens, out_grad, route_weight, expert_ids, w_gate, w_up, w_down):
    devices_ep = lax.axis_size("ep")
    experts = devices_ep // GROUP
    token_count = tokens.shape[0]
    capacity = 6 * GROUP * token_count * TOP // (8 * devices_ep)
    quarter = D // GROUP
    hidden = w_gate.shape[0]
    rows = devices_ep * capacity
    slots = experts * capacity
    short = jnp.bfloat16
    vmem = pl.BlockSpec(memory_space=pltpu.VMEM)
    far = pl.BlockSpec(memory_space=pltpu.HBM)
    grad = jax.ShapeDtypeStruct(w_gate.shape, short)
    dma = pltpu.SemaphoreType.DMA
    results = pl.pallas_call(
        expert_kernel,
        out_shape=(jax.ShapeDtypeStruct((token_count, quarter), short),) * GROUP + (grad,) * 3,
        in_specs=[far] * 7,
        out_specs=(vmem,) * (GROUP + 3),
        scratch_shapes=[
            pltpu.VMEM((1, token_count), jnp.int32),
            pltpu.VMEM((1, token_count), jnp.float32),
            pltpu.VMEM(tokens.shape, short),
            pltpu.VMEM(tokens.shape, short),
            pltpu.VMEM((slots, token_count), short),
            pltpu.VMEM((token_count, slots), short),
            pltpu.VMEM((slots, 1), jnp.float32),
            pltpu.VMEM((slots, D), short),
            pltpu.VMEM((slots, D), short),
            pltpu.VMEM((slots, D), short),
            pltpu.VMEM((2, devices_ep, capacity, quarter), short),
            pltpu.VMEM((2, devices_ep, capacity, quarter), short),
            pltpu.VMEM((3, 2, hidden, quarter), short),
            pltpu.VMEM((2, 2, 3, rows, hidden), short),
            pltpu.VMEM((2, 3, rows, hidden), short),
            pltpu.VMEM((2, 3, rows, hidden), short),
            pltpu.VMEM((2, 3, rows, hidden), short),
            pltpu.VMEM((2, 2, 3, rows, hidden), short),
            pltpu.VMEM((2, 3, hidden, 2 * rows), short),
            pltpu.VMEM((3, hidden, quarter), short),
            pltpu.VMEM((3, hidden, quarter), short),
            pltpu.VMEM((3, hidden, quarter), jnp.float32),
            pltpu.VMEM((devices_ep, capacity, quarter), short),
            pltpu.VMEM((devices_ep, capacity, quarter), short),
            pltpu.VMEM((devices_ep, capacity, quarter), jnp.float32),
            pltpu.VMEM((devices_ep, capacity, quarter), short),
        ]
        + [dma((4,)), dma((GROUP,)), dma((3,)), dma((1,)), dma((3,)), dma((3,))]
        + [dma((1,)), dma((1, devices_ep)), dma((1,)), dma((capacity // 16, devices_ep))]
        + [dma((1,))] * 4
        + [dma((1,)), dma((6,))] * 2
        + [dma((1,)), dma((4,)), dma((1,)), dma((6,)), dma((1,)), dma((devices_ep,))]
        + [dma((1,))] * 2,
        compiler_params=pltpu.CompilerParams(
            collective_id=0, has_side_effects=True, vmem_limit_bytes=48 * 2**20
        ),
    )(
        *(
            pltpu.with_memory_space_constraint(value, pltpu.HBM)
            for value in (
                tokens, out_grad, route_weight.reshape(1, token_count),
                expert_ids.reshape(1, token_count), w_gate, w_up, w_down,
            )
        )
    )
    return tuple(
        pl.pallas_call(
            store_kernel,
            out_shape=(jax.ShapeDtypeStruct(tokens.shape, short), grad, grad, grad),
            in_specs=[vmem] * len(results),
            out_specs=(far,) * 4,
            scratch_shapes=[dma((len(results),))],
            compiler_params=pltpu.CompilerParams(vmem_limit_bytes=40 * 2**20),
        )(*results)
    )


def solution(mesh):
    devices_ep = mesh.shape["ep"]

    def step(*arrays):
        token_count = arrays[0].shape[0]
        capacity = 6 * GROUP * token_count * TOP // (8 * devices_ep)
        hidden = arrays[4].shape[0]
        fits = capacity % 48 == 0 and hidden % 128 == 0 and token_count % 128 == 0
        fits = fits and mesh.shape["dp"] == 4 and devices_ep == 2 * GROUP
        return (fast_body if fits else body)(*arrays)

    placed = (
        P(("dp", "ep"), None),
        P(("dp", "ep"), None),
        P(("dp", "ep"), None),
        P(("dp", "ep"), None),
        P("dp", "ep"),
        P("dp", "ep"),
        P("dp", "ep"),
    )
    return jax.shard_map(
        step,
        mesh=mesh,
        in_specs=placed,
        out_specs=(P(("dp", "ep"), None), P("dp", "ep"), P("dp", "ep"), P("dp", "ep")),
        check_vma=False,
    )
```

```python
import jax
import jax.numpy as jnp
from jax import lax
from jax.experimental import pallas as pl
from jax.experimental.pallas import tpu as pltpu
from jax.sharding import PartitionSpec as P

D = 7168
GROUP = 4
TOP = 1


CONTRACT_LAST = (((1,), (1,)), ((), ()))
CONTRACT_FIRST = (((0,), (0,)), ((), ()))


def as_sent(value):

    def short(part):
        return part.astype(jnp.bfloat16) if part.dtype == jnp.float32 else part

    return jax.tree.map(short, value)


def from_partner(value, axis, distance):
    mask = 2**distance
    pairs = [(source, source ^ mask) for source in range(lax.axis_size(axis))]
    return lax.ppermute(value, axis, pairs)


def slot_tables(expert_ids, route_weight, experts, capacity):
    token_count, top_count = expert_ids.shape
    pair_count = token_count * top_count
    flat_ids = expert_ids.reshape(pair_count)
    onehot = (flat_ids[:, None] == jnp.arange(experts, dtype=jnp.int32)[None, :]).astype(jnp.int32)
    before = jnp.cumsum(onehot, axis=0) - onehot
    ranks = jnp.sum(before * onehot, axis=1)
    kept = ranks < capacity
    slots = jnp.where(kept, flat_ids * capacity + ranks, 0)
    slot_ids = jnp.arange(experts * capacity, dtype=jnp.int32)
    match = (slots[None, :] == slot_ids[:, None]) & kept[None, :]
    pair_ids = jnp.arange(pair_count, dtype=jnp.int32)
    pair_of_slot = jnp.sum(jnp.where(match, pair_ids[None, :], 0), axis=1)
    filled = jnp.any(match, axis=1)
    flat_weight = route_weight.reshape(pair_count)
    weight_of_slot = jnp.sum(jnp.where(match, flat_weight[None, :], jnp.float32(0.0)), axis=1)
    return (kept, slots, pair_of_slot // top_count, filled, weight_of_slot)


def activations(gate, up, back):
    logistic = jax.nn.sigmoid(gate)
    silu = gate * logistic
    hidden = (silu * up).astype(jnp.bfloat16)
    d_gate = (back * up * logistic * (1.0 + gate * (1.0 - logistic))).astype(jnp.bfloat16)
    d_up = (back * silu).astype(jnp.bfloat16)
    return (hidden, d_gate, d_up)


def swap(value, axis, distance):
    return from_partner(value, axis, distance)


def wide(value):
    return value.astype(jnp.float32)


def dot_last(left, right):
    return lax.dot_general(left, right, CONTRACT_LAST, preferred_element_type=jnp.float32)


def dot_first(left, right):
    return lax.dot_general(left, right, CONTRACT_FIRST, preferred_element_type=jnp.float32)


def body(tokens, out_grad, route_weight, expert_ids, w_gate, w_up, w_down):
    devices_ep = lax.axis_size("ep")
    experts = devices_ep // GROUP
    token_count = tokens.shape[0]
    capacity = 6 * GROUP * token_count * TOP // (8 * devices_ep)
    quarter = D // GROUP
    short = jnp.bfloat16
    kept, slots, token_of_slot, filled, weight_of_slot = slot_tables(
        expert_ids, route_weight, experts, capacity
    )
    other_w = tuple(swap(w, "dp", 1) for w in (w_gate, w_up, w_down))
    token_ids = jnp.arange(token_count, dtype=jnp.int32)
    pick = ((token_of_slot[:, None] == token_ids[None, :]) & filled[:, None]).astype(short)
    x_slots = jnp.dot(pick, tokens, preferred_element_type=jnp.float32).astype(short)
    d_slots = (
        jnp.dot(pick, out_grad, preferred_element_type=jnp.float32) * weight_of_slot[:, None]
    ).astype(short)

    def to_owners(rows):
        shaped = rows.reshape(experts, capacity, GROUP, quarter).transpose(0, 2, 1, 3)
        return shaped.reshape(devices_ep, capacity, quarter)

    def sent(rows):
        return lax.all_to_all(to_owners(rows), "ep", split_axis=0, concat_axis=0, tiled=True)

    row_count = devices_ep * capacity
    x_own = sent(x_slots).reshape(row_count, quarter)
    d_own = sent(d_slots).reshape(row_count, quarter)
    x_other, d_other = swap(x_own, "dp", 0), swap(d_own, "dp", 0)
    core = lax.axis_index("ep") % 2
    weights = ((w_gate, w_up, w_down), other_w)
    acts = []
    for x_rows, d_rows in ((x_own, d_own), (x_other, d_other)):
        terms = [
            jnp.concatenate(
                [dot_last(x_rows, wg), dot_last(x_rows, wu), dot_last(d_rows, wd)], axis=1
            ).astype(short)
            for wg, wu, wd in weights
        ]
        give = jnp.where(core == 0, terms[1], terms[0])
        keep = jnp.where(core == 0, terms[0], terms[1])
        pair = (wide(keep) + wide(swap(give, "ep", 0))).astype(short)
        total = wide(pair) + wide(swap(pair, "ep", 1))
        width = total.shape[1] // 3
        mine = jnp.concatenate(
            activations(total[:, :width], total[:, width : 2 * width], total[:, 2 * width :]), axis=1
        )
        theirs = swap(mine, "ep", 0)
        first = jnp.where(core == 0, mine, theirs)
        second = jnp.where(core == 0, theirs, mine)
        acts.append(
            tuple(
                tuple(half[:, piece * width : (piece + 1) * width] for piece in range(3))
                for half in (first, second)
            )
        )

    def grads(half):
        (h0, g0, u0), (h1, g1, u1) = acts[0][half], acts[1][half]
        return (
            dot_first(g0, x_own) + dot_first(g1, x_other),
            dot_first(u0, x_own) + dot_first(u1, x_other),
            dot_first(h0, d_own) + dot_first(h1, d_other),
        )

    def dx(rows):
        return sum(
            jnp.dot(acts[rows][half][1], weights[half][0], preferred_element_type=jnp.float32)
            + jnp.dot(acts[rows][half][2], weights[half][1], preferred_element_type=jnp.float32)
            for half in range(2)
        )

    dx_in = swap(dx(1).astype(short), "dp", 0)
    away = tuple(swap(term.astype(short), "dp", 1) for term in grads(1))
    expert_dx = (dx(0) + wide(dx_in)).astype(short)
    grad_gate, grad_up, grad_down = (
        (own + wide(term)).astype(short) for own, term in zip(grads(0), away)
    )
    returned = lax.all_to_all(
        expert_dx.reshape(devices_ep, capacity, quarter),
        "ep",
        split_axis=0,
        concat_axis=0,
        tiled=True,
    )
    slot_rows = (
        returned.reshape(experts, GROUP, capacity, quarter)
        .transpose(0, 2, 1, 3)
        .reshape(experts * capacity, D)
    )
    in_grad = dot_first(pick, slot_rows).astype(short)
    return (in_grad, grad_gate, grad_up, grad_down)

MESH = pl.DeviceIdType.MESH


def flip(index, bit):
    size = 1 << bit
    return index + size - 2 * size * lax.rem(lax.div(index, size), 2)


def expert_kernel(
    tokens, out_grad, route, ids, wg, wu, wd, in_0, in_1, in_2, in_3, grad_gate, grad_up, grad_down,
    named, paid, tok, ogr, pick, pick_t, scale, xs, ds, slot_rows, x_all, d_all, w_all, part, got, pair, across,
    act, act_t, term_out, term_in, term_own, dx_out, dx_in, dx_own, dx_sum,
    in_sem, tok_sem, w_local, w_send, w_recv, self_sem, x_send, x_recv, d_send, d_recv,
    fx_send, fx_recv, fd_send, fd_recv, give_send, give_recv, pair_send, pair_recv,
    act_send, act_recv, term_send, term_recv, dx_send, dx_recv, back_send, back_recv,
):
    devices_ep, capacity, quarter = dx_sum.shape
    rows = devices_ep * capacity
    half_rows = rows // 2
    hidden = wg.shape[0]
    slots, token_count = pick.shape
    experts = slots // capacity
    short = jnp.bfloat16
    r, s = lax.axis_index("dp"), lax.axis_index("ep")
    core, z = lax.rem(s, 2), lax.div(s, 2)
    side = lax.div(z, 2)
    end = 1 - lax.rem(z + side, 2)
    at_end = end == 1
    row_mate, weight_mate = (flip(r, 0), s), (flip(r, 1), s)
    core_mate, chip_mate = (r, flip(s, 0)), (r, flip(s, 1))
    far_mid, far_end = 2 * (2 - side), 2 * (3 - 3 * side)
    near = [flip(s, 1), flip(flip(s, 1), 0)]
    mids = [far_mid + core, far_mid + 1 - core]
    ends = [far_end + core, far_end + 1 - core]
    others = [flip(s, 0)] + near + ends + mids
    CORE, NEAR, FAR = [0], [1, 2], [3, 4, 5, 6]

    def local(source, target, sem):
        copy = pltpu.make_async_copy(source, target, sem)
        copy.start()
        return copy

    small = [local(ids, named, in_sem.at[2]), local(route, paid, in_sem.at[3])]
    order = (5, 6, 3, 4)
    columns = [
        pl.ds(pl.multiple_of(lax.rem(others[n], GROUP) * quarter, 128), quarter) for n in order
    ]
    tok_copies = [
        local(tokens.at[:, at], tok.at[:, at], tok_sem.at[n]) for n, at in enumerate(columns)
    ]
    small_half = hidden // 2

    def load_weight(i, w):
        for half in range(2):
            local(
                w.at[pl.ds(half * small_half, small_half)], w_all.at[i, half, 0], w_local.at[i]
            )

    load_weight(0, wg)

    barrier = pltpu.get_barrier_semaphore()
    peers = [row_mate, weight_mate] + [(r, other) for other in others]
    for peer in peers:
        pl.semaphore_signal(barrier, inc=1, device_id=peer, device_id_type=MESH)

    for copy in small:
        copy.wait()
    name = named[...]
    wide_rows = max(8, experts)
    expert_row = lax.broadcasted_iota(jnp.int32, (wide_rows, token_count), 0)
    onehot = jnp.where(expert_row == name, 1.0, 0.0)
    earlier = lax.broadcasted_iota(jnp.int32, (token_count, token_count), 0) < (
        lax.broadcasted_iota(jnp.int32, (token_count, token_count), 1)
    )
    before = jnp.dot(
        onehot.astype(short), jnp.where(earlier, 1.0, 0.0).astype(short),
        preferred_element_type=jnp.float32,
    )
    rank = jnp.sum(before * onehot, axis=0, keepdims=True)
    slot = jnp.where(rank < capacity, name.astype(jnp.float32) * capacity + rank, -1.0)
    slot_row = lax.broadcasted_iota(jnp.int32, (slots, token_count), 0).astype(jnp.float32)
    match = jnp.where(slot_row == slot, 1.0, 0.0)
    pick[...] = match.astype(short)
    scale[...] = jnp.sum(match * paid[...], axis=1, keepdims=True)
    pick_t[...] = match.T.astype(short)

    def by_quarters(fn):
        def one(n, carry):
            fn(pl.ds(pl.multiple_of(n * quarter, quarter), quarter))
            return carry

        lax.fori_loop(0, GROUP, one, 0)

    def fill_x(at):
        xs[:, at] = jnp.dot(
            pick[...], tok[:, at], preferred_element_type=jnp.float32
        ).astype(short)

    def fill_d(at):
        ds[:, at] = (
            jnp.dot(pick[...], ogr[:, at], preferred_element_type=jnp.float32) * scale[...]
        ).astype(short)

    tok_copies[0].wait()
    ogr_copy = local(out_grad, ogr, in_sem.at[1])
    load_weight(1, wu)
    load_weight(2, wd)

    def remote(source, target, send, recv, peer, start=True):
        copy = pltpu.make_async_remote_copy(
            src_ref=source, dst_ref=target, send_sem=send, recv_sem=recv,
            device_id=peer, device_id_type=MESH,
        )
        if start:
            copy.start()
        return copy

    def owned(ref, device, part=slice(None)):
        first, size = (0, capacity) if part == slice(None) else part
        row = pl.multiple_of(lax.div(device, GROUP) * capacity, 16) + first
        column = pl.multiple_of(lax.rem(device, GROUP) * quarter, 128)
        return ref.at[pl.ds(pl.multiple_of(row, 16), size), pl.ds(column, quarter)]

    def landed(ref, sem):
        pltpu.make_async_copy(ref, ref, sem.at[0]).wait()

    w_copies = []

    def send_weight(i):
        if i:
            landed(w_all.at[i, :, 0], w_local.at[pl.ds(i, 1)])
        w_copies.append(
            remote(w_all.at[i, :, 0], w_all.at[i, :, 1], w_send.at[0], w_recv.at[i], weight_mate)
        )

    SLICE = 16
    WHOLE = ((0, capacity),)
    SPLIT = tuple((first, SLICE) for first in range(0, capacity, SLICE))
    kinds = ((xs, x_all, x_send, x_recv), (ds, d_all, d_send, d_recv))

    def parts_of(kind, n):
        return SPLIT if kind and n is not None and n in FAR else WHOLE

    def flow(kind, n, piece):
        source, target, send, recv = kinds[kind]
        peer = others[n]
        part = parts_of(kind, n)[piece]
        return remote(
            owned(source, peer, part), target.at[0, s, pl.ds(*part)], send.at[0],
            recv.at[piece, s], (r, peer), start=False,
        )

    def send(kind, which):
        for n in which:
            for piece in range(len(parts_of(kind, n))):
                flow(kind, n, piece).start()

    self_copies = []

    fill_x(columns[0])
    landed(w_all.at[0, :, 0], w_local)
    pl.semaphore_wait(barrier, len(peers))
    send_weight(0)
    for n, peer in enumerate(order):
        if n:
            tok_copies[n].wait()
            fill_x(columns[n])

        @pl.when(jnp.logical_not(at_end))
        def _(peer=peer):
            send(0, (peer,))

    send(0, CORE + NEAR)
    self_copies.append(local(owned(xs, s), x_all.at[0, s], self_sem.at[0]))
    ogr_copy.wait()
    by_quarters(fill_d)
    send_weight(1)
    send_weight(2)
    send(1, CORE + NEAR)
    self_copies.append(local(owned(ds, s), d_all.at[0, s], self_sem.at[1]))

    @pl.when(at_end)
    def _():
        send(0, FAR)


    def pass_on(kind, n, at_middle=None):
        _, target, _, recv = kinds[kind]
        origin = s if n is None else others[n]
        if at_middle is not None:
            origin = end * origin + (1 - end) * others[at_middle]
        to_send, to_recv = ((fx_send, fx_recv), (fd_send, fd_recv))[kind]
        if n is None:
            self_copies[kind].wait()
        for piece, part in enumerate(parts_of(kind, n)):
            here = target.at[0, origin, pl.ds(*part)]
            if n is not None:
                remote(
                    here, here, x_send.at[0], recv.at[piece, origin], (r, origin), start=False
                ).wait_recv()
            remote(
                here, target.at[1, origin, pl.ds(*part)], to_send.at[0], to_recv.at[0], row_mate
            )

    def project(k, i):
        block = (x_all if i < 2 else d_all)[k].reshape(rows, quarter)
        both = dot_last(block, w_all[i].reshape(2 * hidden, quarter)).astype(short)
        for half in range(2):
            part[k, half, i] = both[:, half * hidden : (half + 1) * hidden]

    STEP = 48

    def by_rows(fn):
        def one(n, carry):
            fn(pl.ds(pl.multiple_of(n * STEP, STEP), STEP))
            return carry

        lax.fori_loop(0, rows // STEP, one, 0)

    give_copies, pair_copies, act_copies = {}, {}, {}

    def hand_over(k, i):
        give_copies[k, i] = remote(
            part.at[k, 1 - core, i], got.at[k, i],
            give_send.at[0], give_recv.at[3 * k + i], core_mate,
        )

    def send_pair(k, i):
        give_copies[k, i].wait_recv()

        def add_pair(at):
            pair[k, i, at, :] = (wide(part[k, core, i, at, :]) + wide(got[k, i, at, :])).astype(
                short
            )

        by_rows(add_pair)
        pair_copies[k, i] = remote(
            pair.at[k, i], across.at[k, i],
            pair_send.at[0], pair_recv.at[3 * k + i], chip_mate,
        )

    def total(k, i, at):
        return wide(pair[k, i, at, :]) + wide(across[k, i, at, :])

    def make_hidden(k):
        for i in range(2):
            pair_copies[k, i].wait_recv()

        def one(at):
            gate, up = total(k, 0, at), total(k, 1, at)
            act[k, core, 0, at, :] = (gate * jax.nn.sigmoid(gate) * up).astype(short)

        by_rows(one)
        act_copies[k, 0] = remote(
            act.at[k, core, 0], act.at[k, core, 0],
            act_send.at[0], act_recv.at[2 * k], core_mate,
        )

    def take_hidden():
        for k in range(2):
            act_copies[k, 0].wait_recv()

    def make_slopes(k):
        pair_copies[k, 2].wait_recv()

        def one(at):
            made = activations(total(k, 0, at), total(k, 1, at), total(k, 2, at))
            act[k, core, 1, at, :] = made[1]
            act[k, core, 2, at, :] = made[2]

        by_rows(one)
        act_copies[k, 1] = remote(
            act.at[k, core, pl.ds(1, 2)], act.at[k, core, pl.ds(1, 2)],
            act_send.at[0], act_recv.at[2 * k + 1], core_mate,
        )

    def transpose(half, piece):
        for k in range(2):
            act_t[half, piece, :, k * rows : (k + 1) * rows] = act[k, half, piece].T

    LANES = 896

    def by_columns(fn):
        def one(n, carry):
            fn(pl.ds(pl.multiple_of(n * LANES, LANES), LANES))
            return carry

        lax.fori_loop(0, quarter // LANES, one, 0)

    def term(which, i, half, at, first=0, size=small_half):
        block = (x_all if i < 2 else d_all)[:, :, :, at].reshape(2 * rows, LANES)
        units = pl.ds(which * small_half + first, size)
        return jnp.dot(
            act_t[half, (i + 1) % 3, units, :], block, preferred_element_type=jnp.float32
        )

    FIRST = small_half // 2
    spans = [(core, 0, FIRST), (core, FIRST, small_half - FIRST), (1 - core, 0, small_half)]
    cuts = [
        pl.ds(pl.multiple_of(half * small_half, small_half) + first, size)
        for half, first, size in spans
    ]
    term_copies = {}

    def send_term(i, n):
        (half, first, size), cut = spans[n], cuts[n]

        def make(at):
            term_out[i, cut, at] = term(1, i, half, at, first, size).astype(short)

        by_columns(make)
        term_copies[i, n] = remote(
            term_out.at[i, cut], term_in.at[i, cut],
            term_send.at[0], term_recv.at[len(cuts) * i + n], weight_mate,
        )

    def own_term(i):
        def make(at):
            for half in range(2):
                term_own[i, half * small_half : (half + 1) * small_half, at] = term(
                    0, i, half, at
                )

        by_columns(make)

    def finish(i):
        out = (grad_gate, grad_up, grad_down)[i]
        for n, cut in enumerate(cuts):
            term_copies[i, n].wait_recv()
            out[cut, :] = (term_own[i, cut, :] + wide(term_in[i, cut, :])).astype(short)

    def expert_dx(k, part_of, at):
        here = pl.ds(pl.multiple_of(part_of * half_rows, half_rows), half_rows)
        return sum(
            jnp.dot(
                act[k, half, i + 1, here, :], w_all[i, half, :, :, at].reshape(hidden, LANES),
                preferred_element_type=jnp.float32,
            )
            for half in range(2)
            for i in range(2)
        ).reshape(devices_ep // 2, capacity, LANES)

    dx_blocks = ends + mids + near + [flip(s, 0), s]
    dx_copies = []

    def send_dx(part_of, blocks):
        here = pl.ds(part_of * (devices_ep // 2), devices_ep // 2)

        def make(at):
            dx_out[here, :, at] = expert_dx(1, part_of, at).astype(short)

        by_columns(make)
        for n in blocks:
            block = dx_blocks[n]
            dx_copies.append(
                remote(
                    dx_out.at[block], dx_in.at[block], dx_send.at[0], dx_recv.at[n], row_mate
                )
            )

    def own_dx(part_of):
        here = pl.ds(part_of * (devices_ep // 2), devices_ep // 2)

        def make(at):
            dx_own[here, :, at] = expert_dx(0, part_of, at)

        by_columns(make)

    backs = []

    def give_back(n):
        block = dx_blocks[n]
        dx_copies[n].wait_recv()
        dx_sum[block] = (dx_own[block] + wide(dx_in[block])).astype(short)
        if n < devices_ep - 1:
            backs.append(
                remote(
                    dx_sum.at[block], owned(slot_rows, s), back_send.at[0], back_recv.at[0],
                    (r, block),
                )
            )
        else:
            backs.append(local(dx_sum.at[block], owned(slot_rows, s), self_sem.at[2]))

    pass_on(0, None)
    pass_on(0, 0)
    pass_on(0, 1)
    pass_on(1, None)
    pass_on(0, 2)
    pass_on(0, 5)
    pass_on(0, 6)
    pass_on(0, 3)
    pass_on(0, 4)

    @pl.when(jnp.logical_not(at_end))
    def _():
        send(1, (3, 4, 5, 6))

    @pl.when(at_end)
    def _():
        send(1, (3, 5))

    for n in CORE + NEAR:
        pass_on(1, n)
    w_copies[0].wait_recv()
    project(0, 0)
    hand_over(0, 0)
    send_pair(0, 0)

    @pl.when(at_end)
    def _():
        send(1, (6,))

    landed(x_all.at[1], fx_recv)
    project(1, 0)
    hand_over(1, 0)
    send_pair(1, 0)
    w_copies[1].wait_recv()
    project(0, 1)
    hand_over(0, 1)
    project(1, 1)
    hand_over(1, 1)
    send_pair(0, 1)

    @pl.when(at_end)
    def _():
        send(1, (4,))

    send_pair(1, 1)
    pass_on(1, 3)
    pass_on(1, 5, 4)
    pass_on(1, 6, 5)
    pass_on(1, 4, 6)
    make_hidden(0)
    w_copies[2].wait_recv()
    project(0, 2)
    hand_over(0, 2)
    make_hidden(1)
    transpose(core, 0)
    landed(d_all.at[1], fd_recv)
    send_term(2, 0)
    send_term(2, 1)
    send_pair(0, 2)
    take_hidden()
    transpose(1 - core, 0)
    send_term(2, 2)
    project(1, 2)
    hand_over(1, 2)
    send_pair(1, 2)
    own_term(2)
    make_slopes(0)
    make_slopes(1)
    act_copies[0, 1].wait_recv()
    act_copies[1, 1].wait_recv()
    send_dx(1 - side, range(0, 4))
    send_dx(side, range(4, 8))
    for i in range(2):
        for half in range(2):
            transpose(half, i + 1)
        for n in range(len(cuts)):
            send_term(i, n)
    own_dx(1 - side)
    for n in range(4):
        give_back(n)
    own_dx(side)
    finish(2)
    own_term(0)
    own_term(1)
    for n in range(4, 8):
        give_back(n)
    finish(0)
    backs[-1].wait()
    landed(dx_sum.at[pl.ds(0, devices_ep - 1)], back_recv)

    for n, out in enumerate((in_0, in_1, in_2, in_3)):
        out[...] = jnp.dot(
            pick_t[...], slot_rows[:, n * quarter : (n + 1) * quarter],
            preferred_element_type=jnp.float32,
        ).astype(short)
    finish(1)
    most = pl.ds(0, devices_ep - 1)
    for sem in (x_send, d_send, back_send):
        landed(dx_sum.at[most], sem)
    for sem in (fx_send, fd_send, dx_send):
        landed(dx_sum, sem)
    for sem in (give_send, pair_send, act_send):
        landed(got, sem)
    for sem in (w_send, term_send):
        landed(term_in, sem)


def store_kernel(*refs):
    grads = refs[GROUP : GROUP + 3]
    whole, outs, sem = refs[GROUP + 3], refs[GROUP + 4 : GROUP + 7], refs[-1]
    quarter = whole.shape[1] // GROUP
    stores = [
        pltpu.make_async_copy(part, whole.at[:, pl.ds(n * quarter, quarter)], sem.at[n])
        for n, part in enumerate(refs[:GROUP])
    ]
    stores += [
        pltpu.make_async_copy(grad, out, sem.at[GROUP + n])
        for n, (grad, out) in enumerate(zip(grads, outs))
    ]
    for store in stores:
        store.start()
    for store in stores:
        store.wait()


def fast_body(tokens, out_grad, route_weight, expert_ids, w_gate, w_up, w_down):
    devices_ep = lax.axis_size("ep")
    experts = devices_ep // GROUP
    token_count = tokens.shape[0]
    capacity = 6 * GROUP * token_count * TOP // (8 * devices_ep)
    quarter = D // GROUP
    hidden = w_gate.shape[0]
    rows = devices_ep * capacity
    slots = experts * capacity
    short = jnp.bfloat16
    vmem = pl.BlockSpec(memory_space=pltpu.VMEM)
    far = pl.BlockSpec(memory_space=pltpu.HBM)
    grad = jax.ShapeDtypeStruct(w_gate.shape, short)
    dma = pltpu.SemaphoreType.DMA
    results = pl.pallas_call(
        expert_kernel,
        out_shape=(jax.ShapeDtypeStruct((token_count, quarter), short),) * GROUP + (grad,) * 3,
        in_specs=[far] * 7,
        out_specs=(vmem,) * (GROUP + 3),
        scratch_shapes=[
            pltpu.VMEM((1, token_count), jnp.int32),
            pltpu.VMEM((1, token_count), jnp.float32),
            pltpu.VMEM(tokens.shape, short),
            pltpu.VMEM(tokens.shape, short),
            pltpu.VMEM((slots, token_count), short),
            pltpu.VMEM((token_count, slots), short),
            pltpu.VMEM((slots, 1), jnp.float32),
            pltpu.VMEM((slots, D), short),
            pltpu.VMEM((slots, D), short),
            pltpu.VMEM((slots, D), short),
            pltpu.VMEM((2, devices_ep, capacity, quarter), short),
            pltpu.VMEM((2, devices_ep, capacity, quarter), short),
            pltpu.VMEM((3, 2, 2, hidden // 2, quarter), short),
            pltpu.VMEM((2, 2, 3, rows, hidden), short),
            pltpu.VMEM((2, 3, rows, hidden), short),
            pltpu.VMEM((2, 3, rows, hidden), short),
            pltpu.VMEM((2, 3, rows, hidden), short),
            pltpu.VMEM((2, 2, 3, rows, hidden), short),
            pltpu.VMEM((2, 3, hidden, 2 * rows), short),
            pltpu.VMEM((3, hidden, quarter), short),
            pltpu.VMEM((3, hidden, quarter), short),
            pltpu.VMEM((3, hidden, quarter), jnp.float32),
            pltpu.VMEM((devices_ep, capacity, quarter), short),
            pltpu.VMEM((devices_ep, capacity, quarter), short),
            pltpu.VMEM((devices_ep, capacity, quarter), jnp.float32),
            pltpu.VMEM((devices_ep, capacity, quarter), short),
        ]
        + [dma((4,)), dma((GROUP,)), dma((3,)), dma((1,)), dma((3,)), dma((3,))]
        + [dma((1,)), dma((1, devices_ep)), dma((1,)), dma((capacity // 16, devices_ep))]
        + [dma((1,))] * 4
        + [dma((1,)), dma((6,))] * 2
        + [dma((1,)), dma((4,)), dma((1,)), dma((9,)), dma((1,)), dma((devices_ep,))]
        + [dma((1,))] * 2,
        compiler_params=pltpu.CompilerParams(
            collective_id=0, has_side_effects=True, vmem_limit_bytes=48 * 2**20
        ),
    )(
        *(
            pltpu.with_memory_space_constraint(value, pltpu.HBM)
            for value in (
                tokens, out_grad, route_weight.reshape(1, token_count),
                expert_ids.reshape(1, token_count), w_gate, w_up, w_down,
            )
        )
    )
    return tuple(
        pl.pallas_call(
            store_kernel,
            out_shape=(jax.ShapeDtypeStruct(tokens.shape, short), grad, grad, grad),
            in_specs=[vmem] * len(results),
            out_specs=(far,) * 4,
            scratch_shapes=[dma((len(results),))],
            compiler_params=pltpu.CompilerParams(vmem_limit_bytes=40 * 2**20),
        )(*results)
    )


def solution(mesh):
    devices_ep = mesh.shape["ep"]

    def step(*arrays):
        token_count = arrays[0].shape[0]
        capacity = 6 * GROUP * token_count * TOP // (8 * devices_ep)
        hidden = arrays[4].shape[0]
        fits = capacity % 48 == 0 and hidden % 256 == 0 and token_count % 128 == 0
        fits = fits and mesh.shape["dp"] == 4 and devices_ep == 2 * GROUP
        return (fast_body if fits else body)(*arrays)

    placed = (
        P(("dp", "ep"), None),
        P(("dp", "ep"), None),
        P(("dp", "ep"), None),
        P(("dp", "ep"), None),
        P("dp", "ep"),
        P("dp", "ep"),
        P("dp", "ep"),
    )
    return jax.shard_map(
        step,
        mesh=mesh,
        in_specs=placed,
        out_specs=(P(("dp", "ep"), None), P("dp", "ep"), P("dp", "ep"), P("dp", "ep")),
        check_vma=False,
    )
```

```python
import jax
import jax.numpy as jnp
from jax import lax
from jax.experimental import pallas as pl
from jax.experimental.pallas import tpu as pltpu
from jax.sharding import PartitionSpec as P

D = 7168
GROUP = 4
TOP = 1


CONTRACT_LAST = (((1,), (1,)), ((), ()))
CONTRACT_FIRST = (((0,), (0,)), ((), ()))


def as_sent(value):

    def short(part):
        return part.astype(jnp.bfloat16) if part.dtype == jnp.float32 else part

    return jax.tree.map(short, value)


def from_partner(value, axis, distance):
    mask = 2**distance
    pairs = [(source, source ^ mask) for source in range(lax.axis_size(axis))]
    return lax.ppermute(value, axis, pairs)


def slot_tables(expert_ids, route_weight, experts, capacity):
    token_count, top_count = expert_ids.shape
    pair_count = token_count * top_count
    flat_ids = expert_ids.reshape(pair_count)
    onehot = (flat_ids[:, None] == jnp.arange(experts, dtype=jnp.int32)[None, :]).astype(jnp.int32)
    before = jnp.cumsum(onehot, axis=0) - onehot
    ranks = jnp.sum(before * onehot, axis=1)
    kept = ranks < capacity
    slots = jnp.where(kept, flat_ids * capacity + ranks, 0)
    slot_ids = jnp.arange(experts * capacity, dtype=jnp.int32)
    match = (slots[None, :] == slot_ids[:, None]) & kept[None, :]
    pair_ids = jnp.arange(pair_count, dtype=jnp.int32)
    pair_of_slot = jnp.sum(jnp.where(match, pair_ids[None, :], 0), axis=1)
    filled = jnp.any(match, axis=1)
    flat_weight = route_weight.reshape(pair_count)
    weight_of_slot = jnp.sum(jnp.where(match, flat_weight[None, :], jnp.float32(0.0)), axis=1)
    return (kept, slots, pair_of_slot // top_count, filled, weight_of_slot)


def activations(gate, up, back):
    logistic = jax.nn.sigmoid(gate)
    silu = gate * logistic
    hidden = (silu * up).astype(jnp.bfloat16)
    d_gate = (back * up * logistic * (1.0 + gate * (1.0 - logistic))).astype(jnp.bfloat16)
    d_up = (back * silu).astype(jnp.bfloat16)
    return (hidden, d_gate, d_up)


def swap(value, axis, distance):
    return from_partner(value, axis, distance)


def wide(value):
    return value.astype(jnp.float32)


def dot_last(left, right):
    return lax.dot_general(left, right, CONTRACT_LAST, preferred_element_type=jnp.float32)


def dot_first(left, right):
    return lax.dot_general(left, right, CONTRACT_FIRST, preferred_element_type=jnp.float32)


def body(tokens, out_grad, route_weight, expert_ids, w_gate, w_up, w_down):
    devices_ep = lax.axis_size("ep")
    experts = devices_ep // GROUP
    token_count = tokens.shape[0]
    capacity = 6 * GROUP * token_count * TOP // (8 * devices_ep)
    quarter = D // GROUP
    short = jnp.bfloat16
    kept, slots, token_of_slot, filled, weight_of_slot = slot_tables(
        expert_ids, route_weight, experts, capacity
    )
    other_w = tuple(swap(w, "dp", 1) for w in (w_gate, w_up, w_down))
    token_ids = jnp.arange(token_count, dtype=jnp.int32)
    pick = ((token_of_slot[:, None] == token_ids[None, :]) & filled[:, None]).astype(short)
    x_slots = jnp.dot(pick, tokens, preferred_element_type=jnp.float32).astype(short)
    d_slots = (
        jnp.dot(pick, out_grad, preferred_element_type=jnp.float32) * weight_of_slot[:, None]
    ).astype(short)

    def to_owners(rows):
        shaped = rows.reshape(experts, capacity, GROUP, quarter).transpose(0, 2, 1, 3)
        return shaped.reshape(devices_ep, capacity, quarter)

    def sent(rows):
        return lax.all_to_all(to_owners(rows), "ep", split_axis=0, concat_axis=0, tiled=True)

    row_count = devices_ep * capacity
    x_own = sent(x_slots).reshape(row_count, quarter)
    d_own = sent(d_slots).reshape(row_count, quarter)
    x_other, d_other = swap(x_own, "dp", 0), swap(d_own, "dp", 0)
    core = lax.axis_index("ep") % 2
    weights = ((w_gate, w_up, w_down), other_w)
    acts = []
    for x_rows, d_rows in ((x_own, d_own), (x_other, d_other)):
        terms = [
            jnp.concatenate(
                [dot_last(x_rows, wg), dot_last(x_rows, wu), dot_last(d_rows, wd)], axis=1
            ).astype(short)
            for wg, wu, wd in weights
        ]
        give = jnp.where(core == 0, terms[1], terms[0])
        keep = jnp.where(core == 0, terms[0], terms[1])
        pair = (wide(keep) + wide(swap(give, "ep", 0))).astype(short)
        total = wide(pair) + wide(swap(pair, "ep", 1))
        width = total.shape[1] // 3
        mine = jnp.concatenate(
            activations(total[:, :width], total[:, width : 2 * width], total[:, 2 * width :]), axis=1
        )
        theirs = swap(mine, "ep", 0)
        first = jnp.where(core == 0, mine, theirs)
        second = jnp.where(core == 0, theirs, mine)
        acts.append(
            tuple(
                tuple(half[:, piece * width : (piece + 1) * width] for piece in range(3))
                for half in (first, second)
            )
        )

    def grads(half):
        (h0, g0, u0), (h1, g1, u1) = acts[0][half], acts[1][half]
        return (
            dot_first(g0, x_own) + dot_first(g1, x_other),
            dot_first(u0, x_own) + dot_first(u1, x_other),
            dot_first(h0, d_own) + dot_first(h1, d_other),
        )

    def dx(rows):
        return sum(
            jnp.dot(acts[rows][half][1], weights[half][0], preferred_element_type=jnp.float32)
            + jnp.dot(acts[rows][half][2], weights[half][1], preferred_element_type=jnp.float32)
            for half in range(2)
        )

    dx_in = swap(dx(1).astype(short), "dp", 0)
    away = tuple(swap(term.astype(short), "dp", 1) for term in grads(1))
    expert_dx = (dx(0) + wide(dx_in)).astype(short)
    grad_gate, grad_up, grad_down = (
        (own + wide(term)).astype(short) for own, term in zip(grads(0), away)
    )
    returned = lax.all_to_all(
        expert_dx.reshape(devices_ep, capacity, quarter),
        "ep",
        split_axis=0,
        concat_axis=0,
        tiled=True,
    )
    slot_rows = (
        returned.reshape(experts, GROUP, capacity, quarter)
        .transpose(0, 2, 1, 3)
        .reshape(experts * capacity, D)
    )
    in_grad = dot_first(pick, slot_rows).astype(short)
    return (in_grad, grad_gate, grad_up, grad_down)

MESH = pl.DeviceIdType.MESH


def flip(index, bit):
    size = 1 << bit
    return index + size - 2 * size * lax.rem(lax.div(index, size), 2)


def expert_kernel(
    tokens, out_grad, route, ids, wg, wu, wd, in_0, in_1, in_2, in_3, grad_gate, grad_up, grad_down,
    named, paid, tok, ogr, pick, pick_t, scale, xs, ds, slot_rows, x_all, d_all, w_all, part, got, pair, across,
    act, act_t, term_out, term_in, term_own, dx_out, dx_in, dx_own, dx_sum,
    in_sem, tok_sem, w_local, w_send, w_recv, self_sem, x_send, x_recv, d_send, d_recv,
    fx_send, fx_recv, fd_send, fd_recv, give_send, give_recv, pair_send, pair_recv,
    side_send, side_recv, act_send, act_recv, term_send, term_recv, dx_send, dx_recv, back_send, back_recv,
):
    devices_ep, capacity, quarter = dx_sum.shape
    rows = devices_ep * capacity
    half_rows = rows // 2
    hidden = wg.shape[0]
    slots, token_count = pick.shape
    experts = slots // capacity
    short = jnp.bfloat16
    r, s = lax.axis_index("dp"), lax.axis_index("ep")
    core, z = lax.rem(s, 2), lax.div(s, 2)
    side = lax.div(z, 2)
    end = 1 - lax.rem(z + side, 2)
    at_end = end == 1
    row_mate, weight_mate = (flip(r, 0), s), (flip(r, 1), s)
    core_mate, chip_mate = (r, flip(s, 0)), (r, flip(s, 1))
    far_mid, far_end = 2 * (2 - side), 2 * (3 - 3 * side)
    near = [flip(s, 1), flip(flip(s, 1), 0)]
    mids = [far_mid + core, far_mid + 1 - core]
    ends = [far_end + core, far_end + 1 - core]
    others = [flip(s, 0)] + near + ends + mids
    CORE, NEAR, FAR = [0], [1, 2], [3, 4, 5, 6]

    def local(source, target, sem):
        copy = pltpu.make_async_copy(source, target, sem)
        copy.start()
        return copy

    small = [local(ids, named, in_sem.at[2]), local(route, paid, in_sem.at[3])]
    order = (5, 6, 3, 4)
    columns = [
        pl.ds(pl.multiple_of(lax.rem(others[n], GROUP) * quarter, 128), quarter) for n in order
    ]
    tok_copies = [
        local(tokens.at[:, at], tok.at[:, at], tok_sem.at[n]) for n, at in enumerate(columns)
    ]
    small_half = hidden // 2

    def load_weight(i, w):
        for half in range(2):
            local(
                w.at[pl.ds(half * small_half, small_half)], w_all.at[i, half, 0], w_local.at[i]
            )

    load_weight(0, wg)

    barrier = pltpu.get_barrier_semaphore()
    peers = [row_mate, weight_mate] + [(r, other) for other in others]
    for peer in peers:
        pl.semaphore_signal(barrier, inc=1, device_id=peer, device_id_type=MESH)

    for copy in small:
        copy.wait()
    name = named[...]
    wide_rows = max(8, experts)
    expert_row = lax.broadcasted_iota(jnp.int32, (wide_rows, token_count), 0)
    onehot = jnp.where(expert_row == name, 1.0, 0.0)
    earlier = lax.broadcasted_iota(jnp.int32, (token_count, token_count), 0) < (
        lax.broadcasted_iota(jnp.int32, (token_count, token_count), 1)
    )
    before = jnp.dot(
        onehot.astype(short), jnp.where(earlier, 1.0, 0.0).astype(short),
        preferred_element_type=jnp.float32,
    )
    rank = jnp.sum(before * onehot, axis=0, keepdims=True)
    slot = jnp.where(rank < capacity, name.astype(jnp.float32) * capacity + rank, -1.0)
    slot_row = lax.broadcasted_iota(jnp.int32, (slots, token_count), 0).astype(jnp.float32)
    match = jnp.where(slot_row == slot, 1.0, 0.0)
    pick[...] = match.astype(short)
    scale[...] = jnp.sum(match * paid[...], axis=1, keepdims=True)
    pick_t[...] = match.T.astype(short)

    def by_quarters(fn):
        def one(n, carry):
            fn(pl.ds(pl.multiple_of(n * quarter, quarter), quarter))
            return carry

        lax.fori_loop(0, GROUP, one, 0)

    def fill_x(at):
        xs[:, at] = jnp.dot(
            pick[...], tok[:, at], preferred_element_type=jnp.float32
        ).astype(short)

    def fill_d(at):
        ds[:, at] = (
            jnp.dot(pick[...], ogr[:, at], preferred_element_type=jnp.float32) * scale[...]
        ).astype(short)

    tok_copies[0].wait()
    ogr_copy = local(out_grad, ogr, in_sem.at[1])
    load_weight(1, wu)
    load_weight(2, wd)

    def remote(source, target, send, recv, peer, start=True):
        copy = pltpu.make_async_remote_copy(
            src_ref=source, dst_ref=target, send_sem=send, recv_sem=recv,
            device_id=peer, device_id_type=MESH,
        )
        if start:
            copy.start()
        return copy

    def owned(ref, device, part=slice(None)):
        first, size = (0, capacity) if part == slice(None) else part
        row = pl.multiple_of(lax.div(device, GROUP) * capacity, 16) + first
        column = pl.multiple_of(lax.rem(device, GROUP) * quarter, 128)
        return ref.at[pl.ds(pl.multiple_of(row, 16), size), pl.ds(column, quarter)]

    def landed(ref, sem):
        pltpu.make_async_copy(ref, ref, sem.at[0]).wait()

    w_copies = []

    def send_weight(i):
        if i:
            landed(w_all.at[i, :, 0], w_local.at[pl.ds(i, 1)])
        w_copies.append(
            remote(w_all.at[i, :, 0], w_all.at[i, :, 1], w_send.at[0], w_recv.at[i], weight_mate)
        )

    SLICE = 16
    WHOLE = ((0, capacity),)
    SPLIT = tuple((first, SLICE) for first in range(0, capacity, SLICE))
    kinds = ((xs, x_all, x_send, x_recv), (ds, d_all, d_send, d_recv))

    def parts_of(kind, n):
        return SPLIT if kind and n is not None and n in FAR else WHOLE

    def flow(kind, n, piece):
        source, target, send, recv = kinds[kind]
        peer = others[n]
        part = parts_of(kind, n)[piece]
        return remote(
            owned(source, peer, part), target.at[0, s, pl.ds(*part)], send.at[0],
            recv.at[piece, s], (r, peer), start=False,
        )

    def send(kind, which):
        for n in which:
            for piece in range(len(parts_of(kind, n))):
                flow(kind, n, piece).start()

    self_copies = []

    fill_x(columns[0])
    landed(w_all.at[0, :, 0], w_local)
    pl.semaphore_wait(barrier, len(peers))
    send_weight(0)
    for n, peer in enumerate(order):
        if n:
            tok_copies[n].wait()
            fill_x(columns[n])

        @pl.when(jnp.logical_not(at_end))
        def _(peer=peer):
            send(0, (peer,))

    send(0, CORE + NEAR)
    self_copies.append(local(owned(xs, s), x_all.at[0, s], self_sem.at[0]))
    ogr_copy.wait()
    by_quarters(fill_d)
    send_weight(1)
    send_weight(2)
    send(1, CORE + NEAR)
    self_copies.append(local(owned(ds, s), d_all.at[0, s], self_sem.at[1]))

    @pl.when(at_end)
    def _():
        send(0, FAR)


    def pass_on(kind, n, at_middle=None):
        _, target, _, recv = kinds[kind]
        origin = s if n is None else others[n]
        if at_middle is not None:
            origin = end * origin + (1 - end) * others[at_middle]
        to_send, to_recv = ((fx_send, fx_recv), (fd_send, fd_recv))[kind]
        if n is None:
            self_copies[kind].wait()
        for piece, part in enumerate(parts_of(kind, n)):
            here = target.at[0, origin, pl.ds(*part)]
            if n is not None:
                remote(
                    here, here, x_send.at[0], recv.at[piece, origin], (r, origin), start=False
                ).wait_recv()
            remote(
                here, target.at[1, origin, pl.ds(*part)], to_send.at[0], to_recv.at[0], row_mate
            )

    def project(k, i):
        block = (x_all if i < 2 else d_all)[k].reshape(rows, quarter)
        both = dot_last(block, w_all[i].reshape(2 * hidden, quarter)).astype(short)
        for half in range(2):
            part[k, half, i] = both[:, half * hidden : (half + 1) * hidden]

    STEP = 48

    def by_rows(fn):
        def one(n, carry):
            fn(pl.ds(pl.multiple_of(n * STEP, STEP), STEP))
            return carry

        lax.fori_loop(0, rows // STEP, one, 0)

    def by_my_rows(fn):
        def one(n, carry):
            fn(pl.ds(pl.multiple_of(mine * half_rows + n * STEP, STEP), STEP))
            return carry

        lax.fori_loop(0, half_rows // STEP, one, 0)

    mine = lax.rem(z, 2)
    my_rows = pl.ds(pl.multiple_of(mine * half_rows, half_rows), half_rows)
    their_rows = pl.ds(pl.multiple_of((1 - mine) * half_rows, half_rows), half_rows)
    give_copies, pair_copies, act_copies, side_copies = {}, {}, {}, {}

    def hand_over(k, i):
        give_copies[k, i] = remote(
            part.at[k, 1 - core, i], got.at[k, i],
            give_send.at[0], give_recv.at[3 * k + i], core_mate,
        )

    def send_pair(k, i):
        give_copies[k, i].wait_recv()

        def add_pair(at):
            pair[k, i, at, :] = (wide(part[k, core, i, at, :]) + wide(got[k, i, at, :])).astype(
                short
            )

        by_rows(add_pair)
        pair_copies[k, i] = remote(
            pair.at[k, i, their_rows], across.at[k, i, their_rows],
            pair_send.at[0], pair_recv.at[3 * k + i], chip_mate,
        )

    def total(k, i, at):
        return wide(pair[k, i, at, :]) + wide(across[k, i, at, :])

    def share(k, stage, pieces):
        here = act.at[k, core, pieces, my_rows]
        side_copies[k, stage] = remote(
            here, here, side_send.at[0], side_recv.at[3 * k + stage], chip_mate
        )
        act_copies[k, stage, 0] = remote(
            here, here, act_send.at[0], act_recv.at[6 * k + 2 * stage], core_mate
        )

    def take_side(k, stage, pieces):
        side_copies[k, stage].wait_recv()
        here = act.at[k, core, pieces, their_rows]
        act_copies[k, stage, 1] = remote(
            here, here, act_send.at[0], act_recv.at[6 * k + 2 * stage + 1], core_mate
        )

    def make_hidden(k):
        for i in range(2):
            pair_copies[k, i].wait_recv()

        def one(at):
            gate, up = total(k, 0, at), total(k, 1, at)
            act[k, core, 0, at, :] = (gate * jax.nn.sigmoid(gate) * up).astype(short)

        by_my_rows(one)
        share(k, 0, pl.ds(0, 1))

    def take(stage):
        for k in range(2):
            for n in range(2):
                act_copies[k, stage, n].wait_recv()

    def make_slopes(k):
        pair_copies[k, 2].wait_recv()

        def one(at):
            made = activations(total(k, 0, at), total(k, 1, at), total(k, 2, at))
            act[k, core, 1, at, :] = made[1]
            act[k, core, 2, at, :] = made[2]

        by_my_rows(one)
        share(k, 1, pl.ds(1, 1))

    def transpose(half, piece):
        for k in range(2):
            act_t[half, piece, :, k * rows : (k + 1) * rows] = act[k, half, piece].T

    LANES = 896

    def by_columns(fn):
        def one(n, carry):
            fn(pl.ds(pl.multiple_of(n * LANES, LANES), LANES))
            return carry

        lax.fori_loop(0, quarter // LANES, one, 0)

    def term(which, i, half, at, first=0, size=small_half):
        block = (x_all if i < 2 else d_all)[:, :, :, at].reshape(2 * rows, LANES)
        units = pl.ds(which * small_half + first, size)
        return jnp.dot(
            act_t[half, (i + 1) % 3, units, :], block, preferred_element_type=jnp.float32
        )

    FIRST = small_half // 2
    spans = [(core, 0, FIRST), (core, FIRST, small_half - FIRST), (1 - core, 0, small_half)]
    cuts = [
        pl.ds(pl.multiple_of(half * small_half, small_half) + first, size)
        for half, first, size in spans
    ]
    term_copies = {}

    def send_term(i, n):
        (half, first, size), cut = spans[n], cuts[n]

        def make(at):
            term_out[i, cut, at] = term(1, i, half, at, first, size).astype(short)

        by_columns(make)
        term_copies[i, n] = remote(
            term_out.at[i, cut], term_in.at[i, cut],
            term_send.at[0], term_recv.at[len(cuts) * i + n], weight_mate,
        )

    def own_term(i):
        def make(at):
            for half in range(2):
                term_own[i, half * small_half : (half + 1) * small_half, at] = term(
                    0, i, half, at
                )

        by_columns(make)

    def finish(i):
        out = (grad_gate, grad_up, grad_down)[i]
        for n, cut in enumerate(cuts):
            term_copies[i, n].wait_recv()
            out[cut, :] = (term_own[i, cut, :] + wide(term_in[i, cut, :])).astype(short)

    def expert_dx(k, part_of, at):
        here = pl.ds(pl.multiple_of(part_of * half_rows, half_rows), half_rows)
        return sum(
            jnp.dot(
                act[k, half, i + 1, here, :], w_all[i, half, :, :, at].reshape(hidden, LANES),
                preferred_element_type=jnp.float32,
            )
            for half in range(2)
            for i in range(2)
        ).reshape(devices_ep // 2, capacity, LANES)

    dx_blocks = ends + mids + near + [flip(s, 0), s]
    dx_copies = []

    def send_dx(part_of, blocks):
        here = pl.ds(part_of * (devices_ep // 2), devices_ep // 2)

        def make(at):
            dx_out[here, :, at] = expert_dx(1, part_of, at).astype(short)

        by_columns(make)
        for n in blocks:
            block = dx_blocks[n]
            dx_copies.append(
                remote(
                    dx_out.at[block], dx_in.at[block], dx_send.at[0], dx_recv.at[n], row_mate
                )
            )

    def own_dx(part_of):
        here = pl.ds(part_of * (devices_ep // 2), devices_ep // 2)

        def make(at):
            dx_own[here, :, at] = expert_dx(0, part_of, at)

        by_columns(make)

    backs = []

    def give_back(n):
        block = dx_blocks[n]
        dx_copies[n].wait_recv()
        dx_sum[block] = (dx_own[block] + wide(dx_in[block])).astype(short)
        if n < devices_ep - 1:
            backs.append(
                remote(
                    dx_sum.at[block], owned(slot_rows, s), back_send.at[0], back_recv.at[0],
                    (r, block),
                )
            )
        else:
            backs.append(local(dx_sum.at[block], owned(slot_rows, s), self_sem.at[2]))

    pass_on(0, None)
    pass_on(0, 0)
    pass_on(0, 1)
    pass_on(1, None)
    pass_on(0, 2)
    pass_on(0, 5)
    pass_on(0, 6)
    pass_on(0, 3)
    pass_on(0, 4)

    @pl.when(jnp.logical_not(at_end))
    def _():
        send(1, (3, 4, 5, 6))

    @pl.when(at_end)
    def _():
        send(1, (3, 5))

    for n in CORE + NEAR:
        pass_on(1, n)
    w_copies[0].wait_recv()
    project(0, 0)
    hand_over(0, 0)
    send_pair(0, 0)

    @pl.when(at_end)
    def _():
        send(1, (6,))

    landed(x_all.at[1], fx_recv)
    project(1, 0)
    hand_over(1, 0)
    send_pair(1, 0)
    w_copies[1].wait_recv()
    project(0, 1)
    hand_over(0, 1)
    project(1, 1)
    hand_over(1, 1)
    send_pair(0, 1)

    @pl.when(at_end)
    def _():
        send(1, (4,))

    send_pair(1, 1)
    pass_on(1, 3)
    pass_on(1, 5, 4)

    @pl.when(at_end)
    def _():
        pass_on(1, 6, 5)
        pass_on(1, 4, 6)

    make_hidden(0)
    make_hidden(1)

    @pl.when(jnp.logical_not(at_end))
    def _():
        pass_on(1, 6, 5)
        pass_on(1, 4, 6)

    w_copies[2].wait_recv()
    project(0, 2)
    hand_over(0, 2)
    for k in range(2):
        take_side(k, 0, pl.ds(0, 1))
    transpose(core, 0)
    landed(d_all.at[1], fd_recv)
    send_term(2, 0)
    send_term(2, 1)
    send_pair(0, 2)
    take(0)
    transpose(1 - core, 0)
    send_term(2, 2)
    project(1, 2)
    hand_over(1, 2)
    send_pair(1, 2)
    own_term(2)
    make_slopes(0)
    make_slopes(1)
    for k in range(2):
        share(k, 2, pl.ds(2, 1))
    for k in range(2):
        take_side(k, 1, pl.ds(1, 1))
    take(1)
    for half in range(2):
        transpose(half, 1)
    for n in range(len(cuts)):
        send_term(0, n)
    for k in range(2):
        take_side(k, 2, pl.ds(2, 1))
    take(2)
    send_dx(1 - side, range(0, 4))
    send_dx(side, range(4, 8))
    for half in range(2):
        transpose(half, 2)
    for n in range(len(cuts)):
        send_term(1, n)
    own_dx(1 - side)
    for n in range(4):
        give_back(n)
    own_dx(side)
    finish(2)
    own_term(0)
    own_term(1)
    for n in range(4, 8):
        give_back(n)
    finish(0)
    backs[-1].wait()
    landed(dx_sum.at[pl.ds(0, devices_ep - 1)], back_recv)

    for n, out in enumerate((in_0, in_1, in_2, in_3)):
        out[...] = jnp.dot(
            pick_t[...], slot_rows[:, n * quarter : (n + 1) * quarter],
            preferred_element_type=jnp.float32,
        ).astype(short)
    finish(1)
    most = pl.ds(0, devices_ep - 1)
    for sem in (x_send, d_send, back_send):
        landed(dx_sum.at[most], sem)
    for sem in (fx_send, fd_send, dx_send):
        landed(dx_sum, sem)
    for sem in (give_send, act_send):
        landed(got, sem)
    for sem in (pair_send, side_send):
        landed(got.at[0], sem)
    for sem in (w_send, term_send):
        landed(term_in, sem)


def store_kernel(*refs):
    grads = refs[GROUP : GROUP + 3]
    whole, outs, sem = refs[GROUP + 3], refs[GROUP + 4 : GROUP + 7], refs[-1]
    quarter = whole.shape[1] // GROUP
    stores = [
        pltpu.make_async_copy(part, whole.at[:, pl.ds(n * quarter, quarter)], sem.at[n])
        for n, part in enumerate(refs[:GROUP])
    ]
    stores += [
        pltpu.make_async_copy(grad, out, sem.at[GROUP + n])
        for n, (grad, out) in enumerate(zip(grads, outs))
    ]
    for store in stores:
        store.start()
    for store in stores:
        store.wait()


def fast_body(tokens, out_grad, route_weight, expert_ids, w_gate, w_up, w_down):
    devices_ep = lax.axis_size("ep")
    experts = devices_ep // GROUP
    token_count = tokens.shape[0]
    capacity = 6 * GROUP * token_count * TOP // (8 * devices_ep)
    quarter = D // GROUP
    hidden = w_gate.shape[0]
    rows = devices_ep * capacity
    slots = experts * capacity
    short = jnp.bfloat16
    vmem = pl.BlockSpec(memory_space=pltpu.VMEM)
    far = pl.BlockSpec(memory_space=pltpu.HBM)
    grad = jax.ShapeDtypeStruct(w_gate.shape, short)
    dma = pltpu.SemaphoreType.DMA
    results = pl.pallas_call(
        expert_kernel,
        out_shape=(jax.ShapeDtypeStruct((token_count, quarter), short),) * GROUP + (grad,) * 3,
        in_specs=[far] * 7,
        out_specs=(vmem,) * (GROUP + 3),
        scratch_shapes=[
            pltpu.VMEM((1, token_count), jnp.int32),
            pltpu.VMEM((1, token_count), jnp.float32),
            pltpu.VMEM(tokens.shape, short),
            pltpu.VMEM(tokens.shape, short),
            pltpu.VMEM((slots, token_count), short),
            pltpu.VMEM((token_count, slots), short),
            pltpu.VMEM((slots, 1), jnp.float32),
            pltpu.VMEM((slots, D), short),
            pltpu.VMEM((slots, D), short),
            pltpu.VMEM((slots, D), short),
            pltpu.VMEM((2, devices_ep, capacity, quarter), short),
            pltpu.VMEM((2, devices_ep, capacity, quarter), short),
            pltpu.VMEM((3, 2, 2, hidden // 2, quarter), short),
            pltpu.VMEM((2, 2, 3, rows, hidden), short),
            pltpu.VMEM((2, 3, rows, hidden), short),
            pltpu.VMEM((2, 3, rows, hidden), short),
            pltpu.VMEM((2, 3, rows, hidden), short),
            pltpu.VMEM((2, 2, 3, rows, hidden), short),
            pltpu.VMEM((2, 3, hidden, 2 * rows), short),
            pltpu.VMEM((3, hidden, quarter), short),
            pltpu.VMEM((3, hidden, quarter), short),
            pltpu.VMEM((3, hidden, quarter), jnp.float32),
            pltpu.VMEM((devices_ep, capacity, quarter), short),
            pltpu.VMEM((devices_ep, capacity, quarter), short),
            pltpu.VMEM((devices_ep, capacity, quarter), jnp.float32),
            pltpu.VMEM((devices_ep, capacity, quarter), short),
        ]
        + [dma((4,)), dma((GROUP,)), dma((3,)), dma((1,)), dma((3,)), dma((3,))]
        + [dma((1,)), dma((1, devices_ep)), dma((1,)), dma((capacity // 16, devices_ep))]
        + [dma((1,))] * 4
        + [dma((1,)), dma((6,))] * 2
        + [dma((1,)), dma((6,)), dma((1,)), dma((12,)), dma((1,)), dma((9,)), dma((1,)), dma((devices_ep,))]
        + [dma((1,))] * 2,
        compiler_params=pltpu.CompilerParams(
            collective_id=0, has_side_effects=True, vmem_limit_bytes=48 * 2**20
        ),
    )(
        *(
            pltpu.with_memory_space_constraint(value, pltpu.HBM)
            for value in (
                tokens, out_grad, route_weight.reshape(1, token_count),
                expert_ids.reshape(1, token_count), w_gate, w_up, w_down,
            )
        )
    )
    return tuple(
        pl.pallas_call(
            store_kernel,
            out_shape=(jax.ShapeDtypeStruct(tokens.shape, short), grad, grad, grad),
            in_specs=[vmem] * len(results),
            out_specs=(far,) * 4,
            scratch_shapes=[dma((len(results),))],
            compiler_params=pltpu.CompilerParams(vmem_limit_bytes=40 * 2**20),
        )(*results)
    )


def solution(mesh):
    devices_ep = mesh.shape["ep"]

    def step(*arrays):
        token_count = arrays[0].shape[0]
        capacity = 6 * GROUP * token_count * TOP // (8 * devices_ep)
        hidden = arrays[4].shape[0]
        fits = capacity % 48 == 0 and hidden % 256 == 0 and token_count % 128 == 0
        fits = fits and mesh.shape["dp"] == 4 and devices_ep == 2 * GROUP
        return (fast_body if fits else body)(*arrays)

    placed = (
        P(("dp", "ep"), None),
        P(("dp", "ep"), None),
        P(("dp", "ep"), None),
        P(("dp", "ep"), None),
        P("dp", "ep"),
        P("dp", "ep"),
        P("dp", "ep"),
    )
    return jax.shard_map(
        step,
        mesh=mesh,
        in_specs=placed,
        out_specs=(P(("dp", "ep"), None), P("dp", "ep"), P("dp", "ep"), P("dp", "ep")),
        check_vma=False,
    )
```

```python
import jax
import jax.numpy as jnp
from jax import lax
from jax.experimental import pallas as pl
from jax.experimental.pallas import tpu as pltpu
from jax.sharding import PartitionSpec as P

D = 7168
GROUP = 4
TOP = 1


CONTRACT_LAST = (((1,), (1,)), ((), ()))
CONTRACT_FIRST = (((0,), (0,)), ((), ()))


def as_sent(value):

    def short(part):
        return part.astype(jnp.bfloat16) if part.dtype == jnp.float32 else part

    return jax.tree.map(short, value)


def from_partner(value, axis, distance):
    mask = 2**distance
    pairs = [(source, source ^ mask) for source in range(lax.axis_size(axis))]
    return lax.ppermute(value, axis, pairs)


def slot_tables(expert_ids, route_weight, experts, capacity):
    token_count, top_count = expert_ids.shape
    pair_count = token_count * top_count
    flat_ids = expert_ids.reshape(pair_count)
    onehot = (flat_ids[:, None] == jnp.arange(experts, dtype=jnp.int32)[None, :]).astype(jnp.int32)
    before = jnp.cumsum(onehot, axis=0) - onehot
    ranks = jnp.sum(before * onehot, axis=1)
    kept = ranks < capacity
    slots = jnp.where(kept, flat_ids * capacity + ranks, 0)
    slot_ids = jnp.arange(experts * capacity, dtype=jnp.int32)
    match = (slots[None, :] == slot_ids[:, None]) & kept[None, :]
    pair_ids = jnp.arange(pair_count, dtype=jnp.int32)
    pair_of_slot = jnp.sum(jnp.where(match, pair_ids[None, :], 0), axis=1)
    filled = jnp.any(match, axis=1)
    flat_weight = route_weight.reshape(pair_count)
    weight_of_slot = jnp.sum(jnp.where(match, flat_weight[None, :], jnp.float32(0.0)), axis=1)
    return (kept, slots, pair_of_slot // top_count, filled, weight_of_slot)


def activations(gate, up, back):
    logistic = jax.nn.sigmoid(gate)
    silu = gate * logistic
    hidden = (silu * up).astype(jnp.bfloat16)
    d_gate = (back * up * logistic * (1.0 + gate * (1.0 - logistic))).astype(jnp.bfloat16)
    d_up = (back * silu).astype(jnp.bfloat16)
    return (hidden, d_gate, d_up)


def swap(value, axis, distance):
    return from_partner(value, axis, distance)


def wide(value):
    return value.astype(jnp.float32)


def dot_last(left, right):
    return lax.dot_general(left, right, CONTRACT_LAST, preferred_element_type=jnp.float32)


def dot_first(left, right):
    return lax.dot_general(left, right, CONTRACT_FIRST, preferred_element_type=jnp.float32)


def body(tokens, out_grad, route_weight, expert_ids, w_gate, w_up, w_down):
    devices_ep = lax.axis_size("ep")
    experts = devices_ep // GROUP
    token_count = tokens.shape[0]
    capacity = 6 * GROUP * token_count * TOP // (8 * devices_ep)
    quarter = D // GROUP
    short = jnp.bfloat16
    kept, slots, token_of_slot, filled, weight_of_slot = slot_tables(
        expert_ids, route_weight, experts, capacity
    )
    other_w = tuple(swap(w, "dp", 1) for w in (w_gate, w_up, w_down))
    token_ids = jnp.arange(token_count, dtype=jnp.int32)
    pick = ((token_of_slot[:, None] == token_ids[None, :]) & filled[:, None]).astype(short)
    x_slots = jnp.dot(pick, tokens, preferred_element_type=jnp.float32).astype(short)
    d_slots = (
        jnp.dot(pick, out_grad, preferred_element_type=jnp.float32) * weight_of_slot[:, None]
    ).astype(short)

    def to_owners(rows):
        shaped = rows.reshape(experts, capacity, GROUP, quarter).transpose(0, 2, 1, 3)
        return shaped.reshape(devices_ep, capacity, quarter)

    def sent(rows):
        return lax.all_to_all(to_owners(rows), "ep", split_axis=0, concat_axis=0, tiled=True)

    row_count = devices_ep * capacity
    x_own = sent(x_slots).reshape(row_count, quarter)
    d_own = sent(d_slots).reshape(row_count, quarter)
    x_other, d_other = swap(x_own, "dp", 0), swap(d_own, "dp", 0)
    core = lax.axis_index("ep") % 2
    weights = ((w_gate, w_up, w_down), other_w)
    acts = []
    for x_rows, d_rows in ((x_own, d_own), (x_other, d_other)):
        terms = [
            jnp.concatenate(
                [dot_last(x_rows, wg), dot_last(x_rows, wu), dot_last(d_rows, wd)], axis=1
            ).astype(short)
            for wg, wu, wd in weights
        ]
        give = jnp.where(core == 0, terms[1], terms[0])
        keep = jnp.where(core == 0, terms[0], terms[1])
        pair = (wide(keep) + wide(swap(give, "ep", 0))).astype(short)
        total = wide(pair) + wide(swap(pair, "ep", 1))
        width = total.shape[1] // 3
        mine = jnp.concatenate(
            activations(total[:, :width], total[:, width : 2 * width], total[:, 2 * width :]), axis=1
        )
        theirs = swap(mine, "ep", 0)
        first = jnp.where(core == 0, mine, theirs)
        second = jnp.where(core == 0, theirs, mine)
        acts.append(
            tuple(
                tuple(half[:, piece * width : (piece + 1) * width] for piece in range(3))
                for half in (first, second)
            )
        )

    def grads(half):
        (h0, g0, u0), (h1, g1, u1) = acts[0][half], acts[1][half]
        return (
            dot_first(g0, x_own) + dot_first(g1, x_other),
            dot_first(u0, x_own) + dot_first(u1, x_other),
            dot_first(h0, d_own) + dot_first(h1, d_other),
        )

    def dx(rows):
        return sum(
            jnp.dot(acts[rows][half][1], weights[half][0], preferred_element_type=jnp.float32)
            + jnp.dot(acts[rows][half][2], weights[half][1], preferred_element_type=jnp.float32)
            for half in range(2)
        )

    dx_in = swap(dx(1).astype(short), "dp", 0)
    away = tuple(swap(term.astype(short), "dp", 1) for term in grads(1))
    expert_dx = (dx(0) + wide(dx_in)).astype(short)
    grad_gate, grad_up, grad_down = (
        (own + wide(term)).astype(short) for own, term in zip(grads(0), away)
    )
    returned = lax.all_to_all(
        expert_dx.reshape(devices_ep, capacity, quarter),
        "ep",
        split_axis=0,
        concat_axis=0,
        tiled=True,
    )
    slot_rows = (
        returned.reshape(experts, GROUP, capacity, quarter)
        .transpose(0, 2, 1, 3)
        .reshape(experts * capacity, D)
    )
    in_grad = dot_first(pick, slot_rows).astype(short)
    return (in_grad, grad_gate, grad_up, grad_down)

MESH = pl.DeviceIdType.MESH


def flip(index, bit):
    size = 1 << bit
    return index + size - 2 * size * lax.rem(lax.div(index, size), 2)


def expert_kernel(
    tokens, out_grad, route, ids, wg, wu, wd, in_0, in_1, in_2, in_3, grad_gate, grad_up, grad_down,
    named, paid, tok, ogr, pick, pick_t, scale, xs, ds, slot_rows, x_all, d_all, w_all, part, got, pair, across,
    act, act_t, term_out, term_in, term_own, dx_out, dx_in, dx_own, dx_sum,
    in_sem, tok_sem, w_local, w_send, w_recv, self_sem, x_send, x_recv, d_send, d_recv,
    fx_send, fx_recv, fd_send, fd_recv, give_send, give_recv, pair_send, pair_recv,
    side_send, side_recv, act_send, act_recv, term_send, term_recv, dx_send, dx_recv, back_send, back_recv,
):
    devices_ep, capacity, quarter = dx_sum.shape
    rows = devices_ep * capacity
    half_rows = rows // 2
    hidden = wg.shape[0]
    slots, token_count = pick.shape
    experts = slots // capacity
    short = jnp.bfloat16
    r, s = lax.axis_index("dp"), lax.axis_index("ep")
    core, z = lax.rem(s, 2), lax.div(s, 2)
    side = lax.div(z, 2)
    end = 1 - lax.rem(z + side, 2)
    at_end = end == 1
    row_mate, weight_mate = (flip(r, 0), s), (flip(r, 1), s)
    core_mate, chip_mate = (r, flip(s, 0)), (r, flip(s, 1))
    far_mid, far_end = 2 * (2 - side), 2 * (3 - 3 * side)
    near = [flip(s, 1), flip(flip(s, 1), 0)]
    mids = [far_mid + core, far_mid + 1 - core]
    ends = [far_end + core, far_end + 1 - core]
    others = [flip(s, 0)] + near + ends + mids
    CORE, NEAR, FAR = [0], [1, 2], [3, 4, 5, 6]

    def local(source, target, sem):
        copy = pltpu.make_async_copy(source, target, sem)
        copy.start()
        return copy

    small = [local(ids, named, in_sem.at[2]), local(route, paid, in_sem.at[3])]
    order = (5, 6, 3, 4)
    columns = [
        pl.ds(pl.multiple_of(lax.rem(others[n], GROUP) * quarter, 128), quarter) for n in order
    ]
    tok_copies = [
        local(tokens.at[:, at], tok.at[:, at], tok_sem.at[n]) for n, at in enumerate(columns)
    ]
    small_half = hidden // 2

    def load_weight(i, w):
        for half in range(2):
            local(
                w.at[pl.ds(half * small_half, small_half)], w_all.at[i, half, 0], w_local.at[i]
            )

    load_weight(0, wg)

    barrier = pltpu.get_barrier_semaphore()
    peers = [row_mate, weight_mate] + [(r, other) for other in others]
    for peer in peers:
        pl.semaphore_signal(barrier, inc=1, device_id=peer, device_id_type=MESH)

    for copy in small:
        copy.wait()
    name = named[...]
    wide_rows = max(8, experts)
    expert_row = lax.broadcasted_iota(jnp.int32, (wide_rows, token_count), 0)
    onehot = jnp.where(expert_row == name, 1.0, 0.0)
    earlier = lax.broadcasted_iota(jnp.int32, (token_count, token_count), 0) < (
        lax.broadcasted_iota(jnp.int32, (token_count, token_count), 1)
    )
    before = jnp.dot(
        onehot.astype(short), jnp.where(earlier, 1.0, 0.0).astype(short),
        preferred_element_type=jnp.float32,
    )
    rank = jnp.sum(before * onehot, axis=0, keepdims=True)
    slot = jnp.where(rank < capacity, name.astype(jnp.float32) * capacity + rank, -1.0)
    slot_row = lax.broadcasted_iota(jnp.int32, (slots, token_count), 0).astype(jnp.float32)
    match = jnp.where(slot_row == slot, 1.0, 0.0)
    pick[...] = match.astype(short)
    scale[...] = jnp.sum(match * paid[...], axis=1, keepdims=True)
    pick_t[...] = match.T.astype(short)

    def by_quarters(fn):
        def one(n, carry):
            fn(pl.ds(pl.multiple_of(n * quarter, quarter), quarter))
            return carry

        lax.fori_loop(0, GROUP, one, 0)

    def fill_x(at):
        xs[:, at] = jnp.dot(
            pick[...], tok[:, at], preferred_element_type=jnp.float32
        ).astype(short)

    def fill_d(at):
        ds[:, at] = (
            jnp.dot(pick[...], ogr[:, at], preferred_element_type=jnp.float32) * scale[...]
        ).astype(short)

    tok_copies[0].wait()
    ogr_copy = local(out_grad, ogr, in_sem.at[1])
    load_weight(1, wu)
    load_weight(2, wd)

    def remote(source, target, send, recv, peer, start=True):
        copy = pltpu.make_async_remote_copy(
            src_ref=source, dst_ref=target, send_sem=send, recv_sem=recv,
            device_id=peer, device_id_type=MESH,
        )
        if start:
            copy.start()
        return copy

    def owned(ref, device, part=slice(None)):
        first, size = (0, capacity) if part == slice(None) else part
        row = pl.multiple_of(lax.div(device, GROUP) * capacity, 16) + first
        column = pl.multiple_of(lax.rem(device, GROUP) * quarter, 128)
        return ref.at[pl.ds(pl.multiple_of(row, 16), size), pl.ds(column, quarter)]

    def landed(ref, sem):
        pltpu.make_async_copy(ref, ref, sem.at[0]).wait()

    w_copies = []

    def send_weight(i):
        if i:
            landed(w_all.at[i, :, 0], w_local.at[pl.ds(i, 1)])
        w_copies.append(
            remote(w_all.at[i, :, 0], w_all.at[i, :, 1], w_send.at[0], w_recv.at[i], weight_mate)
        )

    SLICE = 16
    WHOLE = ((0, capacity),)
    SPLIT = tuple((first, SLICE) for first in range(0, capacity, SLICE))
    kinds = ((xs, x_all, x_send, x_recv), (ds, d_all, d_send, d_recv))

    def parts_of(kind, n):
        return SPLIT if kind and n is not None and n in FAR else WHOLE

    def flow(kind, n, piece):
        source, target, send, recv = kinds[kind]
        peer = others[n]
        part = parts_of(kind, n)[piece]
        return remote(
            owned(source, peer, part), target.at[0, s, pl.ds(*part)], send.at[0],
            recv.at[piece, s], (r, peer), start=False,
        )

    def send(kind, which):
        for n in which:
            for piece in range(len(parts_of(kind, n))):
                flow(kind, n, piece).start()

    self_copies = []

    fill_x(columns[0])
    landed(w_all.at[0, :, 0], w_local)
    pl.semaphore_wait(barrier, len(peers))
    send_weight(0)
    for n, peer in enumerate(order):
        if n:
            tok_copies[n].wait()
            fill_x(columns[n])

        @pl.when(jnp.logical_not(at_end))
        def _(peer=peer):
            send(0, (peer,))

    send(0, CORE + NEAR)
    self_copies.append(local(owned(xs, s), x_all.at[0, s], self_sem.at[0]))
    ogr_copy.wait()
    by_quarters(fill_d)
    send_weight(1)
    send_weight(2)
    send(1, CORE + NEAR)
    self_copies.append(local(owned(ds, s), d_all.at[0, s], self_sem.at[1]))

    @pl.when(at_end)
    def _():
        send(0, FAR)


    def pass_on(kind, n, at_middle=None):
        _, target, _, recv = kinds[kind]
        origin = s if n is None else others[n]
        if at_middle is not None:
            origin = end * origin + (1 - end) * others[at_middle]
        to_send, to_recv = ((fx_send, fx_recv), (fd_send, fd_recv))[kind]
        if n is None:
            self_copies[kind].wait()
        for piece, part in enumerate(parts_of(kind, n)):
            here = target.at[0, origin, pl.ds(*part)]
            if n is not None:
                remote(
                    here, here, x_send.at[0], recv.at[piece, origin], (r, origin), start=False
                ).wait_recv()
            remote(
                here, target.at[1, origin, pl.ds(*part)], to_send.at[0], to_recv.at[0], row_mate
            )

    def project(k, i):
        block = (x_all if i < 2 else d_all)[k].reshape(rows, quarter)
        both = dot_last(block, w_all[i].reshape(2 * hidden, quarter)).astype(short)
        for half in range(2):
            part[k, half, i] = both[:, half * hidden : (half + 1) * hidden]

    STEP = 48

    def by_rows(fn):
        def one(n, carry):
            fn(pl.ds(pl.multiple_of(n * STEP, STEP), STEP))
            return carry

        lax.fori_loop(0, rows // STEP, one, 0)

    def by_my_rows(fn):
        def one(n, carry):
            fn(pl.ds(pl.multiple_of(mine * half_rows + n * STEP, STEP), STEP))
            return carry

        lax.fori_loop(0, half_rows // STEP, one, 0)

    mine = lax.rem(z, 2)
    my_rows = pl.ds(pl.multiple_of(mine * half_rows, half_rows), half_rows)
    their_rows = pl.ds(pl.multiple_of((1 - mine) * half_rows, half_rows), half_rows)
    give_copies, pair_copies, act_copies, side_copies = {}, {}, {}, {}

    def hand_over(k, i):
        give_copies[k, i] = remote(
            part.at[k, 1 - core, i], got.at[k, i],
            give_send.at[0], give_recv.at[3 * k + i], core_mate,
        )

    def send_pair(k, i):
        give_copies[k, i].wait_recv()

        def add_pair(at):
            pair[k, i, at, :] = (wide(part[k, core, i, at, :]) + wide(got[k, i, at, :])).astype(
                short
            )

        by_rows(add_pair)
        pair_copies[k, i] = remote(
            pair.at[k, i, their_rows], across.at[k, i, their_rows],
            pair_send.at[0], pair_recv.at[3 * k + i], chip_mate,
        )

    def total(k, i, at):
        return wide(pair[k, i, at, :]) + wide(across[k, i, at, :])

    def share(k, stage, pieces):
        here = act.at[k, core, pieces, my_rows]
        side_copies[k, stage] = remote(
            here, here, side_send.at[0], side_recv.at[3 * k + stage], chip_mate
        )
        act_copies[k, stage, 0] = remote(
            here, here, act_send.at[0], act_recv.at[6 * k + 2 * stage], core_mate
        )

    def take_side(k, stage, pieces):
        side_copies[k, stage].wait_recv()
        here = act.at[k, core, pieces, their_rows]
        act_copies[k, stage, 1] = remote(
            here, here, act_send.at[0], act_recv.at[6 * k + 2 * stage + 1], core_mate
        )

    def make_hidden(k):
        for i in range(2):
            pair_copies[k, i].wait_recv()

        def one(at):
            gate, up = total(k, 0, at), total(k, 1, at)
            act[k, core, 0, at, :] = (gate * jax.nn.sigmoid(gate) * up).astype(short)

        by_my_rows(one)
        share(k, 0, pl.ds(0, 1))

    def take(stage):
        for k in range(2):
            for n in range(2):
                act_copies[k, stage, n].wait_recv()

    def make_slopes(k):
        pair_copies[k, 2].wait_recv()

        def one(at):
            made = activations(total(k, 0, at), total(k, 1, at), total(k, 2, at))
            act[k, core, 1, at, :] = made[1]
            act[k, core, 2, at, :] = made[2]

        by_my_rows(one)
        share(k, 1, pl.ds(1, 1))

    def transpose(half, piece):
        for k in range(2):
            act_t[half, piece, :, k * rows : (k + 1) * rows] = act[k, half, piece].T

    LANES = 896

    def by_columns(fn):
        def one(n, carry):
            fn(pl.ds(pl.multiple_of(n * LANES, LANES), LANES))
            return carry

        lax.fori_loop(0, quarter // LANES, one, 0)

    def term(which, i, half, at):
        block = (x_all if i < 2 else d_all)[:, :, :, at].reshape(2 * rows, LANES)
        units = pl.ds(which * small_half, small_half)
        return jnp.dot(
            act_t[half, (i + 1) % 3, units, :], block, preferred_element_type=jnp.float32
        )

    left, right = pl.ds(0, LANES), pl.ds(LANES, quarter - LANES)
    spans = [(core, left), (core, right), (1 - core, pl.ds(0, quarter))]
    cuts = [
        (pl.ds(pl.multiple_of(half * small_half, small_half), small_half), columns_of)
        for half, columns_of in spans
    ]
    term_copies = {}

    def send_term(i, n):
        half, (rows_of, columns_of) = spans[n][0], cuts[n]

        def make(at):
            term_out[i, rows_of, at] = term(1, i, half, at).astype(short)

        if n < 2:
            make(columns_of)
        else:
            by_columns(make)
        term_copies[i, n] = remote(
            term_out.at[i, rows_of, columns_of], term_in.at[i, rows_of, columns_of],
            term_send.at[0], term_recv.at[len(cuts) * i + n], weight_mate,
        )

    def own_term(i):
        def make(at):
            for half in range(2):
                term_own[i, half * small_half : (half + 1) * small_half, at] = term(
                    0, i, half, at
                )

        by_columns(make)

    def finish(i):
        out = (grad_gate, grad_up, grad_down)[i]
        for n, cut in enumerate(cuts):
            term_copies[i, n].wait_recv()
            out[cut] = (term_own[(i, *cut)] + wide(term_in[(i, *cut)])).astype(short)

    def expert_dx(k, part_of, at):
        here = pl.ds(pl.multiple_of(part_of * half_rows, half_rows), half_rows)
        return sum(
            jnp.dot(
                act[k, half, i + 1, here, :], w_all[i, half, :, :, at].reshape(hidden, LANES),
                preferred_element_type=jnp.float32,
            )
            for half in range(2)
            for i in range(2)
        ).reshape(devices_ep // 2, capacity, LANES)

    dx_blocks = ends + mids + near + [flip(s, 0), s]
    dx_copies = []

    def send_dx(part_of, blocks):
        here = pl.ds(part_of * (devices_ep // 2), devices_ep // 2)

        def make(at):
            dx_out[here, :, at] = expert_dx(1, part_of, at).astype(short)

        by_columns(make)
        for n in blocks:
            block = dx_blocks[n]
            dx_copies.append(
                remote(
                    dx_out.at[block], dx_in.at[block], dx_send.at[0], dx_recv.at[n], row_mate
                )
            )

    def own_dx(part_of):
        here = pl.ds(part_of * (devices_ep // 2), devices_ep // 2)

        def make(at):
            dx_own[here, :, at] = expert_dx(0, part_of, at)

        by_columns(make)

    backs = []

    def give_back(n):
        block = dx_blocks[n]
        dx_copies[n].wait_recv()
        dx_sum[block] = (dx_own[block] + wide(dx_in[block])).astype(short)
        if n < devices_ep - 1:
            backs.append(
                remote(
                    dx_sum.at[block], owned(slot_rows, s), back_send.at[0], back_recv.at[0],
                    (r, block),
                )
            )
        else:
            backs.append(local(dx_sum.at[block], owned(slot_rows, s), self_sem.at[2]))

    pass_on(0, None)
    pass_on(0, 0)
    pass_on(0, 1)
    pass_on(1, None)
    pass_on(0, 2)
    pass_on(0, 5)
    pass_on(0, 6)
    pass_on(0, 3)
    pass_on(0, 4)

    @pl.when(jnp.logical_not(at_end))
    def _():
        send(1, (3, 4, 5, 6))

    @pl.when(at_end)
    def _():
        send(1, (3, 5))

    for n in CORE + NEAR:
        pass_on(1, n)
    w_copies[0].wait_recv()
    project(0, 0)
    hand_over(0, 0)
    send_pair(0, 0)

    @pl.when(at_end)
    def _():
        send(1, (6,))

    landed(x_all.at[1], fx_recv)
    project(1, 0)
    hand_over(1, 0)
    send_pair(1, 0)
    w_copies[1].wait_recv()
    project(0, 1)
    hand_over(0, 1)
    project(1, 1)
    hand_over(1, 1)
    send_pair(0, 1)

    @pl.when(at_end)
    def _():
        send(1, (4,))

    send_pair(1, 1)
    pass_on(1, 3)
    pass_on(1, 5, 4)

    @pl.when(at_end)
    def _():
        pass_on(1, 6, 5)
        pass_on(1, 4, 6)

    make_hidden(0)
    make_hidden(1)

    @pl.when(jnp.logical_not(at_end))
    def _():
        pass_on(1, 6, 5)
        pass_on(1, 4, 6)

    w_copies[2].wait_recv()
    project(0, 2)
    hand_over(0, 2)
    for k in range(2):
        take_side(k, 0, pl.ds(0, 1))
    transpose(core, 0)
    landed(d_all.at[1], fd_recv)
    send_term(2, 0)
    send_term(2, 1)
    send_pair(0, 2)
    take(0)
    transpose(1 - core, 0)
    send_term(2, 2)
    project(1, 2)
    hand_over(1, 2)
    send_pair(1, 2)
    own_term(2)
    make_slopes(0)
    make_slopes(1)
    for k in range(2):
        share(k, 2, pl.ds(2, 1))
    for k in range(2):
        take_side(k, 1, pl.ds(1, 1))
    take(1)
    for half in range(2):
        transpose(half, 1)
    for n in range(len(cuts)):
        send_term(0, n)
    for k in range(2):
        take_side(k, 2, pl.ds(2, 1))
    take(2)
    send_dx(1 - side, range(0, 4))
    send_dx(side, range(4, 8))
    for half in range(2):
        transpose(half, 2)
    for n in range(len(cuts)):
        send_term(1, n)
    own_dx(1 - side)
    for n in range(4):
        give_back(n)
    own_dx(side)
    finish(2)
    own_term(0)
    own_term(1)
    for n in range(4, 8):
        give_back(n)
    finish(0)
    backs[-1].wait()
    landed(dx_sum.at[pl.ds(0, devices_ep - 1)], back_recv)

    for n, out in enumerate((in_0, in_1, in_2, in_3)):
        out[...] = jnp.dot(
            pick_t[...], slot_rows[:, n * quarter : (n + 1) * quarter],
            preferred_element_type=jnp.float32,
        ).astype(short)
    finish(1)
    most = pl.ds(0, devices_ep - 1)
    for sem in (x_send, d_send, back_send):
        landed(dx_sum.at[most], sem)
    for sem in (fx_send, fd_send, dx_send):
        landed(dx_sum, sem)
    for sem in (give_send, act_send):
        landed(got, sem)
    for sem in (pair_send, side_send):
        landed(got.at[0], sem)
    for sem in (w_send, term_send):
        landed(term_in, sem)


def store_kernel(*refs):
    grads = refs[GROUP : GROUP + 3]
    whole, outs, sem = refs[GROUP + 3], refs[GROUP + 4 : GROUP + 7], refs[-1]
    quarter = whole.shape[1] // GROUP
    stores = [
        pltpu.make_async_copy(part, whole.at[:, pl.ds(n * quarter, quarter)], sem.at[n])
        for n, part in enumerate(refs[:GROUP])
    ]
    stores += [
        pltpu.make_async_copy(grad, out, sem.at[GROUP + n])
        for n, (grad, out) in enumerate(zip(grads, outs))
    ]
    for store in stores:
        store.start()
    for store in stores:
        store.wait()


def fast_body(tokens, out_grad, route_weight, expert_ids, w_gate, w_up, w_down):
    devices_ep = lax.axis_size("ep")
    experts = devices_ep // GROUP
    token_count = tokens.shape[0]
    capacity = 6 * GROUP * token_count * TOP // (8 * devices_ep)
    quarter = D // GROUP
    hidden = w_gate.shape[0]
    rows = devices_ep * capacity
    slots = experts * capacity
    short = jnp.bfloat16
    vmem = pl.BlockSpec(memory_space=pltpu.VMEM)
    far = pl.BlockSpec(memory_space=pltpu.HBM)
    grad = jax.ShapeDtypeStruct(w_gate.shape, short)
    dma = pltpu.SemaphoreType.DMA
    results = pl.pallas_call(
        expert_kernel,
        out_shape=(jax.ShapeDtypeStruct((token_count, quarter), short),) * GROUP + (grad,) * 3,
        in_specs=[far] * 7,
        out_specs=(vmem,) * (GROUP + 3),
        scratch_shapes=[
            pltpu.VMEM((1, token_count), jnp.int32),
            pltpu.VMEM((1, token_count), jnp.float32),
            pltpu.VMEM(tokens.shape, short),
            pltpu.VMEM(tokens.shape, short),
            pltpu.VMEM((slots, token_count), short),
            pltpu.VMEM((token_count, slots), short),
            pltpu.VMEM((slots, 1), jnp.float32),
            pltpu.VMEM((slots, D), short),
            pltpu.VMEM((slots, D), short),
            pltpu.VMEM((slots, D), short),
            pltpu.VMEM((2, devices_ep, capacity, quarter), short),
            pltpu.VMEM((2, devices_ep, capacity, quarter), short),
            pltpu.VMEM((3, 2, 2, hidden // 2, quarter), short),
            pltpu.VMEM((2, 2, 3, rows, hidden), short),
            pltpu.VMEM((2, 3, rows, hidden), short),
            pltpu.VMEM((2, 3, rows, hidden), short),
            pltpu.VMEM((2, 3, rows, hidden), short),
            pltpu.VMEM((2, 2, 3, rows, hidden), short),
            pltpu.VMEM((2, 3, hidden, 2 * rows), short),
            pltpu.VMEM((3, hidden, quarter), short),
            pltpu.VMEM((3, hidden, quarter), short),
            pltpu.VMEM((3, hidden, quarter), jnp.float32),
            pltpu.VMEM((devices_ep, capacity, quarter), short),
            pltpu.VMEM((devices_ep, capacity, quarter), short),
            pltpu.VMEM((devices_ep, capacity, quarter), jnp.float32),
            pltpu.VMEM((devices_ep, capacity, quarter), short),
        ]
        + [dma((4,)), dma((GROUP,)), dma((3,)), dma((1,)), dma((3,)), dma((3,))]
        + [dma((1,)), dma((1, devices_ep)), dma((1,)), dma((capacity // 16, devices_ep))]
        + [dma((1,))] * 4
        + [dma((1,)), dma((6,))] * 2
        + [dma((1,)), dma((6,)), dma((1,)), dma((12,)), dma((1,)), dma((9,)), dma((1,)), dma((devices_ep,))]
        + [dma((1,))] * 2,
        compiler_params=pltpu.CompilerParams(
            collective_id=0, has_side_effects=True, vmem_limit_bytes=48 * 2**20
        ),
    )(
        *(
            pltpu.with_memory_space_constraint(value, pltpu.HBM)
            for value in (
                tokens, out_grad, route_weight.reshape(1, token_count),
                expert_ids.reshape(1, token_count), w_gate, w_up, w_down,
            )
        )
    )
    return tuple(
        pl.pallas_call(
            store_kernel,
            out_shape=(jax.ShapeDtypeStruct(tokens.shape, short), grad, grad, grad),
            in_specs=[vmem] * len(results),
            out_specs=(far,) * 4,
            scratch_shapes=[dma((len(results),))],
            compiler_params=pltpu.CompilerParams(vmem_limit_bytes=40 * 2**20),
        )(*results)
    )


def solution(mesh):
    devices_ep = mesh.shape["ep"]

    def step(*arrays):
        token_count = arrays[0].shape[0]
        capacity = 6 * GROUP * token_count * TOP // (8 * devices_ep)
        hidden = arrays[4].shape[0]
        fits = capacity % 48 == 0 and hidden % 256 == 0 and token_count % 128 == 0
        fits = fits and mesh.shape["dp"] == 4 and devices_ep == 2 * GROUP
        return (fast_body if fits else body)(*arrays)

    placed = (
        P(("dp", "ep"), None),
        P(("dp", "ep"), None),
        P(("dp", "ep"), None),
        P(("dp", "ep"), None),
        P("dp", "ep"),
        P("dp", "ep"),
        P("dp", "ep"),
    )
    return jax.shard_map(
        step,
        mesh=mesh,
        in_specs=placed,
        out_specs=(P(("dp", "ep"), None), P("dp", "ep"), P("dp", "ep"), P("dp", "ep")),
        check_vma=False,
    )
```
